32 devices in a mesh: shard: 2 (over x), rep: 16 (over z, y, core).
Axes of the slice: x: 2, y: 2, z: 4, core: 2. Of those that a mesh axis runs over, the one named last changes fastest.
Arguments:
- frames_in: bfloat16 [16, 1500, 384], P('rep', 'shard'), may hold values from -6 to 6
- params: bfloat16 [2, 1774080], P(None, 'shard'), may hold values from -8 to 8
- moment_one: float32 [2, 1774080], P(None, 'shard'), may hold values from -170.41127 to 170.41127
- moment_two: float32 [2, 1774080], P(None, 'shard'), may hold values from 14.4 to 4800
- cotangent: bfloat16 [16, 1500, 384], P('rep', 'shard'), may hold values from -6 to 6
Outputs:
- encoded: bfloat16 [16, 1500, 384], P('rep', 'shard')
- frames_grad: bfloat16 [16, 1500, 384], P('rep', 'shard')
- param_grad: float32 [2, 1774080], P(None, 'shard')
- new_params: float32 [2, 1774080], P(None, 'shard')
- new_one: float32 [2, 1774080], P(None, 'shard')
- new_two: float32 [2, 1774080], P(None, 'shard')
The draws below stay inside these ranges and needn't reach their ends.
All inputs are finite; a program needn't handle non-finite values.
Results may differ from the reference program's by a relative error of at most 0.019.
Values may be sent and summed in bfloat16 or wider, within the bound.
A program may use at most 384 MiB of HBM per device.

```python
import jax
import jax.numpy as jnp
from jax import lax

D = 384
HEADS = 6
FF = 1536
FRAMES = 1500
LAYERS = 2
HEAD_DIM = 64
CLIPS = 16
LAYER_PARAMS = 1774080


def rough(key, shape_of):
    return jnp.clip(jax.random.normal(key, shape_of, jnp.float32), -4.0, 4.0)


def layer_vector(base):
    subkeys = jax.random.split(base, 7)
    column_scale = jnp.concatenate([jnp.full((2 * D,), 1.5, jnp.float32), jnp.ones((D,), jnp.float32)])
    qkv_w = rough(subkeys[0], (D, 3 * D)) * D ** (-0.5) * column_scale
    out_w = rough(subkeys[1], (D, D)) * (3.0 * D ** (-0.5))
    up_w = rough(subkeys[2], (D, FF)) * D ** (-0.5)
    down_w = rough(subkeys[3], (FF, D)) * FF ** (-0.5)
    gain_rows = 1.0 + 0.1 * rough(subkeys[4], (2, D))
    shift_rows = 0.3 * rough(subkeys[5], (6, D))
    up_bias = 0.3 * rough(subkeys[6], (FF,))
    return jnp.concatenate([qkv_w.reshape(-1), out_w.reshape(-1), up_w.reshape(-1), down_w.reshape(-1), gain_rows.reshape(-1), shift_rows.reshape(-1), up_bias])


def draw_params(key, part):
    stacked = []
    for layer_no in range(LAYERS):
        stacked.append(layer_vector(jax.random.fold_in(key, 17 + layer_no)))
    return jnp.stack(stacked).astype(jnp.bfloat16)


def block_sizes():
    pieces = [jnp.full((3 * D * D,), 0.15, jnp.float32), jnp.full((D * D,), 0.3, jnp.float32), jnp.full((D * FF,), 0.6, jnp.float32), jnp.full((FF * D,), 0.6, jnp.float32), jnp.full((8 * D + FF,), 0.7, jnp.float32)]
    return jnp.concatenate(pieces)


def moment_pair(key):
    base = jax.random.fold_in(key, 101)
    first_key, second_key = jax.random.split(base, 2)
    shape_of = (LAYERS, LAYER_PARAMS)
    row_total = float(CLIPS * FRAMES)
    noise = jnp.clip(jax.random.normal(first_key, shape_of, jnp.float32), -3.0, 3.0)
    log_value = jax.random.uniform(second_key, shape_of, jnp.float32, jnp.log(0.03), jnp.log(0.4))
    sizes_row = block_sizes()
    second = jnp.exp(log_value) * row_total * (sizes_row * sizes_row)[None, :]
    first = 0.8 * jnp.sqrt(second) * noise
    return (first, second)


def draw_moment_one(key, part):
    return moment_pair(key)[0].astype(jnp.float32)


def draw_moment_two(key, part):
    return moment_pair(key)[1].astype(jnp.float32)


def block_levels(rng, dims, cuts, low, largest):
    level = 1.0
    for axis_at, shards_of in cuts:
        steps = jax.random.uniform(jax.random.fold_in(jax.random.fold_in(rng, 6), axis_at), (shards_of,), jnp.float32, low / len(cuts), largest / len(cuts))
        level = level * jnp.repeat(jnp.exp(steps), dims[axis_at] // shards_of).reshape((-1,) + (1,) * (len(dims) - 1 - axis_at))
    return level


def normal_values(rng, shape, deviation, most, cuts=(), held_as=jnp.bfloat16):
    values = deviation * jax.random.normal(rng, shape, jnp.float32)
    if cuts:
        values = values * block_levels(rng, shape, cuts, -0.22, 0.18)
    return jnp.clip(values, -most, most).astype(held_as)


def setup_inputs(seed: int = 0) -> dict:
    arg_keys = jax.random.split(jax.random.key(seed), 6)
    return {
        "frames_in": normal_values(arg_keys[0], (CLIPS, FRAMES, D), 1.0, 6.0, ((0, 16), (1, 2))),
        "params": draw_params(jax.random.fold_in(arg_keys[5], 71), 0),
        "moment_one": draw_moment_one(jax.random.fold_in(arg_keys[5], 71), 0),
        "moment_two": draw_moment_two(jax.random.fold_in(arg_keys[5], 71), 0),
        "cotangent": normal_values(arg_keys[4], (CLIPS, FRAMES, D), 1.0, 6.0, ((0, 16), (1, 2))),
    }


@jax.custom_vjp
def low(v):
    return lax.optimization_barrier(v.astype(jnp.bfloat16)).astype(jnp.float32)

@jax.custom_vjp
def low_back(v):
    return v

def low_keep(v):
    return (low(v), None)

def low_pass(kept, grad):
    return (grad,)

def back_keep(v):
    return (v, None)

def back_low(kept, grad):
    return (low(grad),)
low.defvjp(low_keep, low_pass)
low_back.defvjp(back_keep, back_low)
ln_eps = 1e-05
rate = 0.01
beta_one = 0.9
beta_two = 0.95
adam_eps = 1e-08
decay = 0.1
fix_one = 1.0 - 0.9 ** 3
fix_two = 1.0 - 0.95 ** 3
highest = lax.Precision.HIGHEST

def unpack(vector):
    lengths = [D * 3 * D, D * D, D * FF, FF * D, 2 * D, 6 * D, FF]
    shapes = [(D, 3 * D), (D, D), (D, FF), (FF, D), (2, D), (6, D), (FF,)]
    pieces = []
    offset = 0
    for length, shape_of in zip(lengths, shapes):
        pieces.append(vector[offset:offset + length].reshape(shape_of))
        offset += length
    return pieces

def normalize(values, gain, shift):
    center = values - lax.optimization_barrier(jnp.mean(values, axis=-1, keepdims=True))
    spread = lax.optimization_barrier(jnp.mean(center * center, axis=-1, keepdims=True))
    return center * lax.rsqrt(spread + ln_eps) * gain + shift

def product(left, right):
    return jnp.dot(left, right, precision=highest, preferred_element_type=jnp.float32)

def encode(frames, vector):
    stream = frames
    for layer_no in range(LAYERS):
        qkv_w, out_w, up_w, down_w, gain_rows, shift_rows, up_bias = unpack(vector[layer_no])
        normed = low(normalize(stream, gain_rows[0], shift_rows[0]))
        qkv = product(normed, qkv_w)
        query_low = low(low_back(qkv[:, :D] + shift_rows[1]))
        key_low = low(low_back(qkv[:, D:2 * D]))
        value_low = low(low_back(qkv[:, 2 * D:] + shift_rows[2]))
        query_h = query_low.reshape(FRAMES, HEADS, HEAD_DIM)
        key_h = key_low.reshape(FRAMES, HEADS, HEAD_DIM)
        value_h = value_low.reshape(FRAMES, HEADS, HEAD_DIM)
        scores = low_back(jnp.einsum('qhd,khd->hqk', query_h, key_h, precision=highest) * 0.125)
        prob_low = low(jax.nn.softmax(scores, axis=-1))
        mixed = jnp.einsum('hqk,khd->qhd', prob_low, value_h, precision=highest).reshape(FRAMES, D)
        mixed = low(low_back(mixed))
        middle = stream + low_back(product(mixed, out_w) + shift_rows[3])
        normed_two = low(normalize(middle, gain_rows[1], shift_rows[4]))
        pre_act = low_back(product(normed_two, up_w) + up_bias)
        hidden_low = low(jax.nn.gelu(pre_act, approximate=False))
        stream = middle + low_back(product(hidden_low, down_w) + shift_rows[5])
    return stream

def reference(frames_in, params, moment_one, moment_two, cotangent):
    vector = params.astype(jnp.float32)

    def per_clip(grad_total, inputs):
        clip_in, clip_tangent = inputs
        output, pullback = jax.vjp(encode, clip_in.astype(jnp.float32), vector)
        clip_grad, vector_grad = pullback(clip_tangent.astype(jnp.float32))
        return (grad_total + vector_grad, (output.astype(jnp.bfloat16), clip_grad.astype(jnp.bfloat16)))
    grad_total, outputs = lax.scan(per_clip, jnp.zeros(vector.shape, jnp.float32), (frames_in, cotangent))
    encoded, frames_grad = outputs
    new_one = beta_one * moment_one + (1.0 - beta_one) * grad_total
    new_two = beta_two * moment_two + (1.0 - beta_two) * grad_total * grad_total
    step_size = new_one / fix_one / (jnp.sqrt(new_two / fix_two) + adam_eps) + decay * vector
    new_params = vector - rate * step_size
    return (encoded, frames_grad, grad_total, new_params, new_one, new_two)
```

```python
from functools import partial

import jax
import jax.numpy as jnp
from jax import lax
from jax.experimental import pallas as pl
from jax.experimental.layout import Layout, with_layout_constraint
from jax.experimental.pallas import tpu as pltpu
from jax.sharding import PartitionSpec as P

D = 384
HEADS = 6
FF = 1536
LAYERS = 2
HD = D // HEADS
LANES = 128
T_QKV, T_O, T_UP, T_DOWN = 3 * D // LANES, D // LANES, FF // LANES, D // LANES
N_QKV, N_O, N_UP, N_DOWN = D * T_QKV, D * T_O, D * T_UP, FF * T_DOWN
N_SMALL = (8 * D + FF) // LANES
N_MAIN = N_O + N_UP + N_DOWN
N_ROWS = N_QKV + N_MAIN + N_SMALL
N_HALF = N_ROWS // 2
UP_BASE, DOWN_BASE = N_O, N_O + N_UP
MESH = pl.DeviceIdType.MESH
CHUNKS = 4
VECS = 16
FB = 384
RC = 256

ln_eps = 1e-05
rate = 0.01
beta_one = 0.9
beta_two = 0.95
adam_eps = 1e-08
decay = 0.1
fix_one = 1.0 - 0.9**3
fix_two = 1.0 - 0.95**3
LOG2E = 1.4426950408889634
SCALE2 = 0.125 * LOG2E
NEG = -1e30

f32 = jnp.float32
bf16 = jnp.bfloat16


def nn(left, right):
    return lax.dot_general(left, right, (((1,), (0,)), ((), ())), preferred_element_type=f32)


def nt(left, right):
    return lax.dot_general(left, right, (((1,), (1,)), ((), ())), preferred_element_type=f32)


def tn(left, right):
    return lax.dot_general(left, right, (((0,), (0,)), ((), ())), preferred_element_type=f32)


def stats(values):
    center = values - jnp.mean(values, axis=-1, keepdims=True)
    r = lax.rsqrt(jnp.mean(center * center, axis=-1, keepdims=True) + ln_eps)
    return center * r, r


def vec(vec_ref, row):
    return vec_ref[row : row + 1, :]


G1, G2, N1, BQ, BV, BO, N2, BD, BUP = range(9)


def each_chunk(rows, body):
    @pl.loop(0, rows // RC)
    def _(i):
        body(pl.ds(pl.multiple_of(i * RC, RC), RC))


def put_row(ref, row, value):
    for j in range(value.shape[1] // LANES):
        ref[row + j : row + j + 1, :] = value[:, j * LANES : (j + 1) * LANES]


def put_flat(ref, base, stride, value):
    for j in range(value.shape[1] // LANES):
        ref[pl.ds(base + j, value.shape[0], stride=stride), :] = value[:, j * LANES : (j + 1) * LANES]


def put_up(ref, shift, block, value):
    first = N_HALF - N_QKV - UP_BASE
    for j in range(value.shape[1] // LANES):
        tile = 3 * block + j
        piece = value[:, j * LANES : (j + 1) * LANES]
        cut = -(-(first - tile) // T_UP)
        ref[pl.ds(UP_BASE + tile, cut, stride=T_UP), :] = piece[:cut, :]
        ref[pl.ds(UP_BASE + tile + T_UP * cut + shift, D - cut, stride=T_UP), :] = piece[cut:, :]


def to_low(src, base, dst, step=64):
    rows = dst.shape[0]

    @pl.loop(0, rows // step)
    def _(i):
        at = pl.multiple_of(i * step, step)
        dst[pl.ds(at, step), :] = src[pl.ds(base + at, step), :].astype(bf16)


def unpack_kernel(flat_ref, *refs):
    outs, stage = refs[:-1], refs[-1]
    flat = flat_ref.reshape(2 * N_ROWS, LANES)
    start = 0
    for which, (tiles, count) in enumerate(
        ((T_QKV, N_QKV), (T_O, N_O), (T_UP, N_UP), (T_DOWN, N_DOWN))
    ):
        base = start

        @pl.loop(0, count // 192)
        def _(i):
            stage[pl.ds(pl.multiple_of(i * 384, 384), 384), :] = flat[
                pl.ds(pl.multiple_of(2 * base + i * 384, 128), 384), :
            ].astype(f32)

        @pl.loop(0, count // tiles // 128)
        def _(i):
            for layer in range(LAYERS):
                for j in range(tiles):
                    outs[5 * layer + which][
                        pl.ds(pl.multiple_of(i * 128, 128), 128), j * LANES : (j + 1) * LANES
                    ] = stage[pl.ds(i * (256 * tiles) + 2 * j + layer, 128, stride=2 * tiles), :].astype(bf16)

        start += count
    stage[0 : 2 * N_SMALL, :] = flat[2 * start : 2 * start + 2 * N_SMALL, :].astype(f32)
    for layer in range(LAYERS):
        for i in range(N_SMALL):
            row, j = i // 3, i % 3
            outs[5 * layer + 4][row : row + 1, j * LANES : (j + 1) * LANES] = stage[
                2 * i + layer : 2 * i + layer + 1, :
            ]


def gather_weights(w_rows):
    shapes = [
        jax.ShapeDtypeStruct((D, 3 * D), bf16),
        jax.ShapeDtypeStruct((D, D), bf16),
        jax.ShapeDtypeStruct((D, FF), bf16),
        jax.ShapeDtypeStruct((FF, D), bf16),
        jax.ShapeDtypeStruct((VECS, D), f32),
    ]
    sems = pltpu.SemaphoreType.DMA((2, CHUNKS))
    outs = pl.pallas_call(
        gather_kernel,
        out_shape=shapes * 2,
        in_specs=[pl.BlockSpec(memory_space=pl.ANY)],
        scratch_shapes=[
            pltpu.VMEM((N_ROWS, LAYERS, LANES), bf16),
            pltpu.VMEM((2 * N_UP, LANES), f32),
            pltpu.SemaphoreType.DMA,
            sems,
            pltpu.SemaphoreType.DMA((2,)),
            sems,
            sems,
            sems,
        ],
        compiler_params=pltpu.CompilerParams(vmem_limit_bytes=62 << 20, collective_id=0, has_side_effects=True),
        name="gather",
    )(w_rows)
    return outs[:5], outs[5:]


def reduce_grads(ranks, half_rows, pieces):
    bits = ranks.bit_length() - 1
    total = LAYERS * CHUNKS
    h = half_rows // CHUNKS // 2
    sems = pltpu.SemaphoreType.DMA((total, 2 * bits + 2))
    return pl.pallas_call(
        partial(reduce_kernel, ranks),
        out_shape=[jax.ShapeDtypeStruct((half_rows, LANES), bf16)] * 2,
        in_specs=[pl.BlockSpec(memory_space=pl.ANY)] * 6,
        out_specs=[pl.BlockSpec(memory_space=pl.ANY)] * 2,
        scratch_shapes=[
            pltpu.VMEM((LAYERS, 2 * half_rows, LANES), bf16),
            pltpu.VMEM((LAYERS, half_rows, LANES), bf16),
            pltpu.VMEM((total, 2, h, LANES), bf16),
            pltpu.VMEM((total, h, LANES), bf16),
            pltpu.VMEM((total, h, LANES), bf16),
            pltpu.SemaphoreType.DMA((2, 3)),
            pltpu.SemaphoreType.DMA((2,)),
            sems,
            sems,
        ],
        compiler_params=pltpu.CompilerParams(vmem_limit_bytes=62 << 20, collective_id=1, has_side_effects=True),
        name="reduce",
    )(*pieces)


def call(body, shapes, scratch, name):
    return pl.pallas_call(
        body,
        out_shape=shapes,
        scratch_shapes=scratch,
        compiler_params=pltpu.CompilerParams(vmem_limit_bytes=62 << 20),
        name=name,
    )


def qkv_forward(x_ref, wqkv_ref, vec_ref, q_ref, kv_ref):
    def chunk(rows):
        xhat, _ = stats(x_ref[rows, :].astype(f32))
        a = (xhat * vec(vec_ref, G1) + vec(vec_ref, N1)).astype(bf16)
        qkv = nn(a, wqkv_ref[...])
        q_ref[rows, :] = (qkv[:, :D] + vec(vec_ref, BQ)).astype(bf16)
        kv_ref[0, rows, :] = qkv[:, D : 2 * D].astype(bf16)
        kv_ref[1, rows, :] = (qkv[:, 2 * D :] + vec(vec_ref, BV)).astype(bf16)

    each_chunk(x_ref.shape[0], chunk)


def lane_half(shape, which):
    lane = lax.broadcasted_iota(jnp.int32, shape, 1)
    return (lane < HD) if which == 0 else (lane >= HD)


def pad_mask(scores, rows):
    pad = scores.shape[0] // 2
    edge = rows // 8 * 8
    keep = lax.broadcasted_iota(jnp.int32, (pad - edge, scores.shape[1]), 0) < rows - edge
    pieces = []
    for half in range(2):
        base = half * pad
        pieces.append(scores[base : base + edge, :])
        pieces.append(jnp.where(keep, scores[base + edge : base + pad, :], NEG))
    return jnp.concatenate(pieces, axis=0)


def pair(own_ref, oth_ref, which, cols):
    return jnp.concatenate([own_ref[which, :, cols], oth_ref[which, :, cols]], axis=0)


def head_scores(keys, q_pair, t, rows):
    q_one = jnp.where(lane_half(q_pair.shape, t), q_pair, jnp.zeros_like(q_pair))
    return pad_mask(nt(keys, q_one), rows), q_one


def attend(q_ref, own_ref, oth_ref, o_t_ref, lse_ref, rows):
    pad = q_ref.shape[0]
    for hp in range(HEADS // 2):
        cols = slice(hp * LANES, (hp + 1) * LANES)

        @pl.loop(0, pad // RC)
        def _(i):
            block = pl.ds(pl.multiple_of(i * RC, RC), RC)
            keys = pair(own_ref, oth_ref, 0, cols)
            values_t = pair(own_ref, oth_ref, 1, cols).T
            q_pair = q_ref[block, cols]
            for t in range(2):
                scores, _ = head_scores(keys, q_pair, t, rows)
                top = jnp.max(scores, axis=0, keepdims=True) * SCALE2
                probs = jnp.exp2(scores * SCALE2 - top).astype(bf16)
                ones = jnp.ones((16, 2 * pad), bf16)
                mixed = nn(jnp.concatenate([values_t[t * HD : (t + 1) * HD, :], ones], axis=0), probs)
                total = mixed[HD : HD + 1, :]
                head = 2 * hp + t
                o_t_ref[head * HD : (head + 1) * HD, block] = (mixed[:HD, :] / total).astype(bf16)
                lse_ref[head : head + 1, block] = top + jnp.log(total) * LOG2E


def out_forward(x_ref, o_t_ref, wo_ref, vec_ref, h1_ref):
    def chunk(rows):
        h1_ref[rows, :] = x_ref[rows, :].astype(f32) + tn(o_t_ref[:, rows], wo_ref[...]) + vec(vec_ref, BO)

    each_chunk(x_ref.shape[0], chunk)


def second_norm(h1_ref, vec_ref, a2_ref):
    def chunk(rows):
        xhat, _ = stats(h1_ref[rows, :])
        a2_ref[rows, :] = (xhat * vec(vec_ref, G2) + vec(vec_ref, N2)).astype(bf16)

    each_chunk(h1_ref.shape[0], chunk)


def mlp_forward(h1_ref, a2_ref, wup_ref, wdown_ref, vec_ref, x_ref):
    def chunk(rows):
        total = h1_ref[rows, :] + vec(vec_ref, BD)
        for b in range(FF // FB):
            cols = slice(b * FB, (b + 1) * FB)
            u = nn(a2_ref[rows, :], wup_ref[:, cols]) + vec(vec_ref, BUP + b)
            z = (u * (0.5 + 0.5 * lax.erf(u * 0.7071067811865476))).astype(bf16)
            total = total + nn(z, wdown_ref[cols, :])
        x_ref[rows, :] = total.astype(x_ref.dtype)

    each_chunk(h1_ref.shape[0], chunk)


def norm_backward(dy, xhat, r, gain):
    dyg = dy * gain
    inner = jnp.mean(dyg, axis=-1, keepdims=True)
    cross = jnp.mean(dyg * xhat, axis=-1, keepdims=True)
    return r * (dyg - inner - xhat * cross)


def column_sum(values):
    return jnp.sum(values.astype(f32), axis=0, keepdims=True)


def mlp_backward(shift, g_ref, h1_ref, a2_ref, wup_ref, wdown_ref, vec_ref, main_ref, da2_ref, dh1_ref, enc_ref):
    rows_all = g_ref.shape[0]
    small = N_MAIN + shift
    dy2 = g_ref[...].astype(bf16)
    put_row(main_ref, small + 21, column_sum(dy2))
    for b in range(FF // FB):
        cols = slice(b * FB, (b + 1) * FB)
        u = nn(a2_ref[...], wup_ref[:, cols]) + vec(vec_ref, BUP + b)
        cdf = 0.5 + 0.5 * lax.erf(u * 0.7071067811865476)
        z = (u * cdf).astype(bf16)
        slope = cdf + u * jnp.exp2(u * u * (-0.5 * LOG2E)) * 0.3989422804014327
        if enc_ref is not None:
            part = nn(z, wdown_ref[cols, :])
            if b == 0:
                enc_ref[...] = h1_ref[...] + vec(vec_ref, BD) + part
            else:
                enc_ref[...] += part
        put_flat(main_ref, DOWN_BASE + shift + T_DOWN * FB * b, T_DOWN, tn(z, dy2))
        du = (nt(dy2, wdown_ref[cols, :]) * slope).astype(bf16)
        put_row(main_ref, small + 24 + 3 * b, column_sum(du))
        put_up(main_ref, shift, b, tn(a2_ref[...], du))
        part = nt(du, wup_ref[:, cols])
        if b == 0:
            da2_ref[...] = part
        else:
            da2_ref[...] += part
    dgain = jnp.zeros((1, D), f32)
    dshift = jnp.zeros((1, D), f32)
    for i in range(rows_all // RC):
        rows = slice(i * RC, (i + 1) * RC)
        xhat, r = stats(h1_ref[rows, :])
        dy = da2_ref[rows, :]
        dgain += column_sum(dy * xhat)
        dshift += column_sum(dy)
        dh1_ref[rows, :] = g_ref[rows, :].astype(f32) + norm_backward(dy, xhat, r, vec(vec_ref, G2))
    put_row(main_ref, small + 3, dgain)
    put_row(main_ref, small + 18, dshift)


def out_backward(shift, dh1_ref, o_t_ref, wo_ref, main_ref, do_ref, delta_ref):
    dy1 = dh1_ref[...].astype(bf16)
    put_row(main_ref, N_MAIN + shift + 15, column_sum(dy1))
    put_flat(main_ref, 0, T_O, nn(o_t_ref[...], dy1))
    do_ref[...] = nt(dy1, wo_ref[...]).astype(bf16)
    do_t = nt(wo_ref[...], dy1).astype(bf16).astype(f32)
    prod = do_t * o_t_ref[...].astype(f32)
    for h in range(HEADS):
        delta_ref[h : h + 1, :] = jnp.sum(prod[h * HD : (h + 1) * HD, :], axis=0, keepdims=True)


def attend_backward(q_ref, own_ref, oth_ref, lse_ref, do_ref, delta_ref, dq_ref, dkv_own_ref, dkv_oth_ref,
                    dq_t_ref, dk_ref, dv_ref, rows):
    pad = q_ref.shape[0]
    for hp in range(HEADS // 2):
        cols = slice(hp * LANES, (hp + 1) * LANES)
        dk_ref[...] = jnp.zeros_like(dk_ref)
        dv_ref[...] = jnp.zeros_like(dv_ref)

        @pl.loop(0, pad // RC)
        def _(i):
            block = pl.ds(pl.multiple_of(i * RC, RC), RC)
            keys = pair(own_ref, oth_ref, 0, cols)
            values = pair(own_ref, oth_ref, 1, cols)
            keys_t = keys.T
            q_pair = q_ref[block, cols]
            do_pair = do_ref[block, cols]
            for t in range(2):
                head = 2 * hp + t
                scores, q_one = head_scores(keys, q_pair, t, rows)
                do_one = jnp.where(lane_half(do_pair.shape, t), do_pair, jnp.zeros_like(do_pair))
                probs = jnp.exp2(scores * SCALE2 - lse_ref[head : head + 1, block])
                dv_ref[...] += nn(probs.astype(bf16), do_one)
                ds = (probs * (nt(values, do_one) - delta_ref[head : head + 1, block])).astype(bf16)
                dk_ref[...] += nn(ds, q_one)
                dq_t_ref[t * HD : (t + 1) * HD, block] = nn(keys_t[t * HD : (t + 1) * HD, :], ds)

        dq_ref[:, cols] = (dq_t_ref[...] * 0.125).T.astype(bf16)
        dkv_own_ref[0, :, cols] = dk_ref[:pad, :] * 0.125
        dkv_own_ref[1, :, cols] = dv_ref[:pad, :]
        dkv_oth_ref[0, :, cols] = (dk_ref[pad:, :] * 0.125).astype(bf16)
        dkv_oth_ref[1, :, cols] = dv_ref[pad:, :].astype(bf16)


def qkv_backward(shift, x_ref, dq_ref, dkv_own_ref, dkv_in_ref, dh1_ref, wqkv_ref, vec_ref, gq_ref, tail_ref,
                 a_ref, da_ref, dx_ref):
    def first(rows):
        xhat, _ = stats(x_ref[rows, :].astype(f32))
        a_ref[rows, :] = (xhat * vec(vec_ref, G1) + vec(vec_ref, N1)).astype(bf16)

    each_chunk(x_ref.shape[0], first)
    for b in range(3):
        if b == 0:
            low = dq_ref[...]
        else:
            low = (dkv_own_ref[b - 1] + dkv_in_ref[b - 1].astype(f32)).astype(bf16)
        if b == 0:
            put_row(tail_ref, shift + 9, column_sum(low))
        if b == 2:
            put_row(tail_ref, shift + 12, column_sum(low))
        put_flat(gq_ref, 3 * b, T_QKV, tn(a_ref[...], low))
        part = nt(low, wqkv_ref[:, b * D : (b + 1) * D])
        if b == 0:
            da_ref[...] = part
        else:
            da_ref[...] += part
    dgain = jnp.zeros((1, D), f32)
    dshift = jnp.zeros((1, D), f32)
    for i in range(x_ref.shape[0] // RC):
        rows = slice(i * RC, (i + 1) * RC)
        xhat, r = stats(x_ref[rows, :].astype(f32))
        dy = da_ref[rows, :]
        dgain += column_sum(dy * xhat)
        dshift += column_sum(dy)
        dx_ref[rows, :] = (dh1_ref[rows, :] + norm_backward(dy, xhat, r, vec(vec_ref, G1))).astype(dx_ref.dtype)
    put_row(tail_ref, shift + 0, dgain)
    put_row(tail_ref, shift + 6, dshift)


def kernel_b(rows, x_ref, q_ref, own_ref, oth_ref, wo, wup, wdown, vec0, wqkv1, vec1,
             o_t, lse, h1, x1, q1, kv1, a2):
    attend(q_ref, own_ref, oth_ref, o_t, lse, rows)
    out_forward(x_ref, o_t, wo, vec0, h1)
    second_norm(h1, vec0, a2)
    mlp_forward(h1, a2, wup, wdown, vec0, x1)
    qkv_forward(x1, wqkv1, vec1, q1, kv1)


def main_start(main, shift):
    edge = N_HALF - N_QKV
    main[edge : edge + shift, :] = jnp.zeros((shift, LANES), f32)
    last = N_MAIN + shift
    main[last:, :] = jnp.zeros((main.shape[0] - last, LANES), f32)


def main_end(main, main_out, tail_out):
    to_low(main, 0, main_out)
    tail_out[...] = main[N_MAIN:, :]


def kernel_c(rows, shift, x_ref, q_ref, own_ref, oth_ref, wo, wup, wdown, vec1, cot,
             enc, dq, dkv_own, dkv_oth, dh1, main_out, tail_out,
             o_t, lse, h1, a2, enc32, main, da2, do, delta, dq_t, dk, dv):
    main_start(main, shift)
    attend(q_ref, own_ref, oth_ref, o_t, lse, rows)
    out_forward(x_ref, o_t, wo, vec1, h1)
    second_norm(h1, vec1, a2)
    mlp_backward(shift, cot, h1, a2, wup, wdown, vec1, main, da2, dh1, enc32)
    enc[...] = enc32[...].astype(bf16)
    out_backward(shift, dh1, o_t, wo, main, do, delta)
    main_end(main, main_out, tail_out)
    attend_backward(q_ref, own_ref, oth_ref, lse, do, delta, dq, dkv_own, dkv_oth, dq_t, dk, dv, rows)


def kernel_d(rows, shift, x1, dq1, dkv_own1, dkv_in1, dh11, wqkv1, vec1, tail1_in,
             q0, own0, oth0, o_t, lse, h1, wo, wup, wdown, vec0,
             gq1_out, tail1_out, dq, dkv_own, dkv_oth, dh1, main_out, tail_out,
             a, dx, gq1, tail1, main, da, do, delta, dq_t, dk, dv):
    tail1[...] = tail1_in[...]
    qkv_backward(shift, x1, dq1, dkv_own1, dkv_in1, dh11, wqkv1, vec1, gq1, tail1, a, da, dx)
    to_low(gq1, 0, gq1_out)
    tail1_out[...] = tail1[...].astype(bf16)
    main_start(main, shift)
    second_norm(h1, vec0, a)
    mlp_backward(shift, dx, h1, a, wup, wdown, vec0, main, da, dh1, None)
    out_backward(shift, dh1, o_t, wo, main, do, delta)
    main_end(main, main_out, tail_out)
    attend_backward(q0, own0, oth0, lse, do, delta, dq, dkv_own, dkv_oth, dq_t, dk, dv, rows)


def kernel_e(shift, x0, dq, dkv_own, dkv_in, dh1, wqkv, vec0, tail_in, gq_out, tail_out, dx, a, da, gq, tail):
    tail[...] = tail_in[...]
    qkv_backward(shift, x0, dq, dkv_own, dkv_in, dh1, wqkv, vec0, gq, tail, a, da, dx)
    to_low(gq, 0, gq_out)
    tail_out[...] = tail[...].astype(bf16)


def remote(src, dst, send, recv, where):
    copy = pltpu.make_async_remote_copy(
        src_ref=src, dst_ref=dst, send_sem=send, recv_sem=recv, device_id=where, device_id_type=MESH
    )
    copy.start()
    return copy


def meet(partners):
    barrier = pltpu.get_barrier_semaphore()
    for where in partners:
        pl.semaphore_signal(barrier, inc=1, device_id=where, device_id_type=MESH)
    pl.semaphore_wait(barrier, len(partners))


def gather_kernel(own_ref, *refs):
    outs, (both, stage, load, x_sems, tail_sems, core_sems, y_sems, far_sems) = refs[:10], refs[10:]
    s, r = lax.axis_index("shard"), lax.axis_index("rep")
    across, core, beside = {"shard": 1 - s}, {"rep": r ^ 1}, {"rep": r ^ 2}
    quarter = N_HALF // 4
    step = quarter // CHUNKS
    filling = pltpu.make_async_copy(own_ref, both.at[pl.ds(s * N_HALF, N_HALF)], load)
    filling.start()
    meet((across, core, beside))
    filling.wait()

    def part(half, q, c):
        return both.at[pl.ds(half * N_HALF + q * quarter + c * step, step)]

    def send(half, q, c, sems, where):
        ref = part(half, q, c)
        return remote(ref, ref, sems.at[0, c], sems.at[1, c], where)

    q = r % 4
    rest = both.at[pl.ds(s * N_HALF + 4 * quarter, N_HALF - 4 * quarter)]
    xs = [send(s, q, c, x_sems, across) for c in range(CHUNKS)]
    xs.append(remote(rest, rest, tail_sems.at[0], tail_sems.at[1], across))
    cores, ys, fars = [], [], []
    for c in range(CHUNKS + 1):
        if c < CHUNKS:
            xs[c].wait_recv()
            ys.append(send(1 - s, q, c, y_sems, beside))
            cores.append(send(1 - s, q, c, core_sems, core))
        if c > 0:
            ys[c - 1].wait_recv()
            fars.append(send(1 - s, q ^ 2, c - 1, far_sems, core))
    xs[CHUNKS].wait_recv()
    for copy in cores + fars:
        copy.wait_recv()
    for copy in xs + cores + ys + fars:
        copy.wait_send()
    unpack_kernel(both, *outs, stage)


def reduce_kernel(ranks, gq0, main0, tail0, gq1, main1, tail1, out0, out1,
                  acc, res, r_core, r_x, r_rep, load, store, send_sems, recv_sems):
    s, r = lax.axis_index("shard"), lax.axis_index("rep")
    bits = ranks.bit_length() - 1
    half_rows = res.shape[1]
    loads = []
    for layer, pieces in enumerate(((gq0, main0, tail0), (gq1, main1, tail1))):
        at = 0
        for k, piece in enumerate(pieces):
            copy = pltpu.make_async_copy(
                piece, acc.at[layer, pl.ds(at, piece.shape[0])], load.at[layer, k]
            )
            copy.start()
            loads.append(copy)
            at += piece.shape[0]
    across = {"shard": 1 - s}
    peers = [{"rep": r ^ (1 << b)} for b in range(bits)]
    meet([across] + peers)
    for copy in loads:
        copy.wait()
    n = half_rows // CHUNKS
    h = n // 2
    bit = [(r >> b) & 1 for b in range(bits)]
    stages = 2 * bits + 1

    def rows(at, size):
        return pl.ds(pl.multiple_of(at, 16), size)

    def add(layer, at, recv, out, out_at):
        step = 16
        while recv.shape[0] % (2 * step) == 0 and step < 128:
            step *= 2

        @pl.loop(0, recv.shape[0] // step)
        def _(i):
            total = acc[layer, rows(at + i * step, step), :].astype(f32) + recv[rows(i * step, step), :].astype(f32)
            out[layer, rows(out_at + i * step, step), :] = total.astype(bf16)

    def offset(level):
        return bit[0] * h + sum(bit[b] * (h >> b) for b in range(1, level + 1))

    def begin(ci, stage):
        layer, c = ci // CHUNKS, ci % CHUNKS
        base = c * n
        sems = lambda k: (send_sems.at[ci, stage + k], recv_sems.at[ci, stage + k])
        if stage == 0:
            out = []
            for half in range(2):
                src = acc.at[layer, rows(half * half_rows + base + (1 - bit[0]) * h, h)]
                out.append(remote(src, r_core.at[ci, half], *sems(0 if half == 0 else stages), peers[0]))
            return out
        if stage == 1:
            src = acc.at[layer, rows((1 - s) * half_rows + base + offset(0), h)]
            return [remote(src, r_x.at[ci], *sems(0), across)]
        if stage <= bits:
            b = stage - 1
            size = h >> b
            src = acc.at[layer, rows(s * half_rows + base + offset(b - 1) + (1 - bit[b]) * size, size)]
            return [remote(src, r_rep.at[ci, rows(h - 2 * size, size)], *sems(0), peers[b])]
        b = 2 * bits - stage
        ref = res.at[layer, rows(base + offset(b), h >> b)]
        return [remote(ref, ref, *sems(0), peers[b])]

    def finish(ci, stage, copies):
        layer, c = ci // CHUNKS, ci % CHUNKS
        base = c * n
        for copy in copies:
            copy.wait_recv()
        if stage == 0:
            for half in range(2):
                at = half * half_rows + base + offset(0)
                add(layer, at, r_core.at[ci, half], acc, at)
        elif stage == 1:
            at = s * half_rows + base + offset(0)
            add(layer, at, r_x.at[ci], acc, at)
        elif stage <= bits:
            b = stage - 1
            size = h >> b
            at = s * half_rows + base + offset(b)
            recv = r_rep.at[ci, rows(h - 2 * size, size)]
            if stage < bits:
                add(layer, at, recv, acc, at)
            else:
                add(layer, at, recv, res, base + offset(b))

    total = LAYERS * CHUNKS
    flying, everything = {}, []
    for tick in range(total + stages):
        for ci in range(total):
            stage = tick - ci
            if 0 < stage <= stages:
                finish(ci, stage - 1, flying.pop(ci))
            if 0 <= stage < stages:
                flying[ci] = begin(ci, stage)
                everything += flying[ci]
    for copy in everything:
        copy.wait_send()
    outs = [pltpu.make_async_copy(res.at[k], out, store.at[k]) for k, out in enumerate((out0, out1))]
    for copy in outs:
        copy.start()
    for copy in outs:
        copy.wait()


def adam_kernel(g0_ref, g1_ref, w_ref, one_ref, two_ref, g_out, p_out, one_out, two_out, w_stage):
    block = g0_ref.shape[0]
    flat = lambda ref: ref.reshape(LAYERS * block, LANES)
    w_stage[...] = flat(w_ref)[...].astype(f32)
    for layer, g_ref in enumerate((g0_ref, g1_ref)):
        for at in range(0, block, 64):
            rows = pl.ds(LAYERS * at + layer, 64, stride=LAYERS)
            grad = g_ref[at : at + 64, :].astype(f32)
            weight = w_stage[rows, :]
            one = beta_one * flat(one_ref)[rows, :] + (1.0 - beta_one) * grad
            two = beta_two * flat(two_ref)[rows, :] + (1.0 - beta_two) * grad * grad
            step = one / fix_one / (jnp.sqrt(two / fix_two) + adam_eps) + decay * weight
            flat(g_out)[rows, :] = grad
            flat(p_out)[rows, :] = weight - rate * step
            flat(one_out)[rows, :] = one
            flat(two_out)[rows, :] = two


def to_rows(array):
    view = array.reshape(LAYERS, -1, LANES)
    return with_layout_constraint(view, Layout(major_to_minor=(1, 0, 2))).transpose(1, 0, 2)


def from_rows(array):
    view = with_layout_constraint(array.transpose(1, 0, 2), Layout(major_to_minor=(1, 0, 2)))
    return view.reshape(LAYERS, -1)


def body(ranks, frames_in, params, moment_one, moment_two, cotangent):
    rows = frames_in.shape[1]
    pad = -(-rows // RC) * RC
    unit = 16 * ranks * CHUNKS
    half_rows = -(-N_HALF // unit) * unit
    shift = half_rows - N_HALF
    tail_rows = 2 * half_rows - N_QKV - N_MAIN

    def vm(shape, dtype):
        return pltpu.VMEM(shape, dtype)

    def sd(shape, dtype):
        return jax.ShapeDtypeStruct(shape, dtype)

    swap_pairs = []
    for s in range(2):
        for r in range(ranks):
            here = s * ranks + r
            swap_pairs.append((here, here if s == r % 2 else (1 - s) * ranks + (r ^ 1)))
    partner = [(r, r ^ 1) for r in range(ranks)]

    def swap(array):
        return lax.ppermute(array, ("shard", "rep"), swap_pairs)

    def exchange(array):
        return lax.ppermute(array, "rep", partner)

    x0 = swap(jnp.pad(frames_in[0], ((0, pad - rows), (0, 0))))
    cot = swap(jnp.pad(cotangent[0], ((0, pad - rows), (0, 0))))
    w_rows = to_rows(params)
    w0, w1 = gather_weights(w_rows)
    wqkv0, wo0, wup0, wdown0, vec0 = w0
    wqkv1, wo1, wup1, wdown1, vec1 = w1

    row_b = sd((pad, D), bf16)
    kv_b = sd((2, pad, D), bf16)
    kv_f = sd((2, pad, D), f32)
    row_f = sd((pad, D), f32)
    main_b = sd((N_MAIN, LANES), bf16)
    tail_f = sd((tail_rows, LANES), f32)
    tail_b = sd((tail_rows, LANES), bf16)
    gq_b = sd((N_QKV, LANES), bf16)
    main_s = vm((N_MAIN + tail_rows, LANES), f32)
    gq_s = vm((N_QKV, LANES), f32)
    tail_s = vm((tail_rows, LANES), f32)
    lse_f = sd((8, pad), f32)
    o_t_b = sd((D, pad), bf16)
    q0, kv0 = call(qkv_forward, [row_b, kv_b], [], "qkv0")(x0, wqkv0, vec0)
    kv0_in = exchange(kv0)
    o_t0, lse0, h10, x1, q1, kv1 = call(
        partial(kernel_b, rows), [o_t_b, lse_f, row_f, row_f, row_b, kv_b], [vm((pad, D), bf16)], "forward0"
    )(x0, q0, kv0, kv0_in, wo0, wup0, wdown0, vec0, wqkv1, vec1)
    kv1_in = exchange(kv1)
    attn_scratch = [
        vm((pad, D), bf16), vm((8, pad), f32), vm((LANES, pad), f32),
        vm((2 * pad, LANES), f32), vm((2 * pad, LANES), f32),
    ]
    enc, dq1, dkv1, dkv1_oth, dh11, main1, tail1 = call(
        partial(kernel_c, rows, shift), [row_b, row_b, kv_f, kv_b, row_f, main_b, tail_f],
        [vm((D, pad), bf16), vm((8, pad), f32), vm((pad, D), f32), vm((pad, D), bf16), vm((pad, D), f32),
         main_s, vm((pad, D), f32)] + attn_scratch, "middle1",
    )(x1, q1, kv1, kv1_in, wo1, wup1, wdown1, vec1, cot)
    dkv1_in = exchange(dkv1_oth)
    encoded = swap(enc[:rows])[None]
    gq1, tail1, dq0, dkv0, dkv0_oth, dh10, main0, tail0 = call(
        partial(kernel_d, rows, shift), [gq_b, tail_b, row_b, kv_f, kv_b, row_f, main_b, tail_f],
        [vm((pad, D), bf16), vm((pad, D), f32), gq_s, tail_s, main_s, vm((pad, D), f32)] + attn_scratch,
        "backward0",
    )(x1, dq1, dkv1, dkv1_in, dh11, wqkv1, vec1, tail1, q0, kv0, kv0_in, o_t0, lse0, h10, wo0, wup0, wdown0, vec0)
    dkv0_in = exchange(dkv0_oth)
    gq0, tail0, dx = call(
        partial(kernel_e, shift), [gq_b, tail_b, row_b],
        [vm((pad, D), bf16), vm((pad, D), f32), gq_s, tail_s], "last0"
    )(x0, dq0, dkv0, dkv0_in, dh10, wqkv0, vec0, tail0)
    frames_grad = swap(dx[:rows])[None]
    g0, g1 = reduce_grads(ranks, half_rows, (gq0, main0, tail0, gq1, main1, tail1))
    block = 640
    low = pl.BlockSpec((block, LANES), lambda i: (i, 0))
    spec = pl.BlockSpec((block, 2, LANES), lambda i: (i, 0, 0))
    row_shape = sd((N_HALF, 2, LANES), f32)
    grad, new_params, new_one, new_two = pl.pallas_call(
        adam_kernel, grid=(pl.cdiv(N_HALF, block),), in_specs=[low, low, spec, spec, spec], out_specs=[spec] * 4,
        out_shape=[row_shape] * 4, scratch_shapes=[vm((2 * block, LANES), f32)],
        compiler_params=pltpu.CompilerParams(vmem_limit_bytes=62 << 20), name="adam",
    )(g0, g1, w_rows, to_rows(moment_one), to_rows(moment_two))
    return (encoded, frames_grad, from_rows(grad), from_rows(new_params), from_rows(new_one), from_rows(new_two))


def solution(mesh):
    in_specs = (
        P("rep", "shard", None),
        P(None, "shard"),
        P(None, "shard"),
        P(None, "shard"),
        P("rep", "shard", None),
    )
    out_specs = (
        P("rep", "shard", None),
        P("rep", "shard", None),
        P(None, "shard"),
        P(None, "shard"),
        P(None, "shard"),
        P(None, "shard"),
    )
    return jax.shard_map(
        partial(body, mesh.shape["rep"]), mesh=mesh, in_specs=in_specs, out_specs=out_specs, check_vma=False
    )
```

```python
from functools import partial

import jax
import jax.numpy as jnp
from jax import lax
from jax.experimental import pallas as pl
from jax.experimental.layout import Layout, with_layout_constraint
from jax.experimental.pallas import tpu as pltpu
from jax.sharding import PartitionSpec as P

D = 384
HEADS = 6
FF = 1536
LAYERS = 2
HD = D // HEADS
LANES = 128
T_QKV, T_O, T_UP, T_DOWN = 3 * D // LANES, D // LANES, FF // LANES, D // LANES
N_QKV, N_O, N_UP, N_DOWN = D * T_QKV, D * T_O, D * T_UP, FF * T_DOWN
N_SMALL = (8 * D + FF) // LANES
N_MAIN = N_O + N_UP + N_DOWN
N_ROWS = N_QKV + N_MAIN + N_SMALL
N_HALF = N_ROWS // 2
UP_BASE, DOWN_BASE = N_O, N_O + N_UP
MESH = pl.DeviceIdType.MESH
CHUNKS = 4
VECS = 16
FB = 384
RC = 256

ln_eps = 1e-05
rate = 0.01
beta_one = 0.9
beta_two = 0.95
adam_eps = 1e-08
decay = 0.1
fix_one = 1.0 - 0.9**3
fix_two = 1.0 - 0.95**3
LOG2E = 1.4426950408889634
SCALE2 = 0.125 * LOG2E
NEG = -1e30

f32 = jnp.float32
bf16 = jnp.bfloat16


def nn(left, right):
    return lax.dot_general(left, right, (((1,), (0,)), ((), ())), preferred_element_type=f32)


def nt(left, right):
    return lax.dot_general(left, right, (((1,), (1,)), ((), ())), preferred_element_type=f32)


def tn(left, right):
    return lax.dot_general(left, right, (((0,), (0,)), ((), ())), preferred_element_type=f32)


def stats(values):
    center = values - jnp.mean(values, axis=-1, keepdims=True)
    r = lax.rsqrt(jnp.mean(center * center, axis=-1, keepdims=True) + ln_eps)
    return center * r, r


def vec(vec_ref, row):
    return vec_ref[row : row + 1, :]


G1, G2, N1, BQ, BV, BO, N2, BD, BUP = range(9)


def each_chunk(rows, body):
    @pl.loop(0, rows // RC)
    def _(i):
        body(pl.ds(pl.multiple_of(i * RC, RC), RC))


def put_row(ref, row, value):
    for j in range(value.shape[1] // LANES):
        ref[row + j : row + j + 1, :] = value[:, j * LANES : (j + 1) * LANES]


def put_flat(ref, base, stride, value):
    for j in range(value.shape[1] // LANES):
        ref[pl.ds(base + j, value.shape[0], stride=stride), :] = value[:, j * LANES : (j + 1) * LANES]


def put_up(ref, shift, block, value):
    first = N_HALF - N_QKV - UP_BASE
    for j in range(value.shape[1] // LANES):
        tile = 3 * block + j
        piece = value[:, j * LANES : (j + 1) * LANES]
        cut = -(-(first - tile) // T_UP)
        ref[pl.ds(UP_BASE + tile, cut, stride=T_UP), :] = piece[:cut, :]
        ref[pl.ds(UP_BASE + tile + T_UP * cut + shift, D - cut, stride=T_UP), :] = piece[cut:, :]


def to_low(src, base, dst, at, count, step=64):
    @pl.loop(0, count // step)
    def _(i):
        dst[pl.ds(pl.multiple_of(at + i * step, 16), step), :] = src[pl.ds(base + i * step, step), :].astype(bf16)


def unpack_weights(flat, outs, stage):
    start = 0
    for which, (tiles, count) in enumerate(
        ((T_QKV, N_QKV), (T_O, N_O), (T_UP, N_UP), (T_DOWN, N_DOWN))
    ):
        base = start

        @pl.loop(0, count // 192)
        def _(i):
            stage[pl.ds(pl.multiple_of(i * 384, 384), 384), :] = flat[
                pl.ds(pl.multiple_of(2 * base + i * 384, 128), 384), :
            ].astype(f32)

        @pl.loop(0, count // tiles // 128)
        def _(i):
            for layer in range(LAYERS):
                for j in range(tiles):
                    outs[5 * layer + which][
                        pl.ds(pl.multiple_of(i * 128, 128), 128), j * LANES : (j + 1) * LANES
                    ] = stage[pl.ds(i * (256 * tiles) + 2 * j + layer, 128, stride=2 * tiles), :].astype(bf16)

        start += count
    stage[0 : 2 * N_SMALL, :] = flat[2 * start : 2 * start + 2 * N_SMALL, :].astype(f32)
    for layer in range(LAYERS):
        for i in range(N_SMALL):
            row, j = i // 3, i % 3
            outs[5 * layer + 4][row : row + 1, j * LANES : (j + 1) * LANES] = stage[
                2 * i + layer : 2 * i + layer + 1, :
            ]


def qkv_forward(x_ref, wqkv_ref, vec_ref, q_ref, kv_ref):
    def chunk(rows):
        xhat, _ = stats(x_ref[rows, :].astype(f32))
        a = (xhat * vec(vec_ref, G1) + vec(vec_ref, N1)).astype(bf16)
        qkv = nn(a, wqkv_ref[...])
        q_ref[rows, :] = (qkv[:, :D] + vec(vec_ref, BQ)).astype(bf16)
        kv_ref[0, rows, :] = qkv[:, D : 2 * D].astype(bf16)
        kv_ref[1, rows, :] = (qkv[:, 2 * D :] + vec(vec_ref, BV)).astype(bf16)

    each_chunk(x_ref.shape[0], chunk)


def lane_half(shape, which):
    lane = lax.broadcasted_iota(jnp.int32, shape, 1)
    return (lane < HD) if which == 0 else (lane >= HD)


def pad_mask(scores, rows):
    pad = scores.shape[0] // 2
    edge = rows // 8 * 8
    keep = lax.broadcasted_iota(jnp.int32, (pad - edge, scores.shape[1]), 0) < rows - edge
    pieces = []
    for half in range(2):
        base = half * pad
        pieces.append(scores[base : base + edge, :])
        pieces.append(jnp.where(keep, scores[base + edge : base + pad, :], NEG))
    return jnp.concatenate(pieces, axis=0)


def pair(own_ref, oth_ref, which, cols):
    return jnp.concatenate([own_ref[which, :, cols], oth_ref[which, :, cols]], axis=0)


def head_scores(keys, q_pair, t, rows):
    q_one = jnp.where(lane_half(q_pair.shape, t), q_pair, jnp.zeros_like(q_pair))
    return pad_mask(nt(keys, q_one), rows), q_one


def attend(q_ref, own_ref, oth_ref, o_t_ref, lse_ref, rows):
    pad = q_ref.shape[0]
    @pl.loop(0, HEADS // 2)
    def _(hp):
        cols = pl.ds(pl.multiple_of(hp * LANES, LANES), LANES)

        @pl.loop(0, pad // RC)
        def _(i):
            block = pl.ds(pl.multiple_of(i * RC, RC), RC)
            keys = pair(own_ref, oth_ref, 0, cols)
            values_t = pair(own_ref, oth_ref, 1, cols).T
            q_pair = q_ref[block, cols]
            for t in range(2):
                scores, _ = head_scores(keys, q_pair, t, rows)
                top = jnp.max(scores, axis=0, keepdims=True) * SCALE2
                probs = jnp.exp2(scores * SCALE2 - top).astype(bf16)
                ones = jnp.ones((16, 2 * pad), bf16)
                mixed = nn(jnp.concatenate([values_t[t * HD : (t + 1) * HD, :], ones], axis=0), probs)
                total = mixed[HD : HD + 1, :]
                head = 2 * hp + t
                o_t_ref[pl.ds(pl.multiple_of(head * HD, HD), HD), block] = (mixed[:HD, :] / total).astype(bf16)
                lse_ref[pl.ds(head, 1), block] = top + jnp.log(total) * LOG2E


def out_forward(x_ref, o_t_ref, wo_ref, vec_ref, h1_ref):
    def chunk(rows):
        h1_ref[rows, :] = x_ref[rows, :].astype(f32) + tn(o_t_ref[:, rows], wo_ref[...]) + vec(vec_ref, BO)

    each_chunk(x_ref.shape[0], chunk)


def second_norm(h1_ref, vec_ref, a2_ref):
    def chunk(rows):
        xhat, _ = stats(h1_ref[rows, :])
        a2_ref[rows, :] = (xhat * vec(vec_ref, G2) + vec(vec_ref, N2)).astype(bf16)

    each_chunk(h1_ref.shape[0], chunk)


def mlp_forward(h1_ref, a2_ref, wup_ref, wdown_ref, vec_ref, x_ref):
    def chunk(rows):
        total = h1_ref[rows, :] + vec(vec_ref, BD)
        for b in range(FF // FB):
            cols = slice(b * FB, (b + 1) * FB)
            u = nn(a2_ref[rows, :], wup_ref[:, cols]) + vec(vec_ref, BUP + b)
            z = (u * (0.5 + 0.5 * lax.erf(u * 0.7071067811865476))).astype(bf16)
            total = total + nn(z, wdown_ref[cols, :])
        x_ref[rows, :] = total.astype(x_ref.dtype)

    each_chunk(h1_ref.shape[0], chunk)


def norm_backward(dy, xhat, r, gain):
    dyg = dy * gain
    inner = jnp.mean(dyg, axis=-1, keepdims=True)
    cross = jnp.mean(dyg * xhat, axis=-1, keepdims=True)
    return r * (dyg - inner - xhat * cross)


def column_sum(values):
    return jnp.sum(values.astype(f32), axis=0, keepdims=True)


def mlp_backward(shift, g_ref, h1_ref, a2_ref, wup_ref, wdown_ref, vec_ref, main_ref, da2_ref, dh1_ref, enc_ref):
    rows_all = g_ref.shape[0]
    small = N_MAIN + shift
    dy2 = g_ref[...].astype(bf16)
    put_row(main_ref, small + 21, column_sum(dy2))
    da2_ref[...] = jnp.zeros_like(da2_ref)
    if enc_ref is not None:
        enc_ref[...] = h1_ref[...] + vec(vec_ref, BD)
    for b in range(FF // FB):
        cols = slice(b * FB, (b + 1) * FB)
        u = nn(a2_ref[...], wup_ref[:, cols]) + vec(vec_ref, BUP + b)
        cdf = 0.5 + 0.5 * lax.erf(u * 0.7071067811865476)
        z = (u * cdf).astype(bf16)
        slope = cdf + u * jnp.exp2(u * u * (-0.5 * LOG2E)) * 0.3989422804014327
        if enc_ref is not None:
            enc_ref[...] += nn(z, wdown_ref[cols, :])
        put_flat(main_ref, DOWN_BASE + shift + T_DOWN * FB * b, T_DOWN, tn(z, dy2))
        du = (nt(dy2, wdown_ref[cols, :]) * slope).astype(bf16)
        put_row(main_ref, small + 24 + 3 * b, column_sum(du))
        put_up(main_ref, shift, b, tn(a2_ref[...], du))
        da2_ref[...] += nt(du, wup_ref[:, cols])
    dgain = jnp.zeros((1, D), f32)
    dshift = jnp.zeros((1, D), f32)
    for i in range(rows_all // RC):
        rows = slice(i * RC, (i + 1) * RC)
        xhat, r = stats(h1_ref[rows, :])
        dy = da2_ref[rows, :]
        dgain += column_sum(dy * xhat)
        dshift += column_sum(dy)
        dh1_ref[rows, :] = g_ref[rows, :].astype(f32) + norm_backward(dy, xhat, r, vec(vec_ref, G2))
    put_row(main_ref, small + 3, dgain)
    put_row(main_ref, small + 18, dshift)


def out_backward(shift, dh1_ref, o_t_ref, wo_ref, main_ref, do_ref, delta_ref):
    dy1 = dh1_ref[...].astype(bf16)
    put_row(main_ref, N_MAIN + shift + 15, column_sum(dy1))
    put_flat(main_ref, 0, T_O, nn(o_t_ref[...], dy1))
    do_ref[...] = nt(dy1, wo_ref[...]).astype(bf16)
    do_t = nt(wo_ref[...], dy1).astype(bf16).astype(f32)
    prod = do_t * o_t_ref[...].astype(f32)
    for h in range(HEADS):
        delta_ref[h : h + 1, :] = jnp.sum(prod[h * HD : (h + 1) * HD, :], axis=0, keepdims=True)


def attend_backward(q_ref, own_ref, oth_ref, lse_ref, do_ref, delta_ref, dq_ref, dkv_own_ref, dkv_oth_ref,
                    dq_t_ref, dk_ref, dv_ref, rows, after_pair):
    pad = q_ref.shape[0]
    for hp in range(HEADS // 2):
        cols = slice(hp * LANES, (hp + 1) * LANES)
        dk_ref[...] = jnp.zeros_like(dk_ref)
        dv_ref[...] = jnp.zeros_like(dv_ref)

        @pl.loop(0, pad // RC)
        def _(i):
            block = pl.ds(pl.multiple_of(i * RC, RC), RC)
            keys = pair(own_ref, oth_ref, 0, cols)
            values = pair(own_ref, oth_ref, 1, cols)
            keys_t = keys.T
            q_pair = q_ref[block, cols]
            do_pair = do_ref[block, cols]
            for t in range(2):
                head = 2 * hp + t
                scores, q_one = head_scores(keys, q_pair, t, rows)
                do_one = jnp.where(lane_half(do_pair.shape, t), do_pair, jnp.zeros_like(do_pair))
                probs = jnp.exp2(scores * SCALE2 - lse_ref[head : head + 1, block])
                dv_ref[...] += nn(probs.astype(bf16), do_one)
                ds = (probs * (nt(values, do_one) - delta_ref[head : head + 1, block])).astype(bf16)
                dk_ref[...] += nn(ds, q_one)
                dq_t_ref[t * HD : (t + 1) * HD, block] = nn(keys_t[t * HD : (t + 1) * HD, :], ds)

        dq_ref[:, cols] = (dq_t_ref[...] * 0.125).T.astype(bf16)
        dkv_own_ref[0, :, cols] = dk_ref[:pad, :] * 0.125
        dkv_own_ref[1, :, cols] = dv_ref[:pad, :]
        dkv_oth_ref[0, :, cols] = (dk_ref[pad:, :] * 0.125).astype(bf16)
        dkv_oth_ref[1, :, cols] = dv_ref[pad:, :].astype(bf16)
        after_pair(hp)


def qkv_backward(shift, x_ref, dq_ref, dkv_own_ref, dkv_in_ref, dh1_ref, wqkv_ref, vec_ref, gq_ref, tail_ref,
                 a_ref, da_ref, dx_ref):
    def first(rows):
        xhat, _ = stats(x_ref[rows, :].astype(f32))
        a_ref[rows, :] = (xhat * vec(vec_ref, G1) + vec(vec_ref, N1)).astype(bf16)

    each_chunk(x_ref.shape[0], first)
    for b in range(3):
        if b == 0:
            low = dq_ref[...]
        else:
            low = (dkv_own_ref[b - 1] + dkv_in_ref[b - 1].astype(f32)).astype(bf16)
        if b == 0:
            put_row(tail_ref, shift + 9, column_sum(low))
        if b == 2:
            put_row(tail_ref, shift + 12, column_sum(low))
        put_flat(gq_ref, 3 * b, T_QKV, tn(a_ref[...], low))
        part = nt(low, wqkv_ref[:, b * D : (b + 1) * D])
        if b == 0:
            da_ref[...] = part
        else:
            da_ref[...] += part
    dgain = jnp.zeros((1, D), f32)
    dshift = jnp.zeros((1, D), f32)
    for i in range(x_ref.shape[0] // RC):
        rows = slice(i * RC, (i + 1) * RC)
        xhat, r = stats(x_ref[rows, :].astype(f32))
        dy = da_ref[rows, :]
        dgain += column_sum(dy * xhat)
        dshift += column_sum(dy)
        dx_ref[rows, :] = (dh1_ref[rows, :] + norm_backward(dy, xhat, r, vec(vec_ref, G1))).astype(dx_ref.dtype)
    put_row(tail_ref, shift + 0, dgain)
    put_row(tail_ref, shift + 6, dshift)


def meet(partners):
    barrier = pltpu.get_barrier_semaphore()
    for where in partners:
        pl.semaphore_signal(barrier, inc=1, device_id=where, device_id_type=MESH)
    pl.semaphore_wait(barrier, len(partners))


def to(src, dst, send, recv, where):
    return pltpu.make_async_remote_copy(
        src_ref=src, dst_ref=dst, send_sem=send, recv_sem=recv, device_id=where, device_id_type=MESH
    )


def levels_of(ranks):
    bits = ranks.bit_length() - 1
    groups = [(b, min(2, bits - b)) for b in range(2, bits, 2)]
    return [(0, 1), None, (1, 1)] + groups


def peers_of(level):
    low, count = level
    return range(1, 1 << count)


def copies_of(ranks):
    levels = levels_of(ranks)
    down = [2 if k == 0 else 1 if level is None else (1 << level[1]) - 1 for k, level in enumerate(levels)]
    up = [(1 << level[1]) - 1 for level in reversed(levels) if level is not None]
    return down, up


class Reducer:
    def __init__(self, ranks, half_rows, acc, res, landing, send_sems, recv_sems):
        self.acc, self.res, self.landing = acc, res, landing
        self.send_sems, self.recv_sems = send_sems, recv_sems
        self.half_rows = half_rows
        self.n = half_rows // CHUNKS
        self.h = self.n // 2
        self.levels = levels_of(ranks)
        self.back = [level for level in reversed(self.levels) if level is not None]
        self.stages = len(self.levels) + len(self.back)
        down, up = copies_of(ranks)
        self.counts = down + up
        self.state = {}
        self.begun = []

    def place(self):
        return lax.axis_index("shard"), lax.axis_index("rep")

    def index(self, level):
        _, r = self.place()
        return (r >> level[0]) & ((1 << level[1]) - 1)

    def size(self, upto):
        size = self.n
        for level in self.levels[: upto + 1]:
            if level is not None:
                size >>= level[1]
        return size

    def offset(self, upto):
        at = 0
        for k, level in enumerate(self.levels[: upto + 1]):
            if level is not None:
                at = at + self.index(level) * self.size(k)
        return at

    def slot(self, k, m):
        at = 0
        for i in range(k):
            count = self.counts[i]
            at += count * self.size(i)
        return at + m * self.size(k)

    def pair_rows(self, at, size):
        return pl.ds(at // 2 if isinstance(at, int) else lax.div(at, 2), size // 2)

    def acc_at(self, layer, at, size):
        return self.acc.at[self.pair_rows(layer * 2 * self.half_rows + at, size)]

    def describe(self, ci, stage):
        layer, c = ci // CHUNKS, ci % CHUNKS
        base = c * self.n
        s, r = self.place()
        first = sum(self.counts[:stage])
        out = []

        def add(src, dst, where):
            k = first + len(out)
            out.append(to(src, dst, self.send_sems.at[ci, k], self.recv_sems.at[ci, k], where))

        land = lambda k, m: self.landing.at[ci, self.pair_rows(self.slot(k, m), self.size(k))]
        if stage < len(self.levels):
            level = self.levels[stage]
            size = self.size(stage)
            if stage == 0:
                for half in range(2):
                    at = half * self.half_rows + base + (1 - self.index(level)) * size
                    add(self.acc_at(layer, at, size), land(0, half), {"rep": r ^ 1})
            elif level is None:
                at = (1 - s) * self.half_rows + base + self.offset(stage)
                add(self.acc_at(layer, at, size), land(stage, 0), {"shard": 1 - s})
            else:
                for m in peers_of(level):
                    at = s * self.half_rows + base + self.offset(stage - 1) + (self.index(level) ^ m) * size
                    add(self.acc_at(layer, at, size), land(stage, m - 1), {"rep": r ^ (m << level[0])})
        else:
            level = self.back[stage - len(self.levels)]
            k = self.levels.index(level)
            ref = self.res.at[self.pair_rows(layer * self.half_rows + base + self.offset(k), self.size(k))]
            for m in peers_of(level):
                add(ref, ref, {"rep": r ^ (m << level[0])})
        return out

    def begin(self, ci, stage):
        for copy in self.describe(ci, stage):
            copy.start()
        self.begun.append((ci, stage))

    def finish(self, ci, stage):
        layer, c = ci // CHUNKS, ci % CHUNKS
        base = c * self.n
        s, _ = self.place()
        for copy in self.describe(ci, stage):
            copy.wait_recv()
        if stage >= len(self.levels):
            return
        size = self.size(stage)
        acc = self.acc.reshape(2 * self.acc.shape[0], LANES)
        res = self.res.reshape(2 * self.res.shape[0], LANES)
        count = self.landing.shape[1] * 2
        landing = self.landing.reshape(self.landing.shape[0] * count, LANES)
        step = 16
        while size % (2 * step) == 0 and step < 128:
            step *= 2
        last = stage == len(self.levels) - 1
        jobs = []
        if stage == 0:
            for half in range(2):
                jobs.append((half * self.half_rows + base + self.offset(0), [self.slot(0, half)]))
        else:
            jobs.append((s * self.half_rows + base + self.offset(stage),
                         [self.slot(stage, m) for m in range(self.counts[stage])]))
        for at, slots in jobs:
            src = layer * 2 * self.half_rows + at
            out, out_at = acc, src
            if last:
                out, out_at = res, layer * self.half_rows + base + self.offset(stage)

            @pl.loop(0, size // step)
            def _(i):
                def rows(start):
                    return pl.ds(pl.multiple_of(start + i * step, 16), step)

                total = acc[rows(src), :].astype(f32)
                for slot in slots:
                    total = total + landing[rows(ci * count + slot), :].astype(f32)
                out[rows(out_at), :] = total.astype(bf16)

    def advance(self, chunks):
        for ci in chunks:
            stage = self.state.get(ci, -1)
            if stage >= self.stages:
                continue
            if stage >= 0:
                self.finish(ci, stage)
            stage += 1
            self.state[ci] = stage
            if stage < self.stages:
                self.begin(ci, stage)

    def drain(self):
        for ci, stage in self.begun:
            for copy in self.describe(ci, stage):
                copy.wait_send()


def step_kernel(ranks, rows, half_rows, frames, cot_in, weights, enc, frames_out, out0, out1, x0, cot,
                wqkv0, wo0, wup0, wdown0, vec0, wqkv1, wo1, wup1, wdown1, vec1,
                q0, kv0, kv0_in, o_t0, lse0, h10, x1, q1, kv1, kv1_in, o_t1, lse1, h11, a2, dx, da, dh1,
                do, delta, dq, dkv_own, dkv_oth, dkv_in, dq_t, dk, dv, main, tail, acc, res, landing,
                load, store, swap_sems, x_sems, rest_sems, core_sems, y_sems, far_sems, kv_sems, send_sems, recv_sems):
    s, r = lax.axis_index("shard"), lax.axis_index("rep")
    shift = half_rows - N_HALF
    across, core, beside = {"shard": 1 - s}, {"rep": r ^ 1}, {"rep": r ^ 2}
    diagonal = {"shard": 1 - s, "rep": r ^ 1}
    stays = s == r % 2
    filling = pltpu.make_async_copy(weights, acc.at[pl.ds(s * N_HALF, N_HALF)], load.at[0])
    filling.start()
    others = [{"rep": r ^ (m << level[0])} for level in levels_of(ranks) if level is not None for m in peers_of(level)]
    meet([diagonal, across] + others)

    def swap(src, dst, k):
        @pl.when(stays)
        def _():
            pltpu.make_async_copy(src, dst, load.at[1 + k]).start()

        @pl.when(jnp.logical_not(stays))
        def _():
            to(src, dst, swap_sems.at[0, k], swap_sems.at[1, k], diagonal).start()

    def swapped(src, dst, k):
        @pl.when(stays)
        def _():
            pltpu.make_async_copy(src, dst, load.at[1 + k]).wait()

        @pl.when(jnp.logical_not(stays))
        def _():
            to(src, dst, swap_sems.at[0, k], swap_sems.at[1, k], diagonal).wait()

    swap(frames, x0, 0)
    filling.wait()
    quarter = N_HALF // 4
    step = quarter // CHUNKS

    def send(half, q, c, sems, where):
        ref = acc.at[pl.ds(half * N_HALF + q * quarter + c * step, step)]
        copy = to(ref, ref, sems.at[0, c], sems.at[1, c], where)
        copy.start()
        return copy

    q = r % 4
    rest = acc.at[pl.ds(s * N_HALF + 4 * quarter, N_HALF - 4 * quarter)]
    xs = [send(s, q, c, x_sems, across) for c in range(CHUNKS)]
    xs.append(to(rest, rest, rest_sems.at[0], rest_sems.at[1], across))
    xs[-1].start()
    cores, ys, fars = [], [], []
    for c in range(CHUNKS + 1):
        if c < CHUNKS:
            xs[c].wait_recv()
            ys.append(send(1 - s, q, c, y_sems, beside))
            cores.append(send(1 - s, q, c, core_sems, core))
        if c > 0:
            ys[c - 1].wait_recv()
            fars.append(send(1 - s, q ^ 2, c - 1, far_sems, core))
    swap(cot_in, cot, 1)
    xs[CHUNKS].wait_recv()
    for copy in cores + fars:
        copy.wait_recv()
    for copy in xs + cores + ys + fars:
        copy.wait_send()
    outs = [wqkv0, wo0, wup0, wdown0, vec0, wqkv1, wo1, wup1, wdown1, vec1]
    flat = acc.reshape(2 * acc.shape[0], LANES)
    unpack_weights(flat, outs, main)

    exchanges = []

    def exchange(src, dst):
        k = len(exchanges)
        copy = to(src, dst, kv_sems.at[0, k], kv_sems.at[1, k], core)
        copy.start()
        exchanges.append(copy)
        return copy

    swapped(frames, x0, 0)
    qkv_forward(x0, wqkv0, vec0, q0, kv0)
    exchange(kv0, kv0_in).wait_recv()
    attend(q0, kv0, kv0_in, o_t0, lse0, rows)
    out_forward(x0, o_t0, wo0, vec0, h10)
    second_norm(h10, vec0, a2)
    mlp_forward(h10, a2, wup0, wdown0, vec0, x1)
    qkv_forward(x1, wqkv1, vec1, q1, kv1)
    exchange(kv1, kv1_in).wait_recv()
    attend(q1, kv1, kv1_in, o_t1, lse1, rows)
    out_forward(x1, o_t1, wo1, vec1, h11)
    second_norm(h11, vec1, a2)

    reducer = Reducer(ranks, half_rows, acc, res, landing, send_sems, recv_sems)
    early = [[layer * CHUNKS + c for c in range(CHUNKS // 2, CHUNKS)] for layer in range(LAYERS)]
    late = [[layer * CHUNKS + c for c in range(CHUNKS // 2)] for layer in range(LAYERS)]
    moved = (N_MAIN + shift) // 16 * 16

    def main_start():
        edge = N_HALF - N_QKV
        main[edge : edge + shift, :] = jnp.zeros((shift, LANES), f32)
        last = N_MAIN + shift
        main[last:, :] = jnp.zeros((main.shape[0] - last, LANES), f32)

    def main_end(layer):
        base = layer * 2 * half_rows
        to_low(main, 0, flat, base + N_QKV, main.shape[0])
        to_low(main, half_rows - N_QKV, flat, base + N_QKV + moved, 32, 32)
        tail[...] = main[moved : moved + 32, :]

    def late_end(layer):
        base = layer * 2 * half_rows
        to_low(main, 0, flat, base, N_QKV)
        to_low(tail, 0, flat, base + half_rows, 32, 32)

    tail_shift = N_MAIN + shift - moved
    main_start()
    swapped(cot_in, cot, 1)
    mlp_backward(shift, cot, h11, a2, wup1, wdown1, vec1, main, da, dh1, dx)
    enc[...] = dx[...].astype(bf16)
    out_backward(shift, dh1, o_t1, wo1, main, do, delta)
    main_end(1)
    reducer.advance(early[1])
    attend_backward(q1, kv1, kv1_in, lse1, do, delta, dq, dkv_own, dkv_oth, dq_t, dk, dv, rows,
                    lambda hp: reducer.advance(early[1]))
    exchange(dkv_oth, dkv_in.at[1]).wait_recv()
    qkv_backward(tail_shift, x1, dq, dkv_own, dkv_in.at[1], dh1, wqkv1, vec1, main, tail, a2, da, dx)
    late_end(1)
    reducer.advance(early[1])
    reducer.advance(late[1])
    main_start()
    second_norm(h10, vec0, a2)
    reducer.advance(late[1])
    exchanges[-1].wait_send()
    mlp_backward(shift, dx, h10, a2, wup0, wdown0, vec0, main, da, dh1, None)
    reducer.advance(early[1])
    out_backward(shift, dh1, o_t0, wo0, main, do, delta)
    main_end(0)
    reducer.advance(late[1])
    reducer.advance(early[0])
    attend_backward(q0, kv0, kv0_in, lse0, do, delta, dq, dkv_own, dkv_oth, dq_t, dk, dv, rows,
                    lambda hp: reducer.advance(early[1] + late[1] + early[0]))
    exchange(dkv_oth, dkv_in.at[0]).wait_recv()
    qkv_backward(tail_shift, x0, dq, dkv_own, dkv_in.at[0], dh1, wqkv0, vec0, main, tail, a2, da, frames_out)
    late_end(0)
    for tick in range(reducer.stages + 2):
        reducer.advance(early[1] + late[1] + early[0])
        for k, ci in enumerate(late[0]):
            if tick >= k:
                reducer.advance([ci])
    reducer.drain()
    for k, copy in enumerate(exchanges):
        if k != 2:
            copy.wait_send()

    @pl.when(s == 1)
    def _():
        out = res.reshape(2 * res.shape[0], LANES)
        for layer in range(LAYERS):
            one = pl.ds(layer * half_rows, 32)
            two = pl.ds(layer * half_rows + N_QKV + moved - half_rows, 32)
            keep = out[one, :]
            out[one, :] = out[two, :]
            out[two, :] = keep

    outs = [
        pltpu.make_async_copy(res.at[pl.ds(k * half_rows // 2, half_rows // 2)], out, store.at[k])
        for k, out in enumerate((out0, out1))
    ]
    for copy in outs:
        copy.start()
    for copy in outs:
        copy.wait()


def adam_kernel(g0_ref, g1_ref, w_ref, one_ref, two_ref, g_out, p_out, one_out, two_out, w_stage):
    block = 2 * g0_ref.shape[0]
    flat = lambda ref: ref.reshape(LAYERS * block, LANES)
    low = lambda ref: ref.reshape(block, LANES)
    w_stage[...] = flat(w_ref)[...].astype(f32)
    for layer, g_ref in enumerate((g0_ref, g1_ref)):
        for at in range(0, block, 64):
            rows = pl.ds(LAYERS * at + layer, 64, stride=LAYERS)
            grad = low(g_ref)[at : at + 64, :].astype(f32)
            weight = w_stage[rows, :]
            one = beta_one * flat(one_ref)[rows, :] + (1.0 - beta_one) * grad
            two = beta_two * flat(two_ref)[rows, :] + (1.0 - beta_two) * grad * grad
            step = one / fix_one / (jnp.sqrt(two / fix_two) + adam_eps) + decay * weight
            flat(g_out)[rows, :] = grad
            flat(p_out)[rows, :] = weight - rate * step
            flat(one_out)[rows, :] = one
            flat(two_out)[rows, :] = two


def to_rows(array):
    view = array.reshape(LAYERS, -1, LANES)
    return with_layout_constraint(view, Layout(major_to_minor=(1, 0, 2))).transpose(1, 0, 2)


def from_rows(array):
    view = with_layout_constraint(array.transpose(1, 0, 2), Layout(major_to_minor=(1, 0, 2)))
    return view.reshape(LAYERS, -1)


def body(ranks, frames_in, params, moment_one, moment_two, cotangent):
    rows = frames_in.shape[1]
    pad = -(-rows // RC) * RC

    def vm(shape, dtype):
        return pltpu.VMEM(shape, dtype)

    def sd(shape, dtype):
        return jax.ShapeDtypeStruct(shape, dtype)

    swap_pairs = []
    for s in range(2):
        for r in range(ranks):
            here = s * ranks + r
            swap_pairs.append((here, here if s == r % 2 else (1 - s) * ranks + (r ^ 1)))

    def swap(array):
        return lax.ppermute(array, ("shard", "rep"), swap_pairs)

    unit = 16 * ranks * CHUNKS
    half_rows = -(-N_HALF // unit) * unit
    tail_rows = 2 * half_rows - N_QKV - N_MAIN
    padded = lambda array: jnp.pad(array[0], ((0, pad - rows), (0, 0)))
    w_rows = to_rows(params)
    row_b = vm((pad, D), bf16)
    kv_b = vm((2, pad, D), bf16)
    kv_f = vm((2, pad, D), f32)
    row_f = vm((pad, D), f32)
    lse_f = vm((8, pad), f32)
    o_t_b = vm((D, pad), bf16)
    layer_w = [vm((D, 3 * D), bf16), vm((D, D), bf16), vm((D, FF), bf16), vm((FF, D), bf16), vm((VECS, D), f32)]
    down, up = copies_of(ranks)
    total = LAYERS * CHUNKS
    sems = pltpu.SemaphoreType.DMA((2, CHUNKS))
    chunk_sems = pltpu.SemaphoreType.DMA((total, sum(down) + sum(up)))
    anywhere = pl.BlockSpec(memory_space=pl.ANY)
    inside = pl.BlockSpec(memory_space=pltpu.VMEM)
    enc, dx, g0, g1 = pl.pallas_call(
        partial(step_kernel, ranks, rows, half_rows),
        out_shape=[sd((pad, D), bf16)] * 2 + [sd((half_rows // 2, 2, LANES), bf16)] * 2,
        in_specs=[anywhere] * 3,
        out_specs=[inside] * 2 + [anywhere] * 2,
        scratch_shapes=[row_b, row_b] + layer_w * 2
        + [row_b, kv_b, kv_b, o_t_b, lse_f, row_f, row_f, row_b, kv_b, kv_b, o_t_b, lse_f, row_f, row_b]
        + [row_f, row_f, row_f, row_b, lse_f, row_b, kv_f, kv_b, vm((2, 2, pad, D), bf16)]
        + [vm((LANES, pad), f32), vm((2 * pad, LANES), f32), vm((2 * pad, LANES), f32)]
        + [vm((N_MAIN + tail_rows, LANES), f32), vm((32, LANES), f32), vm((2 * half_rows, 2, LANES), bf16)]
        + [vm((half_rows, 2, LANES), bf16), vm((total, half_rows // CHUNKS, 2, LANES), bf16)]
        + [pltpu.SemaphoreType.DMA((3,)), pltpu.SemaphoreType.DMA((2,)), pltpu.SemaphoreType.DMA((2, 2)), sems]
        + [pltpu.SemaphoreType.DMA((2,)), sems, sems, sems, pltpu.SemaphoreType.DMA((2, 4)), chunk_sems, chunk_sems],
        compiler_params=pltpu.CompilerParams(vmem_limit_bytes=67043328, collective_id=0, has_side_effects=True),
        name="step",
    )(padded(frames_in), padded(cotangent), w_rows)
    encoded = swap(enc[:rows])[None]
    frames_grad = swap(dx[:rows])[None]
    block = 640
    low = pl.BlockSpec((block // 2, 2, LANES), lambda i: (i, 0, 0))
    spec = pl.BlockSpec((block, 2, LANES), lambda i: (i, 0, 0))
    row_shape = sd((N_HALF, 2, LANES), f32)
    grad, new_params, new_one, new_two = pl.pallas_call(
        adam_kernel, grid=(pl.cdiv(N_HALF, block),), in_specs=[low, low, spec, spec, spec], out_specs=[spec] * 4,
        out_shape=[row_shape] * 4, scratch_shapes=[vm((2 * block, LANES), f32)],
        compiler_params=pltpu.CompilerParams(vmem_limit_bytes=62 << 20), name="adam",
    )(g0, g1, w_rows, to_rows(moment_one), to_rows(moment_two))
    return (encoded, frames_grad, from_rows(grad), from_rows(new_params), from_rows(new_one), from_rows(new_two))


def solution(mesh):
    in_specs = (
        P("rep", "shard", None),
        P(None, "shard"),
        P(None, "shard"),
        P(None, "shard"),
        P("rep", "shard", None),
    )
    out_specs = (
        P("rep", "shard", None),
        P("rep", "shard", None),
        P(None, "shard"),
        P(None, "shard"),
        P(None, "shard"),
        P(None, "shard"),
    )
    return jax.shard_map(
        partial(body, mesh.shape["rep"]), mesh=mesh, in_specs=in_specs, out_specs=out_specs, check_vma=False
    )
```

```python
from functools import partial

import jax
import jax.numpy as jnp
from jax import lax
from jax.experimental import pallas as pl
from jax.experimental.layout import Layout, with_layout_constraint
from jax.experimental.pallas import tpu as pltpu
from jax.sharding import PartitionSpec as P

D = 384
HEADS = 6
FF = 1536
LAYERS = 2
HD = D // HEADS
LANES = 128
T_QKV, T_O, T_UP, T_DOWN = 3 * D // LANES, D // LANES, FF // LANES, D // LANES
N_QKV, N_O, N_UP, N_DOWN = D * T_QKV, D * T_O, D * T_UP, FF * T_DOWN
N_SMALL = (8 * D + FF) // LANES
N_MAIN = N_O + N_UP + N_DOWN
N_ROWS = N_QKV + N_MAIN + N_SMALL
N_HALF = N_ROWS // 2
UP_BASE, DOWN_BASE = N_O, N_O + N_UP
MESH = pl.DeviceIdType.MESH
CHUNKS = 4
VECS = 16
FB = 384
RC = 256

ln_eps = 1e-05
rate = 0.01
beta_one = 0.9
beta_two = 0.95
adam_eps = 1e-08
decay = 0.1
fix_one = 1.0 - 0.9**3
fix_two = 1.0 - 0.95**3
LOG2E = 1.4426950408889634
SCALE2 = 0.125 * LOG2E
NEG = -1e30

f32 = jnp.float32
bf16 = jnp.bfloat16


def nn(left, right):
    return lax.dot_general(left, right, (((1,), (0,)), ((), ())), preferred_element_type=f32)


def nt(left, right):
    return lax.dot_general(left, right, (((1,), (1,)), ((), ())), preferred_element_type=f32)


def tn(left, right):
    return lax.dot_general(left, right, (((0,), (0,)), ((), ())), preferred_element_type=f32)


def stats(values):
    center = values - jnp.mean(values, axis=-1, keepdims=True)
    r = lax.rsqrt(jnp.mean(center * center, axis=-1, keepdims=True) + ln_eps)
    return center * r, r


def vec(vec_ref, row):
    return vec_ref[row : row + 1, :]


G1, G2, N1, BQ, BV, BO, N2, BD, BUP = range(9)


def each_chunk(rows, body):
    @pl.loop(0, rows // RC)
    def _(i):
        body(pl.ds(pl.multiple_of(i * RC, RC), RC))


def put_row(ref, row, value):
    for j in range(value.shape[1] // LANES):
        ref[pl.ds(row + j, 1), :] = value[:, j * LANES : (j + 1) * LANES]


def put_flat(ref, base, stride, value):
    for j in range(value.shape[1] // LANES):
        ref[pl.ds(base + j, value.shape[0], stride=stride), :] = value[:, j * LANES : (j + 1) * LANES]


def put_up(ref, shift, block, value):
    first = N_HALF - N_QKV - UP_BASE
    whole, edge = first // T_UP, first % T_UP
    for j in range(value.shape[1] // LANES):
        tile = 3 * block + j
        piece = value[:, j * LANES : (j + 1) * LANES]
        at = UP_BASE + tile
        ref[pl.ds(at, whole, stride=T_UP), :] = piece[:whole, :]
        ref[pl.ds(at + T_UP * whole + jnp.where(tile >= edge, shift, 0), 1), :] = piece[whole : whole + 1, :]
        ref[pl.ds(at + T_UP * (whole + 1) + shift, D - whole - 1, stride=T_UP), :] = piece[whole + 1 :, :]


def to_low(src, base, dst, at, count, step=64):
    @pl.loop(0, count // step)
    def _(i):
        dst[pl.ds(pl.multiple_of(at + i * step, 16), step), :] = src[pl.ds(base + i * step, step), :].astype(bf16)


def unpack_weights(flat, outs, stage, which):
    tiles = (T_QKV, T_O, T_UP, T_DOWN)[which]
    base = (0, N_QKV, N_QKV + UP_BASE, N_QKV + DOWN_BASE)[which]
    count = (N_QKV, N_O, N_UP, N_DOWN)[which]

    @pl.loop(0, count // 192)
    def _(i):
        stage[pl.ds(pl.multiple_of(i * 384, 384), 384), :] = flat[
            pl.ds(pl.multiple_of(2 * base + i * 384, 128), 384), :
        ].astype(f32)

    @pl.loop(0, count // tiles // 128)
    def _(i):
        for layer in range(LAYERS):
            for j in range(tiles):
                outs[5 * layer + which][
                    pl.ds(pl.multiple_of(i * 128, 128), 128), j * LANES : (j + 1) * LANES
                ] = stage[pl.ds(i * (256 * tiles) + 2 * j + layer, 128, stride=2 * tiles), :].astype(bf16)


def unpack_small(flat, outs, stage):
    start = N_QKV + N_MAIN
    stage[0 : 2 * N_SMALL, :] = flat[2 * start : 2 * start + 2 * N_SMALL, :].astype(f32)
    for layer in range(LAYERS):
        for i in range(N_SMALL):
            row, j = i // 3, i % 3
            outs[5 * layer + 4][row : row + 1, j * LANES : (j + 1) * LANES] = stage[
                2 * i + layer : 2 * i + layer + 1, :
            ]


def qkv_forward(x_ref, wqkv_ref, vec_ref, q_ref, kv_ref):
    def chunk(rows):
        xhat, _ = stats(x_ref[rows, :].astype(f32))
        a = (xhat * vec(vec_ref, G1) + vec(vec_ref, N1)).astype(bf16)
        qkv = nn(a, wqkv_ref[...])
        q_ref[rows, :] = (qkv[:, :D] + vec(vec_ref, BQ)).astype(bf16)
        kv_ref[0, rows, :] = qkv[:, D : 2 * D].astype(bf16)
        kv_ref[1, rows, :] = (qkv[:, 2 * D :] + vec(vec_ref, BV)).astype(bf16)

    each_chunk(x_ref.shape[0], chunk)


def one_head(values, which):
    lane = lax.broadcasted_iota(jnp.int32, values.shape, 1) - which * HD
    return jnp.where((lane >= 0) & (lane < HD), values, jnp.zeros_like(values))


def pad_mask(scores, rows, pad=None):
    pad = scores.shape[1] if pad is None else pad
    edge = rows // 8 * 8
    keep = lax.broadcasted_iota(jnp.int32, (pad - edge, scores.shape[1]), 0) < rows - edge
    pieces = []
    for base in range(0, scores.shape[0], pad):
        pieces.append(scores[base : base + edge, :])
        pieces.append(jnp.where(keep, scores[base + edge : base + pad, :], NEG))
    return jnp.concatenate(pieces, axis=0)


def attend(q_ref, kv_ref, o_t_ref, lse_ref, values_t, rows):
    pad = q_ref.shape[0]
    values_t[LANES:, :] = jnp.ones((16, 2 * pad), bf16)

    @pl.loop(0, HEADS // 2)
    def _(hp):
        cols = pl.ds(pl.multiple_of(hp * LANES, LANES), LANES)
        values_t[:LANES, :] = jnp.concatenate([kv_ref[0, 1, :, cols], kv_ref[1, 1, :, cols]], axis=0).T

        @pl.loop(0, 2)
        def _(t):
            keys = jnp.concatenate([kv_ref[0, 0, :, cols], kv_ref[1, 0, :, cols]], axis=0)
            scores = pad_mask(nt(keys, one_head(q_ref[:, cols], t)), rows)
            top = jnp.max(scores, axis=0, keepdims=True) * SCALE2
            probs = jnp.exp2(scores * SCALE2 - top).astype(bf16)
            left = jnp.concatenate([values_t[pl.ds(pl.multiple_of(t * HD, HD), HD), :], values_t[LANES:, :]], axis=0)
            mixed = nn(left, probs)
            total = mixed[HD : HD + 1, :]
            head = 2 * hp + t
            o_t_ref[pl.ds(pl.multiple_of(head * HD, HD), HD), :] = (mixed[:HD, :] / total).astype(bf16)
            lse_ref[pl.ds(head, 1), :] = top + jnp.log(total) * LOG2E


def out_forward(x_ref, o_t_ref, wo_ref, vec_ref, h1_ref):
    def chunk(rows):
        h1_ref[rows, :] = x_ref[rows, :].astype(f32) + tn(o_t_ref[:, rows], wo_ref[...]) + vec(vec_ref, BO)

    each_chunk(x_ref.shape[0], chunk)


def second_norm(h1_ref, vec_ref, a2_ref):
    def chunk(rows):
        xhat, _ = stats(h1_ref[rows, :])
        a2_ref[rows, :] = (xhat * vec(vec_ref, G2) + vec(vec_ref, N2)).astype(bf16)

    each_chunk(h1_ref.shape[0], chunk)


def mlp_forward(h1_ref, a2_ref, wup_ref, wdown_ref, vec_ref, x_ref):
    def chunk(rows):
        total = h1_ref[rows, :] + vec(vec_ref, BD)
        for b in range(FF // FB):
            cols = slice(b * FB, (b + 1) * FB)
            u = nn(a2_ref[rows, :], wup_ref[:, cols]) + vec(vec_ref, BUP + b)
            z = (u * (0.5 + 0.5 * lax.erf(u * 0.7071067811865476))).astype(bf16)
            total = total + nn(z, wdown_ref[cols, :])
        x_ref[rows, :] = total.astype(x_ref.dtype)

    each_chunk(h1_ref.shape[0], chunk)


def norm_backward(dy, xhat, r, gain):
    dyg = dy * gain
    inner = jnp.mean(dyg, axis=-1, keepdims=True)
    cross = jnp.mean(dyg * xhat, axis=-1, keepdims=True)
    return r * (dyg - inner - xhat * cross)


def column_sum(values):
    return jnp.sum(values.astype(f32), axis=0, keepdims=True)


def mlp_backward(shift, g_ref, h1_ref, a2_ref, wup_ref, wdown_ref, vec_ref, main_ref, da2_ref, dh1_ref, enc_ref):
    rows_all = g_ref.shape[0]
    small = N_MAIN + shift
    dy2 = g_ref[...].astype(bf16)
    put_row(main_ref, small + 21, column_sum(dy2))
    da2_ref[...] = jnp.zeros_like(da2_ref)
    if enc_ref is not None:
        dh1_ref[...] = h1_ref[...] + vec(vec_ref, BD)

    @pl.loop(0, FF // FB)
    def _(b):
        cols = pl.ds(pl.multiple_of(b * FB, FB), FB)
        u = nn(a2_ref[...], wup_ref[:, cols]) + vec_ref[pl.ds(BUP + b, 1), :]
        cdf = 0.5 + 0.5 * lax.erf(u * 0.7071067811865476)
        z = (u * cdf).astype(bf16)
        slope = cdf + u * jnp.exp2(u * u * (-0.5 * LOG2E)) * 0.3989422804014327
        if enc_ref is not None:
            dh1_ref[...] += nn(z, wdown_ref[cols, :])
        put_flat(main_ref, DOWN_BASE + shift + T_DOWN * FB * b, T_DOWN, tn(z, dy2))
        du = (nt(dy2, wdown_ref[cols, :]) * slope).astype(bf16)
        put_row(main_ref, small + 24 + 3 * b, column_sum(du))
        put_up(main_ref, shift, b, tn(a2_ref[...], du))
        da2_ref[...] += nt(du, wup_ref[:, cols])

    if enc_ref is not None:
        enc_ref[...] = dh1_ref[...].astype(bf16)
    dgain = jnp.zeros((1, D), f32)
    dshift = jnp.zeros((1, D), f32)
    for i in range(rows_all // RC):
        rows = slice(i * RC, (i + 1) * RC)
        xhat, r = stats(h1_ref[rows, :])
        dy = da2_ref[rows, :]
        dgain += column_sum(dy * xhat)
        dshift += column_sum(dy)
        dh1_ref[rows, :] = g_ref[rows, :].astype(f32) + norm_backward(dy, xhat, r, vec(vec_ref, G2))
    put_row(main_ref, small + 3, dgain)
    put_row(main_ref, small + 18, dshift)


def out_backward(shift, dh1_ref, o_t_ref, wo_ref, main_ref, do_ref, delta_ref):
    dy1 = dh1_ref[...].astype(bf16)
    put_row(main_ref, N_MAIN + shift + 15, column_sum(dy1))
    put_flat(main_ref, 0, T_O, nn(o_t_ref[...], dy1))
    do_ref[...] = nt(dy1, wo_ref[...]).astype(bf16)
    do_t = nt(wo_ref[...], dy1).astype(bf16).astype(f32)
    prod = do_t * o_t_ref[...].astype(f32)
    for h in range(HEADS):
        delta_ref[h : h + 1, :] = jnp.sum(prod[h * HD : (h + 1) * HD, :], axis=0, keepdims=True)


def attend_backward(q_ref, kv_ref, lse_ref, do_ref, delta_ref, dq_ref, dkv_ref, dq_t_ref, dk_ref, dv_ref, keys_t,
                    rows, after_pair):
    for hp in range(HEADS // 2):
        cols = slice(hp * LANES, (hp + 1) * LANES)
        dq_t_ref[...] = jnp.zeros_like(dq_t_ref)

        @pl.loop(0, 2)
        def _(half):
            keys_t[...] = kv_ref[half, 0, :, cols].T
            dk_ref[...] = jnp.zeros_like(dk_ref)
            dv_ref[...] = jnp.zeros_like(dv_ref)

            @pl.loop(0, 2)
            def _(t):
                keys, values = kv_ref[half, 0, :, cols], kv_ref[half, 1, :, cols]
                head = pl.ds(2 * hp + t, 1)
                part = pl.ds(pl.multiple_of(t * HD, HD), HD)
                q_one, do_one = one_head(q_ref[:, cols], t), one_head(do_ref[:, cols], t)
                scores = pad_mask(nt(keys, q_one), rows)
                probs = jnp.exp2(scores * SCALE2 - lse_ref[head, :])
                dv_ref[...] += nn(probs.astype(bf16), do_one)
                ds = (probs * (nt(values, do_one) - delta_ref[head, :])).astype(bf16)
                dk_ref[...] += nn(ds, q_one)
                dq_t_ref[part, :] += nn(keys_t[part, :], ds) * 0.125

            dkv_ref[half, 0, :, cols] = (dk_ref[...] * 0.125).astype(bf16)
            dkv_ref[half, 1, :, cols] = dv_ref[...].astype(bf16)

        dq_ref[:, cols] = dq_t_ref[...].T.astype(bf16)
        after_pair(hp)


def qkv_backward(shift, x_ref, dq_ref, dkv_own_ref, dkv_in_ref, dh1_ref, wqkv_ref, vec_ref, gq_ref, tail_ref,
                 a_ref, da_ref, dx_ref):
    def first(rows):
        xhat, _ = stats(x_ref[rows, :].astype(f32))
        a_ref[rows, :] = (xhat * vec(vec_ref, G1) + vec(vec_ref, N1)).astype(bf16)

    each_chunk(x_ref.shape[0], first)
    for b in range(3):
        if b == 0:
            low = dq_ref[...]
        else:
            low = (dkv_own_ref[b - 1].astype(f32) + dkv_in_ref[b - 1].astype(f32)).astype(bf16)
        if b == 0:
            put_row(tail_ref, shift + 9, column_sum(low))
        if b == 2:
            put_row(tail_ref, shift + 12, column_sum(low))
        put_flat(gq_ref, 3 * b, T_QKV, tn(a_ref[...], low))
        part = nt(low, wqkv_ref[:, b * D : (b + 1) * D])
        if b == 0:
            da_ref[...] = part
        else:
            da_ref[...] += part
    dgain = jnp.zeros((1, D), f32)
    dshift = jnp.zeros((1, D), f32)
    for i in range(x_ref.shape[0] // RC):
        rows = slice(i * RC, (i + 1) * RC)
        xhat, r = stats(x_ref[rows, :].astype(f32))
        dy = da_ref[rows, :]
        dgain += column_sum(dy * xhat)
        dshift += column_sum(dy)
        dx_ref[rows, :] = (dh1_ref[rows, :] + norm_backward(dy, xhat, r, vec(vec_ref, G1))).astype(dx_ref.dtype)
    put_row(tail_ref, shift + 0, dgain)
    put_row(tail_ref, shift + 6, dshift)


def meet(partners):
    barrier = pltpu.get_barrier_semaphore()
    for where in partners:
        pl.semaphore_signal(barrier, inc=1, device_id=where, device_id_type=MESH)
    pl.semaphore_wait(barrier, len(partners))


def to(src, dst, send, recv, where):
    return pltpu.make_async_remote_copy(
        src_ref=src, dst_ref=dst, send_sem=send, recv_sem=recv, device_id=where, device_id_type=MESH
    )


def levels_of(ranks):
    bits = ranks.bit_length() - 1
    groups = [(b, min(2, bits - b)) for b in range(2, bits, 2)]
    return [(0, 1), None, (1, 1)] + groups


def peers_of(level):
    low, count = level
    return range(1, 1 << count)


def copies_of(ranks):
    levels = levels_of(ranks)
    down = [2 if k == 0 else 1 if level is None else (1 << level[1]) - 1 for k, level in enumerate(levels)]
    up = [(1 << level[1]) - 1 for level in reversed(levels) if level is not None]
    return down, up


class Reducer:
    def __init__(self, ranks, half_rows, acc, res, landing, send_sems, recv_sems):
        self.acc, self.res, self.landing = acc, res, landing
        self.send_sems, self.recv_sems = send_sems, recv_sems
        self.half_rows = half_rows
        self.n = half_rows // CHUNKS
        self.h = self.n // 2
        self.levels = levels_of(ranks)
        self.back = [level for level in reversed(self.levels) if level is not None]
        self.stages = len(self.levels) + len(self.back)
        down, up = copies_of(ranks)
        self.counts = down + up
        self.state = {}
        self.begun = []

    def place(self):
        return lax.axis_index("shard"), lax.axis_index("rep")

    def index(self, level):
        _, r = self.place()
        return (r >> level[0]) & ((1 << level[1]) - 1)

    def size(self, upto):
        size = self.n
        for level in self.levels[: upto + 1]:
            if level is not None:
                size >>= level[1]
        return size

    def offset(self, upto):
        at = 0
        for k, level in enumerate(self.levels[: upto + 1]):
            if level is not None:
                at = at + self.index(level) * self.size(k)
        return at

    def slot(self, k, m):
        at = 0
        for i in range(k):
            count = self.counts[i]
            at += count * self.size(i)
        return at + m * self.size(k)

    def pair_rows(self, at, size):
        return pl.ds(at // 2 if isinstance(at, int) else lax.div(at, 2), size // 2)

    def acc_at(self, layer, at, size):
        return self.acc.at[self.pair_rows(layer * 2 * self.half_rows + at, size)]

    def describe(self, ci, stage):
        layer, c = ci // CHUNKS, ci % CHUNKS
        base = c * self.n
        s, r = self.place()
        first = sum(self.counts[:stage])
        out = []

        def add(src, dst, where):
            k = first + len(out)
            out.append(to(src, dst, self.send_sems.at[ci, k], self.recv_sems.at[ci, k], where))

        land = lambda k, m: self.landing.at[ci, self.pair_rows(self.slot(k, m), self.size(k))]
        if stage < len(self.levels):
            level = self.levels[stage]
            size = self.size(stage)
            if stage == 0:
                for half in range(2):
                    at = half * self.half_rows + base + (1 - self.index(level)) * size
                    add(self.acc_at(layer, at, size), land(0, half), {"rep": r ^ 1})
            elif level is None:
                at = (1 - s) * self.half_rows + base + self.offset(stage)
                add(self.acc_at(layer, at, size), land(stage, 0), {"shard": 1 - s})
            else:
                for m in peers_of(level):
                    at = s * self.half_rows + base + self.offset(stage - 1) + (self.index(level) ^ m) * size
                    add(self.acc_at(layer, at, size), land(stage, m - 1), {"rep": r ^ (m << level[0])})
        else:
            level = self.back[stage - len(self.levels)]
            k = self.levels.index(level)
            ref = self.res.at[self.pair_rows(layer * self.half_rows + base + self.offset(k), self.size(k))]
            for m in peers_of(level):
                add(ref, ref, {"rep": r ^ (m << level[0])})
        return out

    def begin(self, ci, stage):
        for copy in self.describe(ci, stage):
            copy.start()
        self.begun.append((ci, stage))

    def finish(self, ci, stage):
        layer, c = ci // CHUNKS, ci % CHUNKS
        base = c * self.n
        s, _ = self.place()
        for copy in self.describe(ci, stage):
            copy.wait_recv()
        if stage >= len(self.levels):
            return
        size = self.size(stage)
        acc = self.acc.reshape(2 * self.acc.shape[0], LANES)
        res = self.res.reshape(2 * self.res.shape[0], LANES)
        count = self.landing.shape[1] * 2
        landing = self.landing.reshape(self.landing.shape[0] * count, LANES)
        step = 16
        while size % (2 * step) == 0 and step < 128:
            step *= 2
        last = stage == len(self.levels) - 1
        jobs = []
        if stage == 0:
            for half in range(2):
                jobs.append((half * self.half_rows + base + self.offset(0), [self.slot(0, half)]))
        else:
            jobs.append((s * self.half_rows + base + self.offset(stage),
                         [self.slot(stage, m) for m in range(self.counts[stage])]))
        for at, slots in jobs:
            src = layer * 2 * self.half_rows + at
            out, out_at = acc, src
            if last:
                out, out_at = res, layer * self.half_rows + base + self.offset(stage)

            @pl.loop(0, size // step)
            def _(i):
                def rows(start):
                    return pl.ds(pl.multiple_of(start + i * step, 16), step)

                total = acc[rows(src), :].astype(f32)
                for slot in slots:
                    total = total + landing[rows(ci * count + slot), :].astype(f32)
                out[rows(out_at), :] = total.astype(bf16)

    def advance(self, chunks):
        for ci in chunks:
            stage = self.state.get(ci, -1)
            if stage >= self.stages:
                continue
            if stage >= 0:
                self.finish(ci, stage)
            stage += 1
            self.state[ci] = stage
            if stage < self.stages:
                self.begin(ci, stage)

    def drain(self):
        for ci, stage in self.begun:
            for copy in self.describe(ci, stage):
                copy.wait_send()


def pad_rows(src, dst):
    rows, pad = src.shape[0], dst.shape[0]
    edge = rows // 16 * 16
    dst[:edge, :] = src[:edge, :]
    dst[edge:, :] = jnp.zeros((pad - edge, dst.shape[1]), dst.dtype)
    dst[edge:rows, :] = src[edge:, :]


def step_kernel(ranks, rows, half_rows, frames, cot_in, weights, enc_out, dx_out, out0, out1, x0, cot,
                wqkv0, wo0, wup0, wdown0, vec0, wqkv1, wo1, wup1, wdown1, vec1,
                q0, kv0, o_t0, lse0, h10, x1, q1, kv1, o_t1, lse1, h11, a2, da, dh1,
                do, delta, dq, dkv, dkv_in, dq_t, part_dk, part_dv, keys_t, values_t, enc_in, main, tail, acc, res, landing,
                load, store, swap_sems, rest_sems, hop_sems, kv_sems, send_sems, recv_sems):
    s, r = lax.axis_index("shard"), lax.axis_index("rep")
    shift = half_rows - N_HALF
    across, core, beside = {"shard": 1 - s}, {"rep": r ^ 1}, {"rep": r ^ 2}
    diagonal = {"shard": 1 - s, "rep": r ^ 1}
    stays = s == r % 2
    filling = pltpu.make_async_copy(weights, acc.at[pl.ds(s * N_HALF, N_HALF)], load.at[0])
    filling.start()
    pad_rows(frames, a2)
    pad_rows(cot_in, dq)
    others = [{"rep": r ^ (m << level[0])} for level in levels_of(ranks) if level is not None for m in peers_of(level)]
    meet([diagonal, across] + others)

    def swap(src, dst, k):
        @pl.when(stays)
        def _():
            pltpu.make_async_copy(src, dst, load.at[1 + k]).start()

        @pl.when(jnp.logical_not(stays))
        def _():
            to(src, dst, swap_sems.at[0, k], swap_sems.at[1, k], diagonal).start()

    def swapped(src, dst, k):
        @pl.when(stays)
        def _():
            pltpu.make_async_copy(src, dst, load.at[1 + k]).wait()

        @pl.when(jnp.logical_not(stays))
        def _():
            to(src, dst, swap_sems.at[0, k], swap_sems.at[1, k], diagonal).wait()

    swap(a2, x0, 0)
    filling.wait()
    q = r % 4
    first, second = N_QKV // 4, (N_HALF - N_QKV - N_SMALL) // 4
    parts = []
    for at, quarter in ((0, first), (N_QKV, second)):
        half = quarter // 2
        parts += [(at, quarter, 0, half), (at, quarter, half, quarter - half)]

    def hop(kind, c, half, which, where):
        at, quarter, start, size = parts[c]
        ref = acc.at[pl.ds(half * N_HALF + at + which * quarter + start, size)]
        return to(ref, ref, hop_sems.at[kind, 0, c], hop_sems.at[kind, 1, c], where)

    last = N_QKV + 4 * second
    rest = acc.at[pl.ds(s * N_HALF + last, N_HALF - last)]
    rests = to(rest, rest, rest_sems.at[0], rest_sems.at[1], across)
    rests.start()
    x_hops = [hop(0, c, s, q, across) for c in range(4)]
    y_hops = [hop(1, c, 1 - s, q, beside) for c in range(4)]
    core_hops = [hop(2, c, 1 - s, q, core) for c in range(4)]
    far_hops = [hop(3, c, 1 - s, q ^ 2, core) for c in range(4)]
    for copy in x_hops:
        copy.start()

    def spread(c):
        x_hops[c].wait_recv()
        y_hops[c].start()
        core_hops[c].start()

    def pass_on(c):
        y_hops[c].wait_recv()
        far_hops[c].start()

    def arrived(c):
        core_hops[c].wait_recv()
        far_hops[c].wait_recv()

    outs = [wqkv0, wo0, wup0, wdown0, vec0, wqkv1, wo1, wup1, wdown1, vec1]
    flat = acc.reshape(2 * acc.shape[0], LANES)
    rests.wait_recv()
    unpack_small(flat, outs, main)
    spread(0)
    spread(1)
    pass_on(0)
    pass_on(1)
    arrived(0)
    arrived(1)
    unpack_weights(flat, outs, main, 0)
    spread(2)

    exchanges = []

    def exchange(src, dst):
        k = len(exchanges)
        copy = to(src, dst, kv_sems.at[0, k], kv_sems.at[1, k], core)
        copy.start()
        exchanges.append(copy)
        return copy

    swapped(a2, x0, 0)
    qkv_forward(x0, wqkv0, vec0, q0, kv0.at[0])
    first_kv = exchange(kv0.at[0], kv0.at[1])
    spread(3)
    swap(dq, cot, 1)
    first_kv.wait_recv()
    attend(q0, kv0, o_t0, lse0, values_t, rows)
    pass_on(2)
    pass_on(3)
    arrived(2)
    arrived(3)
    for copy in x_hops + y_hops + core_hops + far_hops + [rests]:
        copy.wait_send()
    for which in (1, 2, 3):
        unpack_weights(flat, outs, main, which)
    out_forward(x0, o_t0, wo0, vec0, h10)
    second_norm(h10, vec0, a2)
    mlp_forward(h10, a2, wup0, wdown0, vec0, x1)
    qkv_forward(x1, wqkv1, vec1, q1, kv1.at[0])
    exchange(kv1.at[0], kv1.at[1]).wait_recv()
    attend(q1, kv1, o_t1, lse1, values_t, rows)
    out_forward(x1, o_t1, wo1, vec1, h11)
    second_norm(h11, vec1, a2)

    enc = wdown1.at[pl.ds(0, x0.shape[0])]
    reducer = Reducer(ranks, half_rows, acc, res, landing, send_sems, recv_sems)
    early = [[layer * CHUNKS + c for c in range(CHUNKS // 2, CHUNKS)] for layer in range(LAYERS)]
    late = [[layer * CHUNKS + c for c in range(CHUNKS // 2)] for layer in range(LAYERS)]
    moved = (N_MAIN + shift) // 16 * 16

    def main_start():
        edge = N_HALF - N_QKV
        main[edge : edge + shift, :] = jnp.zeros((shift, LANES), f32)
        last = N_MAIN + shift
        main[last:, :] = jnp.zeros((main.shape[0] - last, LANES), f32)

    def main_end(layer):
        base = layer * 2 * half_rows
        to_low(main, 0, flat, base + N_QKV, main.shape[0])
        to_low(main, half_rows - N_QKV, flat, base + N_QKV + moved, 32, 32)
        tail[...] = main[moved : moved + 32, :]

    def late_end(layer):
        base = layer * 2 * half_rows
        to_low(main, 0, flat, base, N_QKV)
        to_low(tail, 0, flat, base + half_rows, 32, 32)

    tail_shift = N_MAIN + shift - moved
    main_start()
    swapped(dq, cot, 1)
    mlp_backward(shift, cot, h11, a2, wup1, wdown1, vec1, main, da, dh1, enc)
    swap(enc, enc_in, 2)
    out_backward(shift, dh1, o_t1, wo1, main, do, delta)
    main_end(1)
    reducer.advance(early[1])
    attend_backward(q1, kv1, lse1, do, delta, dq, dkv, dq_t, part_dk, part_dv, keys_t, rows,
                    lambda hp: reducer.advance(early[1]))
    exchange(dkv.at[1], dkv_in).wait_recv()
    qkv_backward(tail_shift, x1, dq, dkv.at[0], dkv_in, dh1, wqkv1, vec1, main, tail, a2, da, h11)
    late_end(1)
    reducer.advance(early[1])
    reducer.advance(late[1])
    main_start()
    second_norm(h10, vec0, a2)
    reducer.advance(late[1])
    exchanges[-1].wait_send()
    mlp_backward(shift, h11, h10, a2, wup0, wdown0, vec0, main, da, dh1, None)
    reducer.advance(early[1])
    out_backward(shift, dh1, o_t0, wo0, main, do, delta)
    main_end(0)
    reducer.advance(late[1])
    reducer.advance(early[0])
    attend_backward(q0, kv0, lse0, do, delta, dq, dkv, dq_t, part_dk, part_dv, keys_t, rows,
                    lambda hp: reducer.advance(early[1] + late[1] + early[0]))
    exchange(dkv.at[1], kv1.at[1]).wait_recv()
    qkv_backward(tail_shift, x0, dq, dkv.at[0], kv1.at[1], dh1, wqkv0, vec0, main, tail, a2, da, do)
    swap(do, cot, 3)
    late_end(0)
    for tick in range(reducer.stages + 2):
        reducer.advance(early[1] + late[1] + early[0])
        for k, ci in enumerate(late[0]):
            if tick >= k:
                reducer.advance([ci])
    reducer.drain()
    for k, copy in enumerate(exchanges):
        if k != 2:
            copy.wait_send()

    @pl.when(s == 1)
    def _():
        out = res.reshape(2 * res.shape[0], LANES)
        for layer in range(LAYERS):
            one = pl.ds(layer * half_rows, 32)
            two = pl.ds(layer * half_rows + N_QKV + moved - half_rows, 32)
            keep = out[one, :]
            out[one, :] = out[two, :]
            out[two, :] = keep

    outs = [
        pltpu.make_async_copy(res.at[pl.ds(k * half_rows // 2, half_rows // 2)], out, store.at[k])
        for k, out in enumerate((out0, out1))
    ]
    for copy in outs:
        copy.start()
    swapped(enc, enc_in, 2)
    enc_out[...] = enc_in[:rows, :]
    swapped(do, cot, 3)
    dx_out[...] = cot[:rows, :]
    for copy in outs:
        copy.wait()


def adam_kernel(g0_ref, g1_ref, w_ref, one_ref, two_ref, g_out, p_out, one_out, two_out):
    block = 2 * g0_ref.shape[0]
    flat = lambda ref: ref.reshape(LAYERS * block, LANES)
    low = lambda ref: ref.reshape(block, LANES)
    for layer, g_ref in enumerate((g0_ref, g1_ref)):
        flat(g_out)[pl.ds(layer, block, stride=LAYERS), :] = low(g_ref)[...].astype(f32)

    @pl.loop(0, LAYERS * block // 128)
    def _(i):
        rows = pl.ds(pl.multiple_of(i * 128, 128), 128)
        grad = flat(g_out)[rows, :]
        weight = flat(w_ref)[rows, :].astype(f32)
        one = beta_one * flat(one_ref)[rows, :] + (1.0 - beta_one) * grad
        two = beta_two * flat(two_ref)[rows, :] + (1.0 - beta_two) * grad * grad
        step = (one * (1.0 / fix_one)) / (jnp.sqrt(two * (1.0 / fix_two)) + adam_eps) + decay * weight
        flat(p_out)[rows, :] = weight - rate * step
        flat(one_out)[rows, :] = one
        flat(two_out)[rows, :] = two


def to_rows(array):
    view = array.reshape(LAYERS, -1, LANES)
    return with_layout_constraint(view, Layout(major_to_minor=(1, 0, 2))).transpose(1, 0, 2)


def from_rows(array):
    view = with_layout_constraint(array.transpose(1, 0, 2), Layout(major_to_minor=(1, 0, 2)))
    return view.reshape(LAYERS, -1)


def body(ranks, frames_in, params, moment_one, moment_two, cotangent):
    rows = frames_in.shape[1]
    pad = -(-rows // RC) * RC

    def vm(shape, dtype):
        return pltpu.VMEM(shape, dtype)

    def sd(shape, dtype):
        return jax.ShapeDtypeStruct(shape, dtype)

    unit = 16 * ranks * CHUNKS
    half_rows = -(-N_HALF // unit) * unit
    tail_rows = -(-(half_rows - N_HALF + N_SMALL + 32) // 64) * 64
    w_rows = to_rows(params)
    row_b = vm((pad, D), bf16)
    kv_b = vm((2, pad, D), bf16)
    kv_both = vm((2, 2, pad, D), bf16)
    row_f = vm((pad, D), f32)
    lse_f = vm((8, pad), f32)
    o_t_b = vm((D, pad), bf16)
    layer_w = [vm((D, 3 * D), bf16), vm((D, D), bf16), vm((D, FF), bf16), vm((FF, D), bf16), vm((VECS, D), f32)]
    down, up = copies_of(ranks)
    total = LAYERS * CHUNKS
    chunk_sems = pltpu.SemaphoreType.DMA((total, sum(down) + sum(up)))
    anywhere = pl.BlockSpec(memory_space=pl.ANY)
    inside = pl.BlockSpec(memory_space=pltpu.VMEM)
    enc, dx, g0, g1 = pl.pallas_call(
        partial(step_kernel, ranks, rows, half_rows),
        out_shape=[sd((rows, D), bf16)] * 2 + [sd((half_rows // 2, 2, LANES), bf16)] * 2,
        in_specs=[inside, inside, anywhere],
        out_specs=[inside] * 2 + [anywhere] * 2,
        scratch_shapes=[row_b, row_b] + layer_w * 2
        + [row_b, kv_both, o_t_b, lse_f, row_f, row_f, row_b, kv_both, o_t_b, lse_f, row_f, row_b]
        + [row_f, row_f, row_b, lse_f, row_b, kv_both, kv_b]
        + [vm((LANES, pad), f32), vm((pad, LANES), f32), vm((pad, LANES), f32), vm((LANES, pad), bf16), vm((LANES + 16, 2 * pad), bf16), row_b]
        + [vm((N_MAIN + tail_rows, LANES), f32), vm((32, LANES), f32), vm((2 * half_rows, 2, LANES), bf16)]
        + [vm((half_rows, 2, LANES), bf16), vm((total, half_rows // CHUNKS, 2, LANES), bf16)]
        + [pltpu.SemaphoreType.DMA((5,)), pltpu.SemaphoreType.DMA((2,)), pltpu.SemaphoreType.DMA((2, 4))]
        + [pltpu.SemaphoreType.DMA((2,)), pltpu.SemaphoreType.DMA((4, 2, 4)), pltpu.SemaphoreType.DMA((2, 4))]
        + [chunk_sems, chunk_sems],
        compiler_params=pltpu.CompilerParams(vmem_limit_bytes=67043328, collective_id=0, has_side_effects=True),
        name="step",
    )(frames_in[0], cotangent[0], w_rows)
    encoded, frames_grad = enc[None], dx[None]
    block = 640
    low = pl.BlockSpec((block // 2, 2, LANES), lambda i: (i, 0, 0))
    spec = pl.BlockSpec((block, 2, LANES), lambda i: (i, 0, 0))
    row_shape = sd((N_HALF, 2, LANES), f32)
    grad, new_params, new_one, new_two = pl.pallas_call(
        adam_kernel, grid=(pl.cdiv(N_HALF, block),), in_specs=[low, low, spec, spec, spec], out_specs=[spec] * 4,
        out_shape=[row_shape] * 4,
        compiler_params=pltpu.CompilerParams(vmem_limit_bytes=62 << 20), name="adam",
    )(g0, g1, w_rows, to_rows(moment_one), to_rows(moment_two))
    return (encoded, frames_grad, from_rows(grad), from_rows(new_params), from_rows(new_one), from_rows(new_two))


def solution(mesh):
    in_specs = (
        P("rep", "shard", None),
        P(None, "shard"),
        P(None, "shard"),
        P(None, "shard"),
        P("rep", "shard", None),
    )
    out_specs = (
        P("rep", "shard", None),
        P("rep", "shard", None),
        P(None, "shard"),
        P(None, "shard"),
        P(None, "shard"),
        P(None, "shard"),
    )
    return jax.shard_map(
        partial(body, mesh.shape["rep"]), mesh=mesh, in_specs=in_specs, out_specs=out_specs, check_vma=False
    )
```

```python
from functools import partial

import jax
import jax.numpy as jnp
from jax import lax
from jax.experimental import pallas as pl
from jax.experimental.layout import Layout, with_layout_constraint
from jax.experimental.pallas import tpu as pltpu
from jax.sharding import PartitionSpec as P

D = 384
HEADS = 6
FF = 1536
LAYERS = 2
HD = D // HEADS
LANES = 128
T_QKV, T_O, T_UP, T_DOWN = 3 * D // LANES, D // LANES, FF // LANES, D // LANES
N_QKV, N_O, N_UP, N_DOWN = D * T_QKV, D * T_O, D * T_UP, FF * T_DOWN
N_SMALL = (8 * D + FF) // LANES
N_MAIN = N_O + N_UP + N_DOWN
N_ROWS = N_QKV + N_MAIN + N_SMALL
N_HALF = N_ROWS // 2
UP_BASE, DOWN_BASE = N_O, N_O + N_UP
MESH = pl.DeviceIdType.MESH
CHUNKS = 4
VECS = 16
FB = 384
RC = 256

ln_eps = 1e-05
rate = 0.01
beta_one = 0.9
beta_two = 0.95
adam_eps = 1e-08
decay = 0.1
fix_one = 1.0 - 0.9**3
fix_two = 1.0 - 0.95**3
LOG2E = 1.4426950408889634
SCALE2 = 0.125 * LOG2E
NEG = -1e30

f32 = jnp.float32
bf16 = jnp.bfloat16


def nn(left, right):
    return lax.dot_general(left, right, (((1,), (0,)), ((), ())), preferred_element_type=f32)


def nt(left, right):
    return lax.dot_general(left, right, (((1,), (1,)), ((), ())), preferred_element_type=f32)


def tn(left, right):
    return lax.dot_general(left, right, (((0,), (0,)), ((), ())), preferred_element_type=f32)


def stats(values):
    center = values - jnp.mean(values, axis=-1, keepdims=True)
    r = lax.rsqrt(jnp.mean(center * center, axis=-1, keepdims=True) + ln_eps)
    return center * r, r


def vec(vec_ref, row):
    return vec_ref[row : row + 1, :]


G1, G2, N1, BQ, BV, BO, N2, BD, BUP = range(9)


def each_chunk(rows, body):
    @pl.loop(0, rows // RC)
    def _(i):
        body(pl.ds(pl.multiple_of(i * RC, RC), RC))


def put_row(ref, row, value):
    for j in range(value.shape[1] // LANES):
        ref[pl.ds(row + j, 1), :] = value[:, j * LANES : (j + 1) * LANES]


def put_flat(ref, base, stride, value):
    for j in range(value.shape[1] // LANES):
        ref[pl.ds(base + j, value.shape[0], stride=stride), :] = value[:, j * LANES : (j + 1) * LANES]


def put_up(ref, shift, block, value):
    first = N_HALF - N_QKV - UP_BASE
    whole, edge = first // T_UP, first % T_UP
    for j in range(value.shape[1] // LANES):
        tile = 3 * block + j
        piece = value[:, j * LANES : (j + 1) * LANES]
        at = UP_BASE + tile
        ref[pl.ds(at, whole, stride=T_UP), :] = piece[:whole, :]
        ref[pl.ds(at + T_UP * whole + jnp.where(tile >= edge, shift, 0), 1), :] = piece[whole : whole + 1, :]
        ref[pl.ds(at + T_UP * (whole + 1) + shift, D - whole - 1, stride=T_UP), :] = piece[whole + 1 :, :]


def to_low(src, base, dst, at, count, step=64):
    @pl.loop(0, count // step)
    def _(i):
        dst[pl.ds(pl.multiple_of(at + i * step, 16), step), :] = src[pl.ds(base + i * step, step), :].astype(bf16)


def unpack_weights(flat, outs, stage, which):
    tiles = (T_QKV, T_O, T_UP, T_DOWN)[which]
    base = (0, N_QKV, N_QKV + UP_BASE, N_QKV + DOWN_BASE)[which]
    count = (N_QKV, N_O, N_UP, N_DOWN)[which]

    @pl.loop(0, count // 192)
    def _(i):
        stage[pl.ds(pl.multiple_of(i * 384, 384), 384), :] = flat[
            pl.ds(pl.multiple_of(2 * base + i * 384, 128), 384), :
        ].astype(f32)

    @pl.loop(0, count // tiles // 128)
    def _(i):
        for layer in range(LAYERS):
            for j in range(tiles):
                outs[5 * layer + which][
                    pl.ds(pl.multiple_of(i * 128, 128), 128), j * LANES : (j + 1) * LANES
                ] = stage[pl.ds(i * (256 * tiles) + 2 * j + layer, 128, stride=2 * tiles), :].astype(bf16)


def unpack_small(flat, outs, stage):
    start = N_QKV + N_MAIN
    stage[0 : 2 * N_SMALL, :] = flat[2 * start : 2 * start + 2 * N_SMALL, :].astype(f32)
    for layer in range(LAYERS):
        for i in range(N_SMALL):
            row, j = i // 3, i % 3
            outs[5 * layer + 4][row : row + 1, j * LANES : (j + 1) * LANES] = stage[
                2 * i + layer : 2 * i + layer + 1, :
            ]


def qkv_forward(x_ref, wqkv_ref, vec_ref, q_ref, kv_ref):
    def chunk(rows):
        xhat, _ = stats(x_ref[rows, :].astype(f32))
        a = (xhat * vec(vec_ref, G1) + vec(vec_ref, N1)).astype(bf16)
        qkv = nn(a, wqkv_ref[...])
        q_ref[rows, :] = (qkv[:, :D] + vec(vec_ref, BQ)).astype(bf16)
        kv_ref[0, rows, :] = qkv[:, D : 2 * D].astype(bf16)
        kv_ref[1, rows, :] = (qkv[:, 2 * D :] + vec(vec_ref, BV)).astype(bf16)

    each_chunk(x_ref.shape[0], chunk)


def one_head(values, which):
    lane = lax.broadcasted_iota(jnp.int32, values.shape, 1) - which * HD
    return jnp.where((lane >= 0) & (lane < HD), values, jnp.zeros_like(values))


def pad_mask(scores, rows, pad=None):
    pad = scores.shape[1] if pad is None else pad
    edge = rows // 8 * 8
    keep = lax.broadcasted_iota(jnp.int32, (pad - edge, scores.shape[1]), 0) < rows - edge
    pieces = []
    for base in range(0, scores.shape[0], pad):
        pieces.append(scores[base : base + edge, :])
        pieces.append(jnp.where(keep, scores[base + edge : base + pad, :], NEG))
    return jnp.concatenate(pieces, axis=0)


def attend(q_ref, kv_ref, o_t_ref, lse_ref, values_t, rows, after_pair=None):
    pad = q_ref.shape[0]
    values_t[LANES:, :] = jnp.ones((16, 2 * pad), bf16)

    @pl.loop(0, HEADS // 2)
    def _(hp):
        cols = pl.ds(pl.multiple_of(hp * LANES, LANES), LANES)
        values_t[:LANES, :] = jnp.concatenate([kv_ref[0, 1, :, cols], kv_ref[1, 1, :, cols]], axis=0).T

        @pl.loop(0, 2)
        def _(t):
            keys = jnp.concatenate([kv_ref[0, 0, :, cols], kv_ref[1, 0, :, cols]], axis=0)
            scores = pad_mask(nt(keys, one_head(q_ref[:, cols], t)), rows)
            top = jnp.max(scores, axis=0, keepdims=True) * SCALE2
            probs = jnp.exp2(scores * SCALE2 - top).astype(bf16)
            left = jnp.concatenate([values_t[pl.ds(pl.multiple_of(t * HD, HD), HD), :], values_t[LANES:, :]], axis=0)
            mixed = nn(left, probs)
            total = mixed[HD : HD + 1, :]
            head = 2 * hp + t
            o_t_ref[pl.ds(pl.multiple_of(head * HD, HD), HD), :] = (mixed[:HD, :] / total).astype(bf16)
            lse_ref[pl.ds(head, 1), :] = top + jnp.log(total) * LOG2E

        for k in range(HEADS // 2 if after_pair else 0):

            @pl.when(hp == k)
            def _():
                after_pair(k)


def out_forward(x_ref, o_t_ref, wo_ref, vec_ref, h1_ref):
    def chunk(rows):
        h1_ref[rows, :] = x_ref[rows, :].astype(f32) + tn(o_t_ref[:, rows], wo_ref[...]) + vec(vec_ref, BO)

    each_chunk(x_ref.shape[0], chunk)


def second_norm(h1_ref, vec_ref, a2_ref):
    def chunk(rows):
        xhat, _ = stats(h1_ref[rows, :])
        a2_ref[rows, :] = (xhat * vec(vec_ref, G2) + vec(vec_ref, N2)).astype(bf16)

    each_chunk(h1_ref.shape[0], chunk)


def mlp_forward(h1_ref, a2_ref, wup_ref, wdown_ref, vec_ref, x_ref):
    x_ref[...] = h1_ref[...] + vec(vec_ref, BD)

    @pl.loop(0, FF // FB)
    def _(b):
        cols = pl.ds(pl.multiple_of(b * FB, FB), FB)
        u = nn(a2_ref[...], wup_ref[:, cols]) + vec_ref[pl.ds(BUP + b, 1), :]
        z = (u * (0.5 + 0.5 * lax.erf(u * 0.7071067811865476))).astype(bf16)
        x_ref[...] += nn(z, wdown_ref[cols, :])


def norm_backward(dy, xhat, r, gain):
    dyg = dy * gain
    inner = jnp.mean(dyg, axis=-1, keepdims=True)
    cross = jnp.mean(dyg * xhat, axis=-1, keepdims=True)
    return r * (dyg - inner - xhat * cross)


def column_sum(values):
    return jnp.sum(values.astype(f32), axis=0, keepdims=True)


def mlp_backward(shift, g_ref, h1_ref, a2_ref, wup_ref, wdown_ref, vec_ref, main_ref, da2_ref, dh1_ref, enc_ref):
    rows_all = g_ref.shape[0]
    small = N_MAIN + shift
    dy2 = g_ref[...].astype(bf16)
    put_row(main_ref, small + 21, column_sum(dy2))
    da2_ref[...] = jnp.zeros_like(da2_ref)
    if enc_ref is not None:
        dh1_ref[...] = h1_ref[...] + vec(vec_ref, BD)

    @pl.loop(0, FF // FB)
    def _(b):
        cols = pl.ds(pl.multiple_of(b * FB, FB), FB)
        u = nn(a2_ref[...], wup_ref[:, cols]) + vec_ref[pl.ds(BUP + b, 1), :]
        cdf = 0.5 + 0.5 * lax.erf(u * 0.7071067811865476)
        z = (u * cdf).astype(bf16)
        slope = cdf + u * jnp.exp2(u * u * (-0.5 * LOG2E)) * 0.3989422804014327
        if enc_ref is not None:
            dh1_ref[...] += nn(z, wdown_ref[cols, :])
        put_flat(main_ref, DOWN_BASE + shift + T_DOWN * FB * b, T_DOWN, tn(z, dy2))
        du = (nt(dy2, wdown_ref[cols, :]) * slope).astype(bf16)
        put_row(main_ref, small + 24 + 3 * b, column_sum(du))
        put_up(main_ref, shift, b, tn(a2_ref[...], du))
        da2_ref[...] += nt(du, wup_ref[:, cols])

    if enc_ref is not None:
        enc_ref[...] = dh1_ref[...].astype(bf16)
    dgain = jnp.zeros((1, D), f32)
    dshift = jnp.zeros((1, D), f32)
    for i in range(rows_all // RC):
        rows = slice(i * RC, (i + 1) * RC)
        xhat, r = stats(h1_ref[rows, :])
        dy = da2_ref[rows, :]
        dgain += column_sum(dy * xhat)
        dshift += column_sum(dy)
        dh1_ref[rows, :] = g_ref[rows, :].astype(f32) + norm_backward(dy, xhat, r, vec(vec_ref, G2))
    put_row(main_ref, small + 3, dgain)
    put_row(main_ref, small + 18, dshift)


def out_backward(shift, dh1_ref, o_t_ref, wo_ref, main_ref, do_ref, delta_ref):
    dy1 = dh1_ref[...].astype(bf16)
    put_row(main_ref, N_MAIN + shift + 15, column_sum(dy1))
    put_flat(main_ref, 0, T_O, nn(o_t_ref[...], dy1))
    do_ref[...] = nt(dy1, wo_ref[...]).astype(bf16)
    do_t = nt(wo_ref[...], dy1).astype(bf16).astype(f32)
    prod = do_t * o_t_ref[...].astype(f32)
    for h in range(HEADS):
        delta_ref[h : h + 1, :] = jnp.sum(prod[h * HD : (h + 1) * HD, :], axis=0, keepdims=True)


def attend_backward(q_ref, kv_ref, lse_ref, do_ref, delta_ref, dqkv_ref, dkv_oth_ref, dq_t_ref, rows, after_pair):
    @pl.loop(0, HEADS // 2)
    def _(hp):
        cols = pl.ds(pl.multiple_of(hp * LANES, LANES), LANES)
        for half in range(2):
            keys, values = kv_ref[half, 0, :, cols], kv_ref[half, 1, :, cols]
            keys_t = keys.T
            dk = dv = 0.0
            for t in range(2):
                head = pl.ds(2 * hp + t, 1)
                part = slice(t * HD, (t + 1) * HD)
                q_one, do_one = one_head(q_ref[:, cols], t), one_head(do_ref[:, cols], t)
                scores = pad_mask(nt(keys, q_one), rows)
                probs = jnp.exp2(scores * SCALE2 - lse_ref[head, :])
                dv += nn(probs.astype(bf16), do_one)
                ds = (probs * (nt(values, do_one) - delta_ref[head, :])).astype(bf16)
                dk += nn(ds, q_one)
                dq_part = nn(keys_t[part, :], ds) * 0.125
                if half == 0:
                    dq_t_ref[part, :] = dq_part
                else:
                    dq_t_ref[part, :] += dq_part
            dst = (dqkv_ref.at[pl.ds(1, 2)], dkv_oth_ref)[half]
            dst[0, :, cols] = (dk * 0.125).astype(bf16)
            dst[1, :, cols] = dv.astype(bf16)
        dqkv_ref[0, :, cols] = dq_t_ref[...].T.astype(bf16)
        for k in range(HEADS // 2):

            @pl.when(hp == k)
            def _():
                after_pair(k)


def qkv_backward(shift, x_ref, dqkv_ref, dkv_in_ref, dh1_ref, wqkv_ref, vec_ref, gq_ref, tail_ref,
                 a_ref, da_ref, dx_ref, after_blocks):
    def first(rows):
        xhat, _ = stats(x_ref[rows, :].astype(f32))
        a_ref[rows, :] = (xhat * vec(vec_ref, G1) + vec(vec_ref, N1)).astype(bf16)
        for b in range(2):
            total = dqkv_ref[b + 1, rows, :].astype(f32) + dkv_in_ref[b, rows, :].astype(f32)
            dqkv_ref[b + 1, rows, :] = total.astype(bf16)

    each_chunk(x_ref.shape[0], first)
    da_ref[...] = jnp.zeros_like(da_ref)

    @pl.loop(0, 3)
    def _(b):
        low = dqkv_ref[b]

        @pl.when(b != 1)
        def _():
            put_row(tail_ref, shift + 9 + jnp.where(b == 2, 3, 0), column_sum(low))

        put_flat(gq_ref, 3 * b, T_QKV, tn(a_ref[...], low))
        da_ref[...] += nt(low, wqkv_ref[:, pl.ds(pl.multiple_of(b * D, D), D)])

    after_blocks()
    dgain = jnp.zeros((1, D), f32)
    dshift = jnp.zeros((1, D), f32)
    for i in range(x_ref.shape[0] // RC):
        rows = slice(i * RC, (i + 1) * RC)
        xhat, r = stats(x_ref[rows, :].astype(f32))
        dy = da_ref[rows, :]
        dgain += column_sum(dy * xhat)
        dshift += column_sum(dy)
        dx_ref[rows, :] = (dh1_ref[rows, :] + norm_backward(dy, xhat, r, vec(vec_ref, G1))).astype(dx_ref.dtype)
    put_row(tail_ref, shift + 0, dgain)
    put_row(tail_ref, shift + 6, dshift)


def greet(partners):
    for where in partners:
        pl.semaphore_signal(pltpu.get_barrier_semaphore(), inc=1, device_id=where, device_id_type=MESH)


def to(src, dst, send, recv, where):
    return pltpu.make_async_remote_copy(
        src_ref=src, dst_ref=dst, send_sem=send, recv_sem=recv, device_id=where, device_id_type=MESH
    )


def levels_of(ranks, late_x=False):
    bits = ranks.bit_length() - 1
    groups = [(b, min(2, bits - b)) for b in range(2, bits, 2)]
    return [(0, 1), (1, 1), None] + groups if late_x else [(0, 1), None, (1, 1)] + groups


def peers_of(level):
    low, count = level
    return range(1, 1 << count)


def copies_of(levels):
    crossing = levels.index(None)
    down = []
    for k, level in enumerate(levels):
        down.append(1 if level is None else ((1 << level[1]) - 1) * (2 if k < crossing else 1))
    up = [(1 << level[1]) - 1 for level in reversed(levels) if level is not None]
    return down, up


class Reducer:
    def __init__(self, ranks, half_rows, acc, res, landing, send_sems, recv_sems):
        self.acc, self.res, self.landing = acc, res, landing
        self.send_sems, self.recv_sems = send_sems, recv_sems
        self.half_rows = half_rows
        self.n = half_rows // CHUNKS
        self.orders = [levels_of(ranks), levels_of(ranks, True)]
        self.stages = 2 * len(self.orders[0]) - 1
        self.state = {}
        self.begun = []

    def plan(self, ci):
        levels = self.orders[ci % 2]
        down, up = copies_of(levels)
        return levels, down + up

    def place(self):
        return lax.axis_index("shard"), lax.axis_index("rep")

    def index(self, level):
        _, r = self.place()
        return (r >> level[0]) & ((1 << level[1]) - 1)

    def size(self, levels, upto):
        size = self.n
        for level in levels[: upto + 1]:
            if level is not None:
                size >>= level[1]
        return size

    def offset(self, levels, upto):
        at = 0
        for k, level in enumerate(levels[: upto + 1]):
            if level is not None:
                at = at + self.index(level) * self.size(levels, k)
        return at

    def slot(self, ci, k, m):
        levels, counts = self.plan(ci)
        return sum(counts[i] * self.size(levels, i) for i in range(k)) + m * self.size(levels, k)

    def pair_rows(self, at, size):
        return pl.ds(at // 2 if isinstance(at, int) else lax.div(at, 2), size // 2)

    def describe(self, ci, stage):
        layer, base = ci // CHUNKS, ci % CHUNKS * self.n
        levels, counts = self.plan(ci)
        s, r = self.place()
        first = sum(counts[:stage])
        out = []

        def add(src, dst, where):
            k = first + len(out)
            out.append(to(src, dst, self.send_sems.at[ci, k], self.recv_sems.at[ci, k], where))

        def send(half, at, size, where):
            rows = self.pair_rows((layer * 2 + half) * self.half_rows + base + at, size)
            add(self.acc.at[rows], self.landing.at[ci, self.pair_rows(self.slot(ci, stage, len(out)), size)], where)

        if stage < len(levels):
            level, size = levels[stage], self.size(levels, stage)
            if level is None:
                send(1 - s, self.offset(levels, stage), size, {"shard": 1 - s})
            else:
                for half in range(2) if stage < levels.index(None) else (s,):
                    for m in peers_of(level):
                        at = self.offset(levels, stage - 1) + (self.index(level) ^ m) * size
                        send(half, at, size, {"rep": r ^ (m << level[0])})
        else:
            level = [one for one in reversed(levels) if one is not None][stage - len(levels)]
            k = levels.index(level)
            at = layer * self.half_rows + base + self.offset(levels, k)
            ref = self.res.at[self.pair_rows(at, self.size(levels, k))]
            for m in peers_of(level):
                add(ref, ref, {"rep": r ^ (m << level[0])})
        return out

    def begin(self, ci, stage):
        for copy in self.describe(ci, stage):
            copy.start()
        self.begun.append((ci, stage))

    def finish(self, ci, stage):
        layer, base = ci // CHUNKS, ci % CHUNKS * self.n
        levels, counts = self.plan(ci)
        s, _ = self.place()
        for copy in self.describe(ci, stage):
            copy.wait_recv()
        if stage >= len(levels):
            return
        size = self.size(levels, stage)
        acc = self.acc.reshape(2 * self.acc.shape[0], LANES)
        res = self.res.reshape(2 * self.res.shape[0], LANES)
        count = self.landing.shape[1] * 2
        landing = self.landing.reshape(self.landing.shape[0] * count, LANES)
        step = 16
        while size % (2 * step) == 0 and step < 128:
            step *= 2
        halves = (0, 1) if stage < levels.index(None) else (s,)
        each = counts[stage] // len(halves)
        for k, half in enumerate(halves):
            slots = [self.slot(ci, stage, k * each + m) for m in range(each)]
            src = (layer * 2 + half) * self.half_rows + base + self.offset(levels, stage)
            out, out_at = acc, src
            if stage == len(levels) - 1:
                out, out_at = res, layer * self.half_rows + base + self.offset(levels, stage)

            @pl.loop(0, size // step)
            def _(i):
                def rows(start):
                    return pl.ds(pl.multiple_of(start + i * step, 16), step)

                total = acc[rows(src), :].astype(f32)
                for slot in slots:
                    total = total + landing[rows(ci * count + slot), :].astype(f32)
                out[rows(out_at), :] = total.astype(bf16)

    def advance(self, chunks):
        for ci in chunks:
            stage = self.state.get(ci, -1)
            if stage >= self.stages:
                continue
            if stage >= 0:
                self.finish(ci, stage)
            stage += 1
            self.state[ci] = stage
            if stage < self.stages:
                self.begin(ci, stage)

    def drain(self):
        for ci, stage in self.begun:
            for copy in self.describe(ci, stage):
                copy.wait_send()


def pad_rows(src, dst):
    rows, pad = src.shape[0], dst.shape[0]
    edge = rows // 16 * 16
    dst[:edge, :] = src[:edge, :]
    dst[edge:, :] = jnp.zeros((pad - edge, dst.shape[1]), dst.dtype)
    dst[edge:rows, :] = src[edge:, :]


def step_kernel(ranks, rows, half_rows, frames, cot_in, weights, enc_out, dx_out, out0, out1, x0, cot,
                wqkv0, wo0, wup0, wdown0, vec0, wqkv1, wo1, wup1, wdown1, vec1,
                q0, kv0, o_t0, lse0, h10, x1, q1, kv1, o_t1, lse1, h11, a2, da, dh1,
                do, delta, dq, dqkv, dkv_oth, dkv_in, dq_t, values_t, enc_in, main, tail, acc, res, landing,
                load, store, swap_sems, relay_sems, rest_sems, hop_sems, kv_sems, send_sems, recv_sems):
    s, r = lax.axis_index("shard"), lax.axis_index("rep")
    shift = half_rows - N_HALF
    across, core, beside = {"shard": 1 - s}, {"rep": r ^ 1}, {"rep": r ^ 2}
    diagonal = {"shard": 1 - s, "rep": r ^ 1}
    stays = s == r % 2
    filling = pltpu.make_async_copy(weights, acc.at[pl.ds(s * N_HALF, N_HALF)], load.at[0])
    filling.start()
    partners = [{"rep": r ^ (m << level[0])} for level in levels_of(ranks) if level is not None for m in peers_of(level)]
    partners += [diagonal, across]
    greet(partners)
    outs = [wqkv0, wo0, wup0, wdown0, vec0, wqkv1, wo1, wup1, wdown1, vec1]
    flat = acc.reshape(2 * acc.shape[0], LANES)
    pad_rows(frames, a2)
    pad_rows(cot_in, dq)
    filling.wait()

    @pl.when(s == 0)
    def _():
        unpack_weights(flat, outs, main, 0)

    pl.semaphore_wait(pltpu.get_barrier_semaphore(), len(partners))

    def swap(src, dst, k):
        @pl.when(stays)
        def _():
            pltpu.make_async_copy(src, dst, load.at[1 + k]).start()

        @pl.when(jnp.logical_not(stays))
        def _():
            to(src, dst, swap_sems.at[0, k], swap_sems.at[1, k], diagonal).start()

    def swapped(src, dst, k):
        @pl.when(stays)
        def _():
            pltpu.make_async_copy(src, dst, load.at[1 + k]).wait()

        @pl.when(jnp.logical_not(stays))
        def _():
            to(src, dst, swap_sems.at[0, k], swap_sems.at[1, k], diagonal).wait()

    q = r % 4
    second = (N_HALF - N_QKV - N_SMALL) // 4
    last = N_QKV + 4 * second
    part = D // 4

    def flow(kind, c, which):
        return (hop_sems.at[kind, 0, c], hop_sems.at[kind, 1, c], (across, beside, core, core)[kind])

    def wide(c, which):
        w, start, size = ((wqkv0, 0, part // 2), (wqkv0, part // 2, part // 2), (wqkv1, 0, part))[c]
        return w.at[pl.ds(pl.multiple_of(which * part + start, 16), size), :]

    def units(c, which, half):
        at, quarter, start, size = (
            (N_QKV, second, 0, second // 2),
            (N_QKV, second, second // 2, second - second // 2),
            (0, N_QKV // 4, 0, N_QKV // 8),
            (0, N_QKV // 4, N_QKV // 8, N_QKV // 8),
        )[c - 3]
        return acc.at[pl.ds(half * N_HALF + at + which * quarter + start, size)]

    def hop(kind, c):
        which = q ^ 2 if kind == 3 else q
        half = s if kind == 0 else 1 - s
        ref = wide(c, which) if c < 3 else units(c, which, half)
        return to(ref, ref, *flow(kind, c, which))

    def only(c, sender):
        if c in (3, 4):
            return lambda do_it: do_it()
        return pl.when(s == ((0 if sender else 1) if c < 3 else (1 if sender else 0)))

    def launch(c):
        @only(c, True)
        def _():
            hop(0, c).start()

    def spread(c):
        @only(c, False)
        def _():
            hop(0, c).wait_recv()
            hop(1, c).start()
            hop(2, c).start()

    def pass_on(c):
        @only(c, False)
        def _():
            hop(1, c).wait_recv()
            hop(3, c).start()

    def arrived(c):
        @only(c, False)
        def _():
            hop(2, c).wait_recv()
            hop(3, c).wait_recv()

    def sent(c):
        @only(c, True)
        def _():
            hop(0, c).wait_send()

        @only(c, False)
        def _():
            for kind in (1, 2, 3):
                hop(kind, c).wait_send()

    rest = acc.at[pl.ds(s * N_HALF + last, N_HALF - last)]
    rests = to(rest, rest, rest_sems.at[0], rest_sems.at[1], across)
    launch(0)
    launch(1)
    rests.start()
    top, low = pl.ds(0, x0.shape[0] // 2), pl.ds(x0.shape[0] // 2, x0.shape[0] // 2)
    direct = to(a2.at[top], x0.at[top], swap_sems.at[0, 0], swap_sems.at[1, 0], diagonal)
    aside = to(a2.at[low], do.at[low], relay_sems.at[0, 0], relay_sems.at[0, 1], core)
    onward = to(do.at[low], x0.at[low], relay_sems.at[1, 0], relay_sems.at[1, 1], across)
    local = pltpu.make_async_copy(a2, x0, load.at[1])

    @pl.when(jnp.logical_not(stays))
    def _():
        aside.start()
        direct.start()

    @pl.when(stays)
    def _():
        local.start()
        aside.wait_recv()
        onward.start()

    for c in (2, 3, 4, 5, 6):
        launch(c)
    spread(0)
    spread(1)
    rests.wait_recv()
    unpack_small(flat, outs, main)
    pass_on(0)
    pass_on(1)
    arrived(0)
    arrived(1)

    exchanges = []

    def exchange(src, dst):
        k = len(exchanges)
        copy = to(src, dst, kv_sems.at[0, k], kv_sems.at[1, k], core)
        copy.start()
        exchanges.append(copy)
        return copy


    @pl.when(jnp.logical_not(stays))
    def _():
        aside.wait_send()
        direct.wait()
        onward.wait_recv()

    @pl.when(stays)
    def _():
        local.wait()

    qkv_forward(x0, wqkv0, vec0, q0, kv0.at[0])
    first_kv = exchange(kv0.at[0], kv0.at[1])
    spread(2)
    spread(3)
    pass_on(2)
    first_kv.wait_recv()

    def relay(k):
        spread(4 + k)
        if k == 0:
            swap(dq, cot, 1)
        if k == 2:
            pass_on(3)
            pass_on(4)

    attend(q0, kv0, o_t0, lse0, values_t, rows, relay)
    pass_on(5)
    pass_on(6)
    for c in (2, 3, 4, 5, 6):
        arrived(c)
    for c in range(7):
        sent(c)
    rests.wait_send()

    @pl.when(stays)
    def _():
        onward.wait_send()

    for which in (1, 2, 3):
        unpack_weights(flat, outs, main, which)
    out_forward(x0, o_t0, wo0, vec0, h10)
    second_norm(h10, vec0, a2)
    mlp_forward(h10, a2, wup0, wdown0, vec0, x1)
    qkv_forward(x1, wqkv1, vec1, q1, kv1.at[0])
    exchange(kv1.at[0], kv1.at[1]).wait_recv()
    attend(q1, kv1, o_t1, lse1, values_t, rows)
    out_forward(x1, o_t1, wo1, vec1, h11)
    second_norm(h11, vec1, a2)

    enc = wdown1.at[pl.ds(0, x0.shape[0])]
    reducer = Reducer(ranks, half_rows, acc, res, landing, send_sems, recv_sems)
    early = [[layer * CHUNKS + c for c in range(CHUNKS // 2, CHUNKS)] for layer in range(LAYERS)]
    late = [[layer * CHUNKS + c for c in range(CHUNKS // 2)] for layer in range(LAYERS)]
    moved = (N_MAIN + shift) // 16 * 16

    def main_start():
        edge = N_HALF - N_QKV
        main[edge : edge + shift, :] = jnp.zeros((shift, LANES), f32)
        last = N_MAIN + shift
        main[last:, :] = jnp.zeros((main.shape[0] - last, LANES), f32)

    def main_end(layer):
        base = layer * 2 * half_rows
        to_low(main, 0, flat, base + N_QKV, main.shape[0])
        to_low(main, half_rows - N_QKV, flat, base + N_QKV + moved, 32, 32)
        tail[...] = main[moved : moved + 32, :]

    def late_start(layer):
        to_low(main, 0, flat, layer * 2 * half_rows, N_QKV)
        reducer.advance(late[layer][1:])

    def late_end(layer):
        to_low(tail, 0, flat, layer * 2 * half_rows + half_rows, 32, 32)
        reducer.advance(late[layer][:1])

    tail_shift = N_MAIN + shift - moved
    main_start()
    swapped(dq, cot, 1)
    mlp_backward(shift, cot, h11, a2, wup1, wdown1, vec1, main, da, dh1, enc)
    swap(enc, enc_in, 2)
    out_backward(shift, dh1, o_t1, wo1, main, do, delta)
    main_end(1)
    reducer.advance(early[1])
    attend_backward(q1, kv1, lse1, do, delta, dqkv, dkv_oth, dq_t, rows,
                    lambda hp: reducer.advance(early[1]))
    exchange(dkv_oth, dkv_in).wait_recv()
    qkv_backward(tail_shift, x1, dqkv, dkv_in, dh1, wqkv1, vec1, main, tail, a2, da, h11,
                 lambda: late_start(1))
    late_end(1)
    reducer.advance(early[1])
    main_start()
    second_norm(h10, vec0, a2)
    reducer.advance(late[1])
    exchanges[-1].wait_send()
    mlp_backward(shift, h11, h10, a2, wup0, wdown0, vec0, main, da, dh1, None)
    reducer.advance(early[1])
    out_backward(shift, dh1, o_t0, wo0, main, do, delta)
    main_end(0)
    reducer.advance(late[1])
    reducer.advance(early[0])
    attend_backward(q0, kv0, lse0, do, delta, dqkv, dkv_oth, dq_t, rows,
                    lambda hp: reducer.advance(early[1] + late[1] + early[0]))
    exchange(dkv_oth, kv1.at[1]).wait_recv()
    qkv_backward(tail_shift, x0, dqkv, kv1.at[1], dh1, wqkv0, vec0, main, tail, a2, da, do,
                 lambda: late_start(0))
    swap(do, cot, 3)
    late_end(0)
    others = early[0] + late[1] + early[1]
    for tick in range(reducer.stages):
        reducer.advance(late[0][::-1])
        reducer.advance(others)
    reducer.drain()
    for k, copy in enumerate(exchanges):
        if k != 2:
            copy.wait_send()

    @pl.when(s == 1)
    def _():
        out = res.reshape(2 * res.shape[0], LANES)
        for layer in range(LAYERS):
            one = pl.ds(layer * half_rows, 32)
            two = pl.ds(layer * half_rows + N_QKV + moved - half_rows, 32)
            keep = out[one, :]
            out[one, :] = out[two, :]
            out[two, :] = keep

    outs = [
        pltpu.make_async_copy(res.at[pl.ds(k * half_rows // 2, half_rows // 2)], out, store.at[k])
        for k, out in enumerate((out0, out1))
    ]
    for copy in outs:
        copy.start()
    swapped(enc, enc_in, 2)
    enc_out[...] = enc_in[:rows, :]
    swapped(do, cot, 3)
    dx_out[...] = cot[:rows, :]
    for copy in outs:
        copy.wait()


def adam_kernel(g0_ref, g1_ref, w_ref, one_ref, two_ref, g_out, p_out, one_out, two_out):
    block = 2 * g0_ref.shape[0]
    flat = lambda ref: ref.reshape(LAYERS * block, LANES)
    low = lambda ref: ref.reshape(block, LANES)
    for layer, g_ref in enumerate((g0_ref, g1_ref)):
        flat(g_out)[pl.ds(layer, block, stride=LAYERS), :] = low(g_ref)[...].astype(f32)

    @pl.loop(0, LAYERS * block // 128)
    def _(i):
        rows = pl.ds(pl.multiple_of(i * 128, 128), 128)
        grad = flat(g_out)[rows, :]
        weight = flat(w_ref)[rows, :].astype(f32)
        one = beta_one * flat(one_ref)[rows, :] + (1.0 - beta_one) * grad
        two = beta_two * flat(two_ref)[rows, :] + (1.0 - beta_two) * grad * grad
        square = two * (1.0 / fix_two)
        root = square * lax.rsqrt(square)
        step = one * lax.rsqrt(square + adam_eps * (2.0 * root + adam_eps))
        flat(p_out)[rows, :] = weight * (1.0 - rate * decay) - (rate / fix_one) * step
        flat(one_out)[rows, :] = one
        flat(two_out)[rows, :] = two


def to_rows(array):
    view = array.reshape(LAYERS, -1, LANES)
    return with_layout_constraint(view, Layout(major_to_minor=(1, 0, 2))).transpose(1, 0, 2)


def from_rows(array):
    view = with_layout_constraint(array.transpose(1, 0, 2), Layout(major_to_minor=(1, 0, 2)))
    return view.reshape(LAYERS, -1)


def body(ranks, frames_in, params, moment_one, moment_two, cotangent):
    rows = frames_in.shape[1]
    pad = -(-rows // RC) * RC

    def vm(shape, dtype):
        return pltpu.VMEM(shape, dtype)

    def sd(shape, dtype):
        return jax.ShapeDtypeStruct(shape, dtype)

    unit = 16 * ranks * CHUNKS
    half_rows = -(-N_HALF // unit) * unit
    tail_rows = -(-(half_rows - N_HALF + N_SMALL + 32) // 64) * 64
    w_rows = to_rows(params)
    row_b = vm((pad, D), bf16)
    kv_b = vm((2, pad, D), bf16)
    kv_both = vm((2, 2, pad, D), bf16)
    row_f = vm((pad, D), f32)
    lse_f = vm((8, pad), f32)
    o_t_b = vm((D, pad), bf16)
    layer_w = [vm((D, 3 * D), bf16), vm((D, D), bf16), vm((D, FF), bf16), vm((FF, D), bf16), vm((VECS, D), f32)]
    down, up = copies_of(levels_of(ranks, True))
    total = LAYERS * CHUNKS
    chunk_sems = pltpu.SemaphoreType.DMA((total, sum(down) + sum(up)))
    anywhere = pl.BlockSpec(memory_space=pl.ANY)
    inside = pl.BlockSpec(memory_space=pltpu.VMEM)
    enc, dx, g0, g1 = pl.pallas_call(
        partial(step_kernel, ranks, rows, half_rows),
        out_shape=[sd((rows, D), bf16)] * 2 + [sd((half_rows // 2, 2, LANES), bf16)] * 2,
        in_specs=[inside, inside, anywhere],
        out_specs=[inside] * 2 + [anywhere] * 2,
        scratch_shapes=[row_b, row_b] + layer_w * 2
        + [row_b, kv_both, o_t_b, lse_f, row_f, row_f, row_b, kv_both, o_t_b, lse_f, row_f, row_b]
        + [row_f, row_f, row_b, lse_f, row_b, vm((3, pad, D), bf16), kv_b, kv_b]
        + [vm((LANES, pad), f32), vm((LANES + 16, 2 * pad), bf16), row_b]
        + [vm((N_MAIN + tail_rows, LANES), f32), vm((32, LANES), f32), vm((2 * half_rows, 2, LANES), bf16)]
        + [vm((half_rows, 2, LANES), bf16), vm((total, half_rows // CHUNKS, 2, LANES), bf16)]
        + [pltpu.SemaphoreType.DMA((5,)), pltpu.SemaphoreType.DMA((2,)), pltpu.SemaphoreType.DMA((2, 4))]
        + [pltpu.SemaphoreType.DMA((2, 2)), pltpu.SemaphoreType.DMA((2,)), pltpu.SemaphoreType.DMA((4, 2, 7)), pltpu.SemaphoreType.DMA((2, 4))]
        + [chunk_sems, chunk_sems],
        compiler_params=pltpu.CompilerParams(vmem_limit_bytes=67043328, collective_id=0, has_side_effects=True),
        name="step",
    )(frames_in[0], cotangent[0], w_rows)
    encoded, frames_grad = enc[None], dx[None]
    block = 1280
    low = pl.BlockSpec((block // 2, 2, LANES), lambda i: (i, 0, 0))
    spec = pl.BlockSpec((block, 2, LANES), lambda i: (i, 0, 0))
    row_shape = sd((N_HALF, 2, LANES), f32)
    grad, new_params, new_one, new_two = pl.pallas_call(
        adam_kernel, grid=(pl.cdiv(N_HALF, block),), in_specs=[low, low, spec, spec, spec], out_specs=[spec] * 4,
        out_shape=[row_shape] * 4,
        compiler_params=pltpu.CompilerParams(vmem_limit_bytes=62 << 20), name="adam",
    )(g0, g1, w_rows, to_rows(moment_one), to_rows(moment_two))
    return (encoded, frames_grad, from_rows(grad), from_rows(new_params), from_rows(new_one), from_rows(new_two))


def solution(mesh):
    in_specs = (
        P("rep", "shard", None),
        P(None, "shard"),
        P(None, "shard"),
        P(None, "shard"),
        P("rep", "shard", None),
    )
    out_specs = (
        P("rep", "shard", None),
        P("rep", "shard", None),
        P(None, "shard"),
        P(None, "shard"),
        P(None, "shard"),
        P(None, "shard"),
    )
    return jax.shard_map(
        partial(body, mesh.shape["rep"]), mesh=mesh, in_specs=in_specs, out_specs=out_specs, check_vma=False
    )
```

```python
from functools import partial

import jax
import jax.numpy as jnp
from jax import lax
from jax.experimental import pallas as pl
from jax.experimental.layout import Layout, with_layout_constraint
from jax.experimental.pallas import tpu as pltpu
from jax.sharding import PartitionSpec as P

D = 384
HEADS = 6
FF = 1536
LAYERS = 2
HD = D // HEADS
LANES = 128
T_QKV, T_O, T_UP, T_DOWN = 3 * D // LANES, D // LANES, FF // LANES, D // LANES
N_QKV, N_O, N_UP, N_DOWN = D * T_QKV, D * T_O, D * T_UP, FF * T_DOWN
N_SMALL = (8 * D + FF) // LANES
N_MAIN = N_O + N_UP + N_DOWN
N_ROWS = N_QKV + N_MAIN + N_SMALL
N_HALF = N_ROWS // 2
UP_BASE, DOWN_BASE = N_O, N_O + N_UP
MESH = pl.DeviceIdType.MESH
CHUNKS = 4
VECS = 16
FB = 384
RC = 256

ln_eps = 1e-05
rate = 0.01
beta_one = 0.9
beta_two = 0.95
adam_eps = 1e-08
decay = 0.1
fix_one = 1.0 - 0.9**3
fix_two = 1.0 - 0.95**3
LOG2E = 1.4426950408889634
SCALE2 = 0.125 * LOG2E
NEG = -1e30

f32 = jnp.float32
bf16 = jnp.bfloat16


def nn(left, right):
    return lax.dot_general(left, right, (((1,), (0,)), ((), ())), preferred_element_type=f32)


def nt(left, right):
    return lax.dot_general(left, right, (((1,), (1,)), ((), ())), preferred_element_type=f32)


def tn(left, right):
    return lax.dot_general(left, right, (((0,), (0,)), ((), ())), preferred_element_type=f32)


def stats(values):
    center = values - jnp.mean(values, axis=-1, keepdims=True)
    r = lax.rsqrt(jnp.mean(center * center, axis=-1, keepdims=True) + ln_eps)
    return center * r, r


def vec(vec_ref, row):
    return vec_ref[row : row + 1, :]


G1, G2, N1, BQ, BV, BO, N2, BD, BUP = range(9)


def each_chunk(rows, body):
    @pl.loop(0, rows // RC)
    def _(i):
        body(pl.ds(pl.multiple_of(i * RC, RC), RC))


def put_row(ref, row, value):
    for j in range(value.shape[1] // LANES):
        ref[pl.ds(row + j, 1), :] = value[:, j * LANES : (j + 1) * LANES]


def put_flat(ref, base, stride, value):
    for j in range(value.shape[1] // LANES):
        ref[pl.ds(base + j, value.shape[0], stride=stride), :] = value[:, j * LANES : (j + 1) * LANES]


def put_up(ref, shift, block, value):
    first = N_HALF - N_QKV - UP_BASE
    whole, edge = first // T_UP, first % T_UP
    for j in range(value.shape[1] // LANES):
        tile = 3 * block + j
        piece = value[:, j * LANES : (j + 1) * LANES]
        at = UP_BASE + tile
        ref[pl.ds(at, whole, stride=T_UP), :] = piece[:whole, :]
        ref[pl.ds(at + T_UP * whole + jnp.where(tile >= edge, shift, 0), 1), :] = piece[whole : whole + 1, :]
        ref[pl.ds(at + T_UP * (whole + 1) + shift, D - whole - 1, stride=T_UP), :] = piece[whole + 1 :, :]


def to_low(src, base, dst, at, count, step=64):
    @pl.loop(0, count // step)
    def _(i):
        dst[pl.ds(pl.multiple_of(at + i * step, 16), step), :] = src[pl.ds(base + i * step, step), :].astype(bf16)


def unpack_weights(flat, outs, stage, which):
    tiles = (T_QKV, T_O, T_UP, T_DOWN)[which]
    base = (0, N_QKV, N_QKV + UP_BASE, N_QKV + DOWN_BASE)[which]
    count = (N_QKV, N_O, N_UP, N_DOWN)[which]

    @pl.loop(0, count // 192)
    def _(i):
        stage[pl.ds(pl.multiple_of(i * 384, 384), 384), :] = flat[
            pl.ds(pl.multiple_of(2 * base + i * 384, 128), 384), :
        ].astype(f32)

    @pl.loop(0, count // tiles // 128)
    def _(i):
        for layer in range(LAYERS):
            for j in range(tiles):
                outs[5 * layer + which][
                    pl.ds(pl.multiple_of(i * 128, 128), 128), j * LANES : (j + 1) * LANES
                ] = stage[pl.ds(i * (256 * tiles) + 2 * j + layer, 128, stride=2 * tiles), :].astype(bf16)


def unpack_small(flat, outs, stage):
    start = N_QKV + N_MAIN
    stage[0 : 2 * N_SMALL, :] = flat[2 * start : 2 * start + 2 * N_SMALL, :].astype(f32)
    for layer in range(LAYERS):
        for i in range(N_SMALL):
            row, j = i // 3, i % 3
            outs[5 * layer + 4][row : row + 1, j * LANES : (j + 1) * LANES] = stage[
                2 * i + layer : 2 * i + layer + 1, :
            ]


def qkv_forward(x_ref, wqkv_ref, vec_ref, q_ref, kv_ref):
    def chunk(rows):
        xhat, _ = stats(x_ref[rows, :].astype(f32))
        a = (xhat * vec(vec_ref, G1) + vec(vec_ref, N1)).astype(bf16)
        qkv = nn(a, wqkv_ref[...])
        q_ref[rows, :] = (qkv[:, :D] + vec(vec_ref, BQ)).astype(bf16)
        kv_ref[0, rows, :] = qkv[:, D : 2 * D].astype(bf16)
        kv_ref[1, rows, :] = (qkv[:, 2 * D :] + vec(vec_ref, BV)).astype(bf16)

    each_chunk(x_ref.shape[0], chunk)


def one_head(values, which):
    lane = lax.broadcasted_iota(jnp.int32, values.shape, 1) - which * HD
    return jnp.where((lane >= 0) & (lane < HD), values, jnp.zeros_like(values))


def pad_mask(scores, rows, pad=None):
    pad = scores.shape[1] if pad is None else pad
    edge = rows // 8 * 8
    keep = lax.broadcasted_iota(jnp.int32, (pad - edge, scores.shape[1]), 0) < rows - edge
    pieces = []
    for base in range(0, scores.shape[0], pad):
        pieces.append(scores[base : base + edge, :])
        pieces.append(jnp.where(keep, scores[base + edge : base + pad, :], NEG))
    return jnp.concatenate(pieces, axis=0)


def attend(q_ref, kv_ref, o_t_ref, lse_ref, values_t, rows, after_pair=None):
    pad = q_ref.shape[0]
    values_t[LANES:, :] = jnp.ones((16, 2 * pad), bf16)

    @pl.loop(0, HEADS // 2)
    def _(hp):
        cols = pl.ds(pl.multiple_of(hp * LANES, LANES), LANES)
        values_t[:LANES, :] = jnp.concatenate([kv_ref[0, 1, :, cols], kv_ref[1, 1, :, cols]], axis=0).T

        @pl.loop(0, 2)
        def _(t):
            keys = jnp.concatenate([kv_ref[0, 0, :, cols], kv_ref[1, 0, :, cols]], axis=0)
            scores = pad_mask(nt(keys, one_head(q_ref[:, cols], t)), rows)
            top = jnp.max(scores, axis=0, keepdims=True) * SCALE2
            probs = jnp.exp2(scores * SCALE2 - top).astype(bf16)
            left = jnp.concatenate([values_t[pl.ds(pl.multiple_of(t * HD, HD), HD), :], values_t[LANES:, :]], axis=0)
            mixed = nn(left, probs)
            total = mixed[HD : HD + 1, :]
            head = 2 * hp + t
            o_t_ref[pl.ds(pl.multiple_of(head * HD, HD), HD), :] = (mixed[:HD, :] / total).astype(bf16)
            lse_ref[pl.ds(head, 1), :] = top + jnp.log(total) * LOG2E

        for k in range(HEADS // 2 if after_pair else 0):

            @pl.when(hp == k)
            def _():
                after_pair(k)


def out_forward(x_ref, o_t_ref, wo_ref, vec_ref, h1_ref):
    def chunk(rows):
        h1_ref[rows, :] = x_ref[rows, :].astype(f32) + tn(o_t_ref[:, rows], wo_ref[...]) + vec(vec_ref, BO)

    each_chunk(x_ref.shape[0], chunk)


def second_norm(h1_ref, vec_ref, a2_ref):
    def chunk(rows):
        xhat, _ = stats(h1_ref[rows, :])
        a2_ref[rows, :] = (xhat * vec(vec_ref, G2) + vec(vec_ref, N2)).astype(bf16)

    each_chunk(h1_ref.shape[0], chunk)


def mlp_forward(h1_ref, a2_ref, wup_ref, wdown_ref, vec_ref, x_ref):
    x_ref[...] = h1_ref[...] + vec(vec_ref, BD)

    @pl.loop(0, FF // FB)
    def _(b):
        cols = pl.ds(pl.multiple_of(b * FB, FB), FB)
        u = nn(a2_ref[...], wup_ref[:, cols]) + vec_ref[pl.ds(BUP + b, 1), :]
        z = (u * (0.5 + 0.5 * lax.erf(u * 0.7071067811865476))).astype(bf16)
        x_ref[...] += nn(z, wdown_ref[cols, :])


def norm_backward(dy, xhat, r, gain):
    dyg = dy * gain
    inner = jnp.mean(dyg, axis=-1, keepdims=True)
    cross = jnp.mean(dyg * xhat, axis=-1, keepdims=True)
    return r * (dyg - inner - xhat * cross)


def column_sum(values):
    return jnp.sum(values.astype(f32), axis=0, keepdims=True)


def mlp_backward(shift, g_ref, h1_ref, a2_ref, a_t_ref, wup_ref, wdown_ref, vec_ref, main_ref, da2_ref, dh1_ref, enc_ref):
    rows_all = g_ref.shape[0]
    small = N_MAIN + shift
    dy2 = g_ref[...].astype(bf16)
    put_row(main_ref, small + 21, column_sum(dy2))
    da2_ref[...] = jnp.zeros_like(da2_ref)
    a_t_ref[...] = a2_ref[...].T
    if enc_ref is not None:
        dh1_ref[...] = h1_ref[...] + vec(vec_ref, BD)

    @pl.loop(0, FF // FB)
    def _(b):
        cols = pl.ds(pl.multiple_of(b * FB, FB), FB)
        u = nn(a2_ref[...], wup_ref[:, cols]) + vec_ref[pl.ds(BUP + b, 1), :]
        cdf = 0.5 + 0.5 * lax.erf(u * 0.7071067811865476)
        z = (u * cdf).astype(bf16)
        slope = cdf + u * jnp.exp2(u * u * (-0.5 * LOG2E)) * 0.3989422804014327
        if enc_ref is not None:
            dh1_ref[...] += nn(z, wdown_ref[cols, :])
        put_flat(main_ref, DOWN_BASE + shift + T_DOWN * FB * b, T_DOWN, tn(z, dy2))
        du = (nt(dy2, wdown_ref[cols, :]) * slope).astype(bf16)
        put_row(main_ref, small + 24 + 3 * b, column_sum(du))
        put_up(main_ref, shift, b, nn(a_t_ref[...], du))
        da2_ref[...] += nt(du, wup_ref[:, cols])

    if enc_ref is not None:
        enc_ref[...] = dh1_ref[...].astype(bf16)
    dgain = jnp.zeros((1, D), f32)
    dshift = jnp.zeros((1, D), f32)
    for i in range(rows_all // RC):
        rows = slice(i * RC, (i + 1) * RC)
        xhat, r = stats(h1_ref[rows, :])
        dy = da2_ref[rows, :]
        dgain += column_sum(dy * xhat)
        dshift += column_sum(dy)
        dh1_ref[rows, :] = g_ref[rows, :].astype(f32) + norm_backward(dy, xhat, r, vec(vec_ref, G2))
    put_row(main_ref, small + 3, dgain)
    put_row(main_ref, small + 18, dshift)


def out_backward(shift, dh1_ref, o_t_ref, wo_ref, main_ref, do_ref, delta_ref):
    dy1 = dh1_ref[...].astype(bf16)
    put_row(main_ref, N_MAIN + shift + 15, column_sum(dy1))
    put_flat(main_ref, 0, T_O, nn(o_t_ref[...], dy1))
    do_ref[...] = nt(dy1, wo_ref[...]).astype(bf16)
    do_t = nt(wo_ref[...], dy1).astype(bf16).astype(f32)
    prod = do_t * o_t_ref[...].astype(f32)
    for h in range(HEADS):
        delta_ref[h : h + 1, :] = jnp.sum(prod[h * HD : (h + 1) * HD, :], axis=0, keepdims=True)


def attend_backward(q_ref, kv_ref, lse_ref, do_ref, delta_ref, dqkv_ref, dkv_oth_ref, dq_t_ref, rows, after_pair):
    @pl.loop(0, HEADS // 2)
    def _(hp):
        cols = pl.ds(pl.multiple_of(hp * LANES, LANES), LANES)
        for half in range(2):
            keys, values = kv_ref[half, 0, :, cols], kv_ref[half, 1, :, cols]
            keys_t = keys.T
            dk = dv = 0.0
            for t in range(2):
                head = pl.ds(2 * hp + t, 1)
                part = slice(t * HD, (t + 1) * HD)
                q_one, do_one = one_head(q_ref[:, cols], t), one_head(do_ref[:, cols], t)
                scores = pad_mask(nt(keys, q_one), rows)
                probs = jnp.exp2(scores * SCALE2 - lse_ref[head, :])
                dv += nn(probs.astype(bf16), do_one)
                ds = (probs * (nt(values, do_one) - delta_ref[head, :])).astype(bf16)
                dk += nn(ds, q_one)
                dq_part = nn(keys_t[part, :], ds) * 0.125
                if half == 0:
                    dq_t_ref[part, :] = dq_part
                else:
                    dq_t_ref[part, :] += dq_part
            dst = (dqkv_ref.at[pl.ds(1, 2)], dkv_oth_ref)[half]
            dst[0, :, cols] = (dk * 0.125).astype(bf16)
            dst[1, :, cols] = dv.astype(bf16)
        dqkv_ref[0, :, cols] = dq_t_ref[...].T.astype(bf16)
        for k in range(HEADS // 2):

            @pl.when(hp == k)
            def _():
                after_pair(k)


def qkv_backward(shift, x_ref, dqkv_ref, dkv_in_ref, dh1_ref, wqkv_ref, vec_ref, gq_ref, tail_ref,
                 a_ref, a_t_ref, da_ref, dx_ref, after_blocks):
    def first(rows):
        xhat, _ = stats(x_ref[rows, :].astype(f32))
        a_ref[rows, :] = (xhat * vec(vec_ref, G1) + vec(vec_ref, N1)).astype(bf16)
        for b in range(2):
            total = dqkv_ref[b + 1, rows, :].astype(f32) + dkv_in_ref[b, rows, :].astype(f32)
            dqkv_ref[b + 1, rows, :] = total.astype(bf16)

    each_chunk(x_ref.shape[0], first)
    a_t_ref[...] = a_ref[...].T
    da_ref[...] = jnp.zeros_like(da_ref)

    @pl.loop(0, 3)
    def _(b):
        low = dqkv_ref[b]

        @pl.when(b != 1)
        def _():
            put_row(tail_ref, shift + 9 + jnp.where(b == 2, 3, 0), column_sum(low))

        put_flat(gq_ref, 3 * b, T_QKV, nn(a_t_ref[...], low))
        da_ref[...] += nt(low, wqkv_ref[:, pl.ds(pl.multiple_of(b * D, D), D)])

    after_blocks()
    dgain = jnp.zeros((1, D), f32)
    dshift = jnp.zeros((1, D), f32)
    for i in range(x_ref.shape[0] // RC):
        rows = slice(i * RC, (i + 1) * RC)
        xhat, r = stats(x_ref[rows, :].astype(f32))
        dy = da_ref[rows, :]
        dgain += column_sum(dy * xhat)
        dshift += column_sum(dy)
        dx_ref[rows, :] = (dh1_ref[rows, :] + norm_backward(dy, xhat, r, vec(vec_ref, G1))).astype(dx_ref.dtype)
    put_row(tail_ref, shift + 0, dgain)
    put_row(tail_ref, shift + 6, dshift)


def greet(partners):
    for where in partners:
        pl.semaphore_signal(pltpu.get_barrier_semaphore(), inc=1, device_id=where, device_id_type=MESH)


def to(src, dst, send, recv, where):
    return pltpu.make_async_remote_copy(
        src_ref=src, dst_ref=dst, send_sem=send, recv_sem=recv, device_id=where, device_id_type=MESH
    )


def levels_of(ranks, late_x=False):
    bits = ranks.bit_length() - 1
    groups = [(b, min(2, bits - b)) for b in range(2, bits, 2)]
    return [(0, 1), (1, 1), None] + groups if late_x else [(0, 1), None, (1, 1)] + groups


def peers_of(level):
    low, count = level
    return range(1, 1 << count)


def copies_of(levels):
    crossing = levels.index(None)
    down = []
    for k, level in enumerate(levels):
        down.append(1 if level is None else ((1 << level[1]) - 1) * (2 if k < crossing else 1))
    up = [(1 << level[1]) - 1 for level in reversed(levels) if level is not None]
    return down, up


class Reducer:
    def __init__(self, ranks, half_rows, acc, res, landing, send_sems, recv_sems):
        self.acc, self.res, self.landing = acc, res, landing
        self.send_sems, self.recv_sems = send_sems, recv_sems
        self.half_rows = half_rows
        self.n = half_rows // CHUNKS
        self.orders = [levels_of(ranks), levels_of(ranks, True)]
        self.stages = 2 * len(self.orders[0]) - 1
        self.state = {}
        self.begun = []

    def plan(self, ci):
        levels = self.orders[ci % 2]
        down, up = copies_of(levels)
        return levels, down + up

    def place(self):
        return lax.axis_index("shard"), lax.axis_index("rep")

    def index(self, level):
        _, r = self.place()
        return (r >> level[0]) & ((1 << level[1]) - 1)

    def size(self, levels, upto):
        size = self.n
        for level in levels[: upto + 1]:
            if level is not None:
                size >>= level[1]
        return size

    def offset(self, levels, upto):
        at = 0
        for k, level in enumerate(levels[: upto + 1]):
            if level is not None:
                at = at + self.index(level) * self.size(levels, k)
        return at

    def slot(self, ci, k, m):
        levels, counts = self.plan(ci)
        return sum(counts[i] * self.size(levels, i) for i in range(k)) + m * self.size(levels, k)

    def pair_rows(self, at, size):
        return pl.ds(at // 2 if isinstance(at, int) else lax.div(at, 2), size // 2)

    def describe(self, ci, stage):
        layer, base = ci // CHUNKS, ci % CHUNKS * self.n
        levels, counts = self.plan(ci)
        s, r = self.place()
        first = sum(counts[:stage])
        out = []

        def add(src, dst, where):
            k = first + len(out)
            out.append(to(src, dst, self.send_sems.at[ci, k], self.recv_sems.at[ci, k], where))

        def send(half, at, size, where):
            rows = self.pair_rows((layer * 2 + half) * self.half_rows + base + at, size)
            add(self.acc.at[rows], self.landing.at[ci, self.pair_rows(self.slot(ci, stage, len(out)), size)], where)

        if stage < len(levels):
            level, size = levels[stage], self.size(levels, stage)
            if level is None:
                send(1 - s, self.offset(levels, stage), size, {"shard": 1 - s})
            else:
                for half in range(2) if stage < levels.index(None) else (s,):
                    for m in peers_of(level):
                        at = self.offset(levels, stage - 1) + (self.index(level) ^ m) * size
                        send(half, at, size, {"rep": r ^ (m << level[0])})
        else:
            level = [one for one in reversed(levels) if one is not None][stage - len(levels)]
            k = levels.index(level)
            at = layer * self.half_rows + base + self.offset(levels, k)
            ref = self.res.at[self.pair_rows(at, self.size(levels, k))]
            for m in peers_of(level):
                add(ref, ref, {"rep": r ^ (m << level[0])})
        return out

    def begin(self, ci, stage):
        for copy in self.describe(ci, stage):
            copy.start()
        self.begun.append((ci, stage))

    def finish(self, ci, stage):
        layer, base = ci // CHUNKS, ci % CHUNKS * self.n
        levels, counts = self.plan(ci)
        s, _ = self.place()
        for copy in self.describe(ci, stage):
            copy.wait_recv()
        if stage >= len(levels):
            return
        size = self.size(levels, stage)
        acc = self.acc.reshape(2 * self.acc.shape[0], LANES)
        res = self.res.reshape(2 * self.res.shape[0], LANES)
        count = self.landing.shape[1] * 2
        landing = self.landing.reshape(self.landing.shape[0] * count, LANES)
        step = 16
        while size % (2 * step) == 0 and step < 128:
            step *= 2
        halves = (0, 1) if stage < levels.index(None) else (s,)
        each = counts[stage] // len(halves)
        for k, half in enumerate(halves):
            slots = [self.slot(ci, stage, k * each + m) for m in range(each)]
            src = (layer * 2 + half) * self.half_rows + base + self.offset(levels, stage)
            out, out_at = acc, src
            if stage == len(levels) - 1:
                out, out_at = res, layer * self.half_rows + base + self.offset(levels, stage)

            @pl.loop(0, size // step)
            def _(i):
                def rows(start):
                    return pl.ds(pl.multiple_of(start + i * step, 16), step)

                total = acc[rows(src), :].astype(f32)
                for slot in slots:
                    total = total + landing[rows(ci * count + slot), :].astype(f32)
                out[rows(out_at), :] = total.astype(bf16)

    def advance(self, chunks):
        for ci in chunks:
            stage = self.state.get(ci, -1)
            if stage >= self.stages:
                continue
            if stage >= 0:
                self.finish(ci, stage)
            stage += 1
            self.state[ci] = stage
            if stage < self.stages:
                self.begin(ci, stage)

    def drain(self):
        for ci, stage in self.begun:
            for copy in self.describe(ci, stage):
                copy.wait_send()


def pad_rows(src, dst):
    rows, pad = src.shape[0], dst.shape[0]
    edge = rows // 16 * 16
    dst[:edge, :] = src[:edge, :]
    dst[edge:, :] = jnp.zeros((pad - edge, dst.shape[1]), dst.dtype)
    dst[edge:rows, :] = src[edge:, :]


def step_kernel(ranks, rows, half_rows, frames, cot_in, weights, enc_out, dx_out, out0, out1, x0, cot,
                wqkv0, wo0, wup0, wdown0, vec0, wqkv1, wo1, wup1, wdown1, vec1,
                q0, kv0, o_t0, lse0, h10, x1, q1, kv1, o_t1, lse1, h11, a2, a_t, da, dh1,
                do, delta, dq, dqkv, dkv_oth, dkv_in, dq_t, values_t, enc_in, main, tail, acc, res, landing,
                load, store, swap_sems, relay_sems, rest_sems, hop_sems, kv_sems, send_sems, recv_sems):
    s, r = lax.axis_index("shard"), lax.axis_index("rep")
    shift = half_rows - N_HALF
    across, core, beside = {"shard": 1 - s}, {"rep": r ^ 1}, {"rep": r ^ 2}
    diagonal = {"shard": 1 - s, "rep": r ^ 1}
    stays = s == r % 2
    filling = pltpu.make_async_copy(weights, acc.at[pl.ds(s * N_HALF, N_HALF)], load.at[0])
    filling.start()
    partners = [{"rep": r ^ (m << level[0])} for level in levels_of(ranks) if level is not None for m in peers_of(level)]
    partners += [diagonal, across]
    greet(partners)
    outs = [wqkv0, wo0, wup0, wdown0, vec0, wqkv1, wo1, wup1, wdown1, vec1]
    flat = acc.reshape(2 * acc.shape[0], LANES)
    pad_rows(frames, a2)
    pad_rows(cot_in, dq)
    filling.wait()

    @pl.when(s == 0)
    def _():
        unpack_weights(flat, outs, main, 0)

    pl.semaphore_wait(pltpu.get_barrier_semaphore(), len(partners))

    def swap(src, dst, k):
        @pl.when(stays)
        def _():
            pltpu.make_async_copy(src, dst, load.at[1 + k]).start()

        @pl.when(jnp.logical_not(stays))
        def _():
            to(src, dst, swap_sems.at[0, k], swap_sems.at[1, k], diagonal).start()

    def swapped(src, dst, k):
        @pl.when(stays)
        def _():
            pltpu.make_async_copy(src, dst, load.at[1 + k]).wait()

        @pl.when(jnp.logical_not(stays))
        def _():
            to(src, dst, swap_sems.at[0, k], swap_sems.at[1, k], diagonal).wait()

    q = r % 4
    second = (N_HALF - N_QKV - N_SMALL) // 4
    last = N_QKV + 4 * second
    part = D // 4

    def flow(kind, c, which):
        return (hop_sems.at[kind, 0, c], hop_sems.at[kind, 1, c], (across, beside, core, core)[kind])

    def wide(c, which):
        w, start, size = ((wqkv0, 0, part // 2), (wqkv0, part // 2, part // 2), (wqkv1, 0, part))[c]
        return w.at[pl.ds(pl.multiple_of(which * part + start, 16), size), :]

    def units(c, which, half):
        at, quarter, start, size = (
            (N_QKV, second, 0, second // 2),
            (N_QKV, second, second // 2, second - second // 2),
            (0, N_QKV // 4, 0, N_QKV // 8),
            (0, N_QKV // 4, N_QKV // 8, N_QKV // 8),
        )[c - 3]
        return acc.at[pl.ds(half * N_HALF + at + which * quarter + start, size)]

    def hop(kind, c):
        which = q ^ 2 if kind == 3 else q
        half = s if kind == 0 else 1 - s
        ref = wide(c, which) if c < 3 else units(c, which, half)
        return to(ref, ref, *flow(kind, c, which))

    def only(c, sender):
        if c in (3, 4):
            return lambda do_it: do_it()
        return pl.when(s == ((0 if sender else 1) if c < 3 else (1 if sender else 0)))

    def launch(c):
        @only(c, True)
        def _():
            hop(0, c).start()

    def spread(c):
        @only(c, False)
        def _():
            hop(0, c).wait_recv()
            hop(1, c).start()
            hop(2, c).start()

    def pass_on(c):
        @only(c, False)
        def _():
            hop(1, c).wait_recv()
            hop(3, c).start()

    def arrived(c):
        @only(c, False)
        def _():
            hop(2, c).wait_recv()
            hop(3, c).wait_recv()

    def sent(c):
        @only(c, True)
        def _():
            hop(0, c).wait_send()

        @only(c, False)
        def _():
            for kind in (1, 2, 3):
                hop(kind, c).wait_send()

    rest = acc.at[pl.ds(s * N_HALF + last, N_HALF - last)]
    rests = to(rest, rest, rest_sems.at[0], rest_sems.at[1], across)
    launch(0)
    launch(1)
    rests.start()
    top, low = pl.ds(0, x0.shape[0] // 2), pl.ds(x0.shape[0] // 2, x0.shape[0] // 2)
    direct = to(a2.at[top], x0.at[top], swap_sems.at[0, 0], swap_sems.at[1, 0], diagonal)
    aside = to(a2.at[low], do.at[low], relay_sems.at[0, 0], relay_sems.at[0, 1], core)
    onward = to(do.at[low], x0.at[low], relay_sems.at[1, 0], relay_sems.at[1, 1], across)
    local = pltpu.make_async_copy(a2, x0, load.at[1])

    @pl.when(jnp.logical_not(stays))
    def _():
        aside.start()
        direct.start()

    @pl.when(stays)
    def _():
        local.start()
        aside.wait_recv()
        onward.start()

    for c in (2, 3, 4, 5, 6):
        launch(c)
    spread(0)
    spread(1)
    rests.wait_recv()
    unpack_small(flat, outs, main)
    pass_on(0)
    pass_on(1)
    arrived(0)
    arrived(1)

    exchanges = []

    def exchange(src, dst):
        k = len(exchanges)
        copy = to(src, dst, kv_sems.at[0, k], kv_sems.at[1, k], core)
        copy.start()
        exchanges.append(copy)
        return copy


    @pl.when(jnp.logical_not(stays))
    def _():
        aside.wait_send()
        direct.wait()
        onward.wait_recv()

    @pl.when(stays)
    def _():
        local.wait()

    qkv_forward(x0, wqkv0, vec0, q0, kv0.at[0])
    first_kv = exchange(kv0.at[0], kv0.at[1])
    spread(2)
    spread(3)
    pass_on(2)
    first_kv.wait_recv()

    def relay(k):
        spread(4 + k)
        if k == 0:
            swap(dq, cot, 1)
        if k == 2:
            pass_on(3)
            pass_on(4)

    attend(q0, kv0, o_t0, lse0, values_t, rows, relay)
    pass_on(5)
    pass_on(6)
    for c in (2, 3, 4, 5, 6):
        arrived(c)
    for c in range(7):
        sent(c)
    rests.wait_send()

    @pl.when(stays)
    def _():
        onward.wait_send()

    for which in (1, 2, 3):
        unpack_weights(flat, outs, main, which)
    out_forward(x0, o_t0, wo0, vec0, h10)
    second_norm(h10, vec0, a2)
    mlp_forward(h10, a2, wup0, wdown0, vec0, x1)
    qkv_forward(x1, wqkv1, vec1, q1, kv1.at[0])
    exchange(kv1.at[0], kv1.at[1]).wait_recv()
    attend(q1, kv1, o_t1, lse1, values_t, rows)
    out_forward(x1, o_t1, wo1, vec1, h11)
    second_norm(h11, vec1, a2)

    enc = wdown1.at[pl.ds(0, x0.shape[0])]
    reducer = Reducer(ranks, half_rows, acc, res, landing, send_sems, recv_sems)
    early = [[layer * CHUNKS + c for c in range(CHUNKS // 2, CHUNKS)] for layer in range(LAYERS)]
    late = [[layer * CHUNKS + c for c in range(CHUNKS // 2)] for layer in range(LAYERS)]
    moved = (N_MAIN + shift) // 16 * 16

    def main_start():
        edge = N_HALF - N_QKV
        main[edge : edge + shift, :] = jnp.zeros((shift, LANES), f32)
        last = N_MAIN + shift
        main[last:, :] = jnp.zeros((main.shape[0] - last, LANES), f32)

    def main_end(layer):
        base = layer * 2 * half_rows
        to_low(main, 0, flat, base + N_QKV, N_MAIN, 192)
        to_low(main, N_MAIN, flat, base + N_QKV + N_MAIN, main.shape[0] - N_MAIN)
        to_low(main, half_rows - N_QKV, flat, base + N_QKV + moved, 32, 32)
        tail[...] = main[moved : moved + 32, :]

    def late_start(layer):
        to_low(main, 0, flat, layer * 2 * half_rows, N_QKV, 192)
        reducer.advance(late[layer][1:])

    def late_end(layer):
        to_low(tail, 0, flat, layer * 2 * half_rows + half_rows, 32, 32)
        reducer.advance(late[layer][:1])

    tail_shift = N_MAIN + shift - moved
    main_start()
    swapped(dq, cot, 1)
    mlp_backward(shift, cot, h11, a2, a_t, wup1, wdown1, vec1, main, da, dh1, enc)
    swap(enc, enc_in, 2)
    out_backward(shift, dh1, o_t1, wo1, main, do, delta)
    main_end(1)
    reducer.advance(early[1])
    attend_backward(q1, kv1, lse1, do, delta, dqkv, dkv_oth, dq_t, rows,
                    lambda hp: reducer.advance(early[1]))
    exchange(dkv_oth, dkv_in).wait_recv()
    qkv_backward(tail_shift, x1, dqkv, dkv_in, dh1, wqkv1, vec1, main, tail, a2, a_t, da, h11,
                 lambda: late_start(1))
    late_end(1)
    reducer.advance(early[1])
    main_start()
    second_norm(h10, vec0, a2)
    reducer.advance(late[1])
    exchanges[-1].wait_send()
    mlp_backward(shift, h11, h10, a2, a_t, wup0, wdown0, vec0, main, da, dh1, None)
    reducer.advance(early[1])
    out_backward(shift, dh1, o_t0, wo0, main, do, delta)
    main_end(0)
    reducer.advance(late[1])
    reducer.advance(early[0])
    attend_backward(q0, kv0, lse0, do, delta, dqkv, dkv_oth, dq_t, rows,
                    lambda hp: reducer.advance(early[1] + late[1] + early[0]))
    exchange(dkv_oth, kv1.at[1]).wait_recv()
    qkv_backward(tail_shift, x0, dqkv, kv1.at[1], dh1, wqkv0, vec0, main, tail, a2, a_t, da, do,
                 lambda: late_start(0))
    swap(do, cot, 3)
    late_end(0)
    others = early[0] + late[1] + early[1]
    for tick in range(reducer.stages):
        reducer.advance(late[0][::-1])
        reducer.advance(others)
    reducer.drain()
    for k, copy in enumerate(exchanges):
        if k != 2:
            copy.wait_send()

    @pl.when(s == 1)
    def _():
        out = res.reshape(2 * res.shape[0], LANES)
        for layer in range(LAYERS):
            one = pl.ds(layer * half_rows, 32)
            two = pl.ds(layer * half_rows + N_QKV + moved - half_rows, 32)
            keep = out[one, :]
            out[one, :] = out[two, :]
            out[two, :] = keep

    outs = [
        pltpu.make_async_copy(res.at[pl.ds(k * half_rows // 2, half_rows // 2)], out, store.at[k])
        for k, out in enumerate((out0, out1))
    ]
    for copy in outs:
        copy.start()
    swapped(enc, enc_in, 2)
    enc_out[...] = enc_in[:rows, :]
    swapped(do, cot, 3)
    dx_out[...] = cot[:rows, :]
    for copy in outs:
        copy.wait()


def adam_kernel(g0_ref, g1_ref, w_ref, one_ref, two_ref, g_out, p_out, one_out, two_out):
    block = 2 * g0_ref.shape[0]
    flat = lambda ref: ref.reshape(LAYERS * block, LANES)
    low = lambda ref: ref.reshape(block, LANES)
    for layer, g_ref in enumerate((g0_ref, g1_ref)):
        flat(g_out)[pl.ds(layer, block, stride=LAYERS), :] = low(g_ref)[...].astype(f32)

    @pl.loop(0, LAYERS * block // 128)
    def _(i):
        rows = pl.ds(pl.multiple_of(i * 128, 128), 128)
        grad = flat(g_out)[rows, :]
        weight = flat(w_ref)[rows, :].astype(f32)
        one = beta_one * flat(one_ref)[rows, :] + (1.0 - beta_one) * grad
        two = beta_two * flat(two_ref)[rows, :] + (1.0 - beta_two) * grad * grad
        square = two * (1.0 / fix_two)
        root = square * lax.rsqrt(square)
        step = one * lax.rsqrt(square + adam_eps * (2.0 * root + adam_eps))
        flat(p_out)[rows, :] = weight * (1.0 - rate * decay) - (rate / fix_one) * step
        flat(one_out)[rows, :] = one
        flat(two_out)[rows, :] = two


def to_rows(array):
    view = array.reshape(LAYERS, -1, LANES)
    return with_layout_constraint(view, Layout(major_to_minor=(1, 0, 2))).transpose(1, 0, 2)


def from_rows(array):
    view = with_layout_constraint(array.transpose(1, 0, 2), Layout(major_to_minor=(1, 0, 2)))
    return view.reshape(LAYERS, -1)


def body(ranks, frames_in, params, moment_one, moment_two, cotangent):
    rows = frames_in.shape[1]
    pad = -(-rows // RC) * RC

    def vm(shape, dtype):
        return pltpu.VMEM(shape, dtype)

    def sd(shape, dtype):
        return jax.ShapeDtypeStruct(shape, dtype)

    unit = 16 * ranks * CHUNKS
    half_rows = -(-N_HALF // unit) * unit
    tail_rows = -(-(half_rows - N_HALF + N_SMALL + 32) // 64) * 64
    w_rows = to_rows(params)
    row_b = vm((pad, D), bf16)
    kv_b = vm((2, pad, D), bf16)
    kv_both = vm((2, 2, pad, D), bf16)
    row_f = vm((pad, D), f32)
    lse_f = vm((8, pad), f32)
    o_t_b = vm((D, pad), bf16)
    layer_w = [vm((D, 3 * D), bf16), vm((D, D), bf16), vm((D, FF), bf16), vm((FF, D), bf16), vm((VECS, D), f32)]
    down, up = copies_of(levels_of(ranks, True))
    total = LAYERS * CHUNKS
    chunk_sems = pltpu.SemaphoreType.DMA((total, sum(down) + sum(up)))
    anywhere = pl.BlockSpec(memory_space=pl.ANY)
    inside = pl.BlockSpec(memory_space=pltpu.VMEM)
    enc, dx, g0, g1 = pl.pallas_call(
        partial(step_kernel, ranks, rows, half_rows),
        out_shape=[sd((rows, D), bf16)] * 2 + [sd((half_rows // 2, 2, LANES), bf16)] * 2,
        in_specs=[inside, inside, anywhere],
        out_specs=[inside] * 2 + [anywhere] * 2,
        scratch_shapes=[row_b, row_b] + layer_w * 2
        + [row_b, kv_both, o_t_b, lse_f, row_f, row_f, row_b, kv_both, o_t_b, lse_f, row_f, row_b, o_t_b]
        + [row_f, row_f, row_b, lse_f, row_b, vm((3, pad, D), bf16), kv_b, kv_b]
        + [vm((LANES, pad), f32), vm((LANES + 16, 2 * pad), bf16), row_b]
        + [vm((N_MAIN + tail_rows, LANES), f32), vm((32, LANES), f32), vm((2 * half_rows, 2, LANES), bf16)]
        + [vm((half_rows, 2, LANES), bf16), vm((total, half_rows // CHUNKS, 2, LANES), bf16)]
        + [pltpu.SemaphoreType.DMA((5,)), pltpu.SemaphoreType.DMA((2,)), pltpu.SemaphoreType.DMA((2, 4))]
        + [pltpu.SemaphoreType.DMA((2, 2)), pltpu.SemaphoreType.DMA((2,)), pltpu.SemaphoreType.DMA((4, 2, 7)), pltpu.SemaphoreType.DMA((2, 4))]
        + [chunk_sems, chunk_sems],
        compiler_params=pltpu.CompilerParams(vmem_limit_bytes=67043328, collective_id=0, has_side_effects=True),
        name="step",
    )(frames_in[0], cotangent[0], w_rows)
    encoded, frames_grad = enc[None], dx[None]
    block = 1280
    low = pl.BlockSpec((block // 2, 2, LANES), lambda i: (i, 0, 0))
    spec = pl.BlockSpec((block, 2, LANES), lambda i: (i, 0, 0))
    row_shape = sd((N_HALF, 2, LANES), f32)
    grad, new_params, new_one, new_two = pl.pallas_call(
        adam_kernel, grid=(pl.cdiv(N_HALF, block),), in_specs=[low, low, spec, spec, spec], out_specs=[spec] * 4,
        out_shape=[row_shape] * 4,
        compiler_params=pltpu.CompilerParams(vmem_limit_bytes=62 << 20), name="adam",
    )(g0, g1, w_rows, to_rows(moment_one), to_rows(moment_two))
    return (encoded, frames_grad, from_rows(grad), from_rows(new_params), from_rows(new_one), from_rows(new_two))


def solution(mesh):
    in_specs = (
        P("rep", "shard", None),
        P(None, "shard"),
        P(None, "shard"),
        P(None, "shard"),
        P("rep", "shard", None),
    )
    out_specs = (
        P("rep", "shard", None),
        P("rep", "shard", None),
        P(None, "shard"),
        P(None, "shard"),
        P(None, "shard"),
        P(None, "shard"),
    )
    return jax.shard_map(
        partial(body, mesh.shape["rep"]), mesh=mesh, in_specs=in_specs, out_specs=out_specs, check_vma=False
    )
```

```python
from functools import partial

import jax
import jax.numpy as jnp
from jax import lax
from jax.experimental import pallas as pl
from jax.experimental.layout import Layout, with_layout_constraint
from jax.experimental.pallas import tpu as pltpu
from jax.sharding import PartitionSpec as P

D = 384
HEADS = 6
FF = 1536
LAYERS = 2
HD = D // HEADS
LANES = 128
T_QKV, T_O, T_UP, T_DOWN = 3 * D // LANES, D // LANES, FF // LANES, D // LANES
N_QKV, N_O, N_UP, N_DOWN = D * T_QKV, D * T_O, D * T_UP, FF * T_DOWN
N_SMALL = (8 * D + FF) // LANES
N_MAIN = N_O + N_UP + N_DOWN
N_ROWS = N_QKV + N_MAIN + N_SMALL
N_HALF = N_ROWS // 2
UP_BASE, DOWN_BASE = N_O, N_O + N_UP
MESH = pl.DeviceIdType.MESH
CHUNKS = 4
VECS = 16
FB = 384
RC = 256

ln_eps = 1e-05
rate = 0.01
beta_one = 0.9
beta_two = 0.95
adam_eps = 1e-08
decay = 0.1
fix_one = 1.0 - 0.9**3
fix_two = 1.0 - 0.95**3
LOG2E = 1.4426950408889634
SCALE2 = 0.125 * LOG2E
NEG = -1e30

f32 = jnp.float32
bf16 = jnp.bfloat16


def nn(left, right):
    return lax.dot_general(left, right, (((1,), (0,)), ((), ())), preferred_element_type=f32)


def nt(left, right):
    return lax.dot_general(left, right, (((1,), (1,)), ((), ())), preferred_element_type=f32)


def tn(left, right):
    return lax.dot_general(left, right, (((0,), (0,)), ((), ())), preferred_element_type=f32)


def stats(values):
    center = values - jnp.mean(values, axis=-1, keepdims=True)
    r = lax.rsqrt(jnp.mean(center * center, axis=-1, keepdims=True) + ln_eps)
    return center * r, r


def vec(vec_ref, row):
    return vec_ref[row : row + 1, :]


G1, G2, N1, BQ, BV, BO, N2, BD, BUP = range(9)


def each_chunk(rows, body):
    @pl.loop(0, rows // RC)
    def _(i):
        body(pl.ds(pl.multiple_of(i * RC, RC), RC))


def put_row(ref, row, value):
    for j in range(value.shape[1] // LANES):
        ref[pl.ds(row + j, 1), :] = value[:, j * LANES : (j + 1) * LANES]


def put_flat(ref, base, stride, value):
    for j in range(value.shape[1] // LANES):
        ref[pl.ds(base + j, value.shape[0], stride=stride), :] = value[:, j * LANES : (j + 1) * LANES]


def put_up(ref, shift, block, value):
    first = N_HALF - N_QKV - UP_BASE
    whole, edge = first // T_UP, first % T_UP
    for j in range(value.shape[1] // LANES):
        tile = 3 * block + j
        piece = value[:, j * LANES : (j + 1) * LANES]
        at = UP_BASE + tile
        ref[pl.ds(at, whole, stride=T_UP), :] = piece[:whole, :]
        ref[pl.ds(at + T_UP * whole + jnp.where(tile >= edge, shift, 0), 1), :] = piece[whole : whole + 1, :]
        ref[pl.ds(at + T_UP * (whole + 1) + shift, D - whole - 1, stride=T_UP), :] = piece[whole + 1 :, :]


def to_low(src, base, dst, at, count, step=64):
    @pl.loop(0, count // step)
    def _(i):
        dst[pl.ds(pl.multiple_of(at + i * step, 16), step), :] = src[pl.ds(base + i * step, step), :].astype(bf16)


def unpack_weights(flat, outs, stage, which):
    tiles = (T_QKV, T_O, T_UP, T_DOWN)[which]
    base = (0, N_QKV, N_QKV + UP_BASE, N_QKV + DOWN_BASE)[which]
    count = (N_QKV, N_O, N_UP, N_DOWN)[which]

    @pl.loop(0, count // 192)
    def _(i):
        stage[pl.ds(pl.multiple_of(i * 384, 384), 384), :] = flat[
            pl.ds(pl.multiple_of(2 * base + i * 384, 128), 384), :
        ].astype(f32)

    @pl.loop(0, count // tiles // 64)
    def _(i):
        for layer in range(LAYERS):
            for j in range(tiles):
                outs[5 * layer + which][
                    pl.ds(pl.multiple_of(i * 64, 64), 64), j * LANES : (j + 1) * LANES
                ] = stage[pl.ds(i * (128 * tiles) + 2 * j + layer, 64, stride=2 * tiles), :].astype(bf16)


def unpack_small(flat, outs, stage):
    start = N_QKV + N_MAIN
    stage[0 : 2 * N_SMALL, :] = flat[2 * start : 2 * start + 2 * N_SMALL, :].astype(f32)
    for layer in range(LAYERS):
        for i in range(N_SMALL):
            row, j = i // 3, i % 3
            outs[5 * layer + 4][row : row + 1, j * LANES : (j + 1) * LANES] = stage[
                2 * i + layer : 2 * i + layer + 1, :
            ]


def qkv_forward(x_ref, wqkv_ref, vec_ref, q_ref, kv_ref):
    def chunk(rows):
        xhat, _ = stats(x_ref[rows, :].astype(f32))
        a = (xhat * vec(vec_ref, G1) + vec(vec_ref, N1)).astype(bf16)
        qkv = nn(a, wqkv_ref[...])
        q_ref[rows, :] = (qkv[:, :D] + vec(vec_ref, BQ)).astype(bf16)
        kv_ref[0, rows, :] = qkv[:, D : 2 * D].astype(bf16)
        kv_ref[1, rows, :] = (qkv[:, 2 * D :] + vec(vec_ref, BV)).astype(bf16)

    each_chunk(x_ref.shape[0], chunk)


def one_head(values, which):
    lane = lax.broadcasted_iota(jnp.int32, values.shape, 1) - which * HD
    return jnp.where((lane >= 0) & (lane < HD), values, jnp.zeros_like(values))


def pad_mask(scores, rows, pad=None):
    pad = scores.shape[1] if pad is None else pad
    edge = rows // 8 * 8
    keep = lax.broadcasted_iota(jnp.int32, (pad - edge, scores.shape[1]), 0) < rows - edge
    pieces = []
    for base in range(0, scores.shape[0], pad):
        pieces.append(scores[base : base + edge, :])
        pieces.append(jnp.where(keep, scores[base + edge : base + pad, :], NEG))
    return jnp.concatenate(pieces, axis=0)


def attend(q_ref, kv_ref, o_t_ref, lse_ref, values_t, rows, after_pair=None):
    pad = q_ref.shape[0]
    values_t[LANES:, :] = jnp.ones((16, 2 * pad), bf16)

    @pl.loop(0, HEADS // 2)
    def _(hp):
        cols = pl.ds(pl.multiple_of(hp * LANES, LANES), LANES)
        values_t[:LANES, :] = jnp.concatenate([kv_ref[0, 1, :, cols], kv_ref[1, 1, :, cols]], axis=0).T

        @pl.loop(0, 2)
        def _(t):
            keys = jnp.concatenate([kv_ref[0, 0, :, cols], kv_ref[1, 0, :, cols]], axis=0)
            scores = pad_mask(nt(keys, one_head(q_ref[:, cols], t)), rows)
            top = jnp.max(scores, axis=0, keepdims=True) * SCALE2
            probs = jnp.exp2(scores * SCALE2 - top).astype(bf16)
            left = jnp.concatenate([values_t[pl.ds(pl.multiple_of(t * HD, HD), HD), :], values_t[LANES:, :]], axis=0)
            mixed = nn(left, probs)
            total = mixed[HD : HD + 1, :]
            head = 2 * hp + t
            o_t_ref[pl.ds(pl.multiple_of(head * HD, HD), HD), :] = (mixed[:HD, :] / total).astype(bf16)
            lse_ref[pl.ds(head, 1), :] = top + jnp.log(total) * LOG2E

        for k in range(HEADS // 2 if after_pair else 0):

            @pl.when(hp == k)
            def _():
                after_pair(k)


def out_forward(x_ref, o_t_ref, wo_ref, vec_ref, h1_ref):
    def chunk(rows):
        h1_ref[rows, :] = x_ref[rows, :].astype(f32) + tn(o_t_ref[:, rows], wo_ref[...]) + vec(vec_ref, BO)

    each_chunk(x_ref.shape[0], chunk)


def second_norm(h1_ref, vec_ref, a2_ref):
    def chunk(rows):
        xhat, _ = stats(h1_ref[rows, :])
        a2_ref[rows, :] = (xhat * vec(vec_ref, G2) + vec(vec_ref, N2)).astype(bf16)

    each_chunk(h1_ref.shape[0], chunk)


def mlp_forward(h1_ref, a2_ref, wup_ref, wdown_ref, vec_ref, x_ref):
    x_ref[...] = h1_ref[...] + vec(vec_ref, BD)

    @pl.loop(0, FF // FB)
    def _(b):
        cols = pl.ds(pl.multiple_of(b * FB, FB), FB)
        u = nn(a2_ref[...], wup_ref[:, cols]) + vec_ref[pl.ds(BUP + b, 1), :]
        z = (u * (0.5 + 0.5 * lax.erf(u * 0.7071067811865476))).astype(bf16)
        x_ref[...] += nn(z, wdown_ref[cols, :])


def norm_backward(dy, xhat, r, gain):
    dyg = dy * gain
    inner = jnp.mean(dyg, axis=-1, keepdims=True)
    cross = jnp.mean(dyg * xhat, axis=-1, keepdims=True)
    return r * (dyg - inner - xhat * cross)


def column_sum(values):
    return jnp.sum(values.astype(f32), axis=0, keepdims=True)


def mlp_backward(shift, g_ref, h1_ref, a2_ref, a_t_ref, wup_ref, wdown_ref, vec_ref, main_ref, da2_ref, dh1_ref, enc_ref):
    rows_all = g_ref.shape[0]
    small = N_MAIN + shift
    dy2 = g_ref[...].astype(bf16)
    put_row(main_ref, small + 21, column_sum(dy2))
    da2_ref[...] = jnp.zeros_like(da2_ref)
    a_t_ref[...] = a2_ref[...].T
    if enc_ref is not None:
        dh1_ref[...] = h1_ref[...] + vec(vec_ref, BD)

    @pl.loop(0, FF // FB)
    def _(b):
        cols = pl.ds(pl.multiple_of(b * FB, FB), FB)
        u = nn(a2_ref[...], wup_ref[:, cols]) + vec_ref[pl.ds(BUP + b, 1), :]
        cdf = 0.5 + 0.5 * lax.erf(u * 0.7071067811865476)
        z = (u * cdf).astype(bf16)
        slope = cdf + u * jnp.exp2(u * u * (-0.5 * LOG2E)) * 0.3989422804014327
        if enc_ref is not None:
            dh1_ref[...] += nn(z, wdown_ref[cols, :])
        put_flat(main_ref, DOWN_BASE + shift + T_DOWN * FB * b, T_DOWN, tn(z, dy2))
        du = (nt(dy2, wdown_ref[cols, :]) * slope).astype(bf16)
        put_row(main_ref, small + 24 + 3 * b, column_sum(du))
        put_up(main_ref, shift, b, nn(a_t_ref[...], du))
        da2_ref[...] += nt(du, wup_ref[:, cols])

    if enc_ref is not None:
        enc_ref[...] = dh1_ref[...].astype(bf16)
    dgain = jnp.zeros((1, D), f32)
    dshift = jnp.zeros((1, D), f32)
    for i in range(rows_all // RC):
        rows = slice(i * RC, (i + 1) * RC)
        xhat, r = stats(h1_ref[rows, :])
        dy = da2_ref[rows, :]
        dgain += column_sum(dy * xhat)
        dshift += column_sum(dy)
        dh1_ref[rows, :] = g_ref[rows, :].astype(f32) + norm_backward(dy, xhat, r, vec(vec_ref, G2))
    put_row(main_ref, small + 3, dgain)
    put_row(main_ref, small + 18, dshift)


def out_backward(shift, dh1_ref, o_t_ref, wo_ref, main_ref, do_ref, delta_ref):
    dy1 = dh1_ref[...].astype(bf16)
    put_row(main_ref, N_MAIN + shift + 15, column_sum(dy1))
    put_flat(main_ref, 0, T_O, nn(o_t_ref[...], dy1))
    do_ref[...] = nt(dy1, wo_ref[...]).astype(bf16)
    do_t = nt(wo_ref[...], dy1).astype(bf16).astype(f32)
    prod = do_t * o_t_ref[...].astype(f32)
    for h in range(HEADS):
        delta_ref[h : h + 1, :] = jnp.sum(prod[h * HD : (h + 1) * HD, :], axis=0, keepdims=True)


def attend_backward(q_ref, kv_ref, lse_ref, do_ref, delta_ref, dqkv_ref, dkv_oth_ref, dq_t_ref, rows, after_pair):
    @pl.loop(0, HEADS // 2)
    def _(hp):
        cols = pl.ds(pl.multiple_of(hp * LANES, LANES), LANES)
        for half in range(2):
            keys, values = kv_ref[half, 0, :, cols], kv_ref[half, 1, :, cols]
            keys_t = keys.T
            dk = dv = 0.0
            for t in range(2):
                head = pl.ds(2 * hp + t, 1)
                part = slice(t * HD, (t + 1) * HD)
                q_one, do_one = one_head(q_ref[:, cols], t), one_head(do_ref[:, cols], t)
                scores = pad_mask(nt(keys, q_one), rows)
                probs = jnp.exp2(scores * SCALE2 - lse_ref[head, :])
                dv += nn(probs.astype(bf16), do_one)
                ds = (probs * (nt(values, do_one) - delta_ref[head, :])).astype(bf16)
                dk += nn(ds, q_one)
                dq_part = nn(keys_t[part, :], ds) * 0.125
                if half == 0:
                    dq_t_ref[part, :] = dq_part
                else:
                    dq_t_ref[part, :] += dq_part
            dst = (dqkv_ref.at[pl.ds(1, 2)], dkv_oth_ref)[half]
            dst[0, :, cols] = (dk * 0.125).astype(bf16)
            dst[1, :, cols] = dv.astype(bf16)
        dqkv_ref[0, :, cols] = dq_t_ref[...].T.astype(bf16)
        for k in range(HEADS // 2):

            @pl.when(hp == k)
            def _():
                after_pair(k)


def qkv_backward(shift, x_ref, dqkv_ref, dkv_in_ref, dh1_ref, wqkv_ref, vec_ref, gq_ref, tail_ref,
                 a_ref, a_t_ref, da_ref, dx_ref, after_blocks):
    def first(rows):
        xhat, _ = stats(x_ref[rows, :].astype(f32))
        a_ref[rows, :] = (xhat * vec(vec_ref, G1) + vec(vec_ref, N1)).astype(bf16)
        for b in range(2):
            total = dqkv_ref[b + 1, rows, :].astype(f32) + dkv_in_ref[b, rows, :].astype(f32)
            dqkv_ref[b + 1, rows, :] = total.astype(bf16)

    each_chunk(x_ref.shape[0], first)
    a_t_ref[...] = a_ref[...].T
    da_ref[...] = jnp.zeros_like(da_ref)

    @pl.loop(0, 3)
    def _(b):
        low = dqkv_ref[b]

        @pl.when(b != 1)
        def _():
            put_row(tail_ref, shift + 9 + jnp.where(b == 2, 3, 0), column_sum(low))

        put_flat(gq_ref, 3 * b, T_QKV, nn(a_t_ref[...], low))
        da_ref[...] += nt(low, wqkv_ref[:, pl.ds(pl.multiple_of(b * D, D), D)])

    after_blocks()
    dgain = jnp.zeros((1, D), f32)
    dshift = jnp.zeros((1, D), f32)
    for i in range(x_ref.shape[0] // RC):
        rows = slice(i * RC, (i + 1) * RC)
        xhat, r = stats(x_ref[rows, :].astype(f32))
        dy = da_ref[rows, :]
        dgain += column_sum(dy * xhat)
        dshift += column_sum(dy)
        dx_ref[rows, :] = (dh1_ref[rows, :] + norm_backward(dy, xhat, r, vec(vec_ref, G1))).astype(dx_ref.dtype)
    put_row(tail_ref, shift + 0, dgain)
    put_row(tail_ref, shift + 6, dshift)


def greet(partners):
    for where in partners:
        pl.semaphore_signal(pltpu.get_barrier_semaphore(), inc=1, device_id=where, device_id_type=MESH)


def to(src, dst, send, recv, where):
    return pltpu.make_async_remote_copy(
        src_ref=src, dst_ref=dst, send_sem=send, recv_sem=recv, device_id=where, device_id_type=MESH
    )


def levels_of(ranks, late_x=False):
    bits = ranks.bit_length() - 1
    groups = [(b, min(2, bits - b)) for b in range(2, bits, 2)]
    return [(0, 1), (1, 1), None] + groups if late_x else [(0, 1), None, (1, 1)] + groups


def peers_of(level):
    low, count = level
    return range(1, 1 << count)


def copies_of(levels):
    crossing = levels.index(None)
    down = []
    for k, level in enumerate(levels):
        down.append(1 if level is None else ((1 << level[1]) - 1) * (2 if k < crossing else 1))
    up = [(1 << level[1]) - 1 for level in reversed(levels) if level is not None]
    return down, up


class Reducer:
    def __init__(self, ranks, half_rows, acc, res, landing, send_sems, recv_sems):
        self.acc, self.res, self.landing = acc, res, landing
        self.send_sems, self.recv_sems = send_sems, recv_sems
        self.half_rows = half_rows
        self.n = half_rows // CHUNKS
        self.orders = [levels_of(ranks), levels_of(ranks, True)]
        self.stages = 2 * len(self.orders[0]) - 1
        self.state = {}
        self.begun = []

    def plan(self, ci):
        levels = self.orders[ci % 2]
        down, up = copies_of(levels)
        return levels, down + up

    def place(self):
        return lax.axis_index("shard"), lax.axis_index("rep")

    def index(self, level):
        _, r = self.place()
        return (r >> level[0]) & ((1 << level[1]) - 1)

    def size(self, levels, upto):
        size = self.n
        for level in levels[: upto + 1]:
            if level is not None:
                size >>= level[1]
        return size

    def offset(self, levels, upto):
        at = 0
        for k, level in enumerate(levels[: upto + 1]):
            if level is not None:
                at = at + self.index(level) * self.size(levels, k)
        return at

    def slot(self, ci, k, m):
        levels, counts = self.plan(ci)
        return sum(counts[i] * self.size(levels, i) for i in range(k)) + m * self.size(levels, k)

    def pair_rows(self, at, size):
        return pl.ds(at // 2 if isinstance(at, int) else lax.div(at, 2), size // 2)

    def describe(self, ci, stage):
        layer, base = ci // CHUNKS, ci % CHUNKS * self.n
        levels, counts = self.plan(ci)
        s, r = self.place()
        first = sum(counts[:stage])
        out = []

        def add(src, dst, where):
            k = first + len(out)
            out.append(to(src, dst, self.send_sems.at[ci, k], self.recv_sems.at[ci, k], where))

        def send(half, at, size, where):
            rows = self.pair_rows((layer * 2 + half) * self.half_rows + base + at, size)
            add(self.acc.at[rows], self.landing.at[ci, self.pair_rows(self.slot(ci, stage, len(out)), size)], where)

        if stage < len(levels):
            level, size = levels[stage], self.size(levels, stage)
            if level is None:
                send(1 - s, self.offset(levels, stage), size, {"shard": 1 - s})
            else:
                for half in range(2) if stage < levels.index(None) else (s,):
                    for m in peers_of(level):
                        at = self.offset(levels, stage - 1) + (self.index(level) ^ m) * size
                        send(half, at, size, {"rep": r ^ (m << level[0])})
        else:
            level = [one for one in reversed(levels) if one is not None][stage - len(levels)]
            k = levels.index(level)
            at = layer * self.half_rows + base + self.offset(levels, k)
            ref = self.res.at[self.pair_rows(at, self.size(levels, k))]
            for m in peers_of(level):
                add(ref, ref, {"rep": r ^ (m << level[0])})
        return out

    def begin(self, ci, stage):
        for copy in self.describe(ci, stage):
            copy.start()
        self.begun.append((ci, stage))

    def finish(self, ci, stage):
        layer, base = ci // CHUNKS, ci % CHUNKS * self.n
        levels, counts = self.plan(ci)
        s, _ = self.place()
        for copy in self.describe(ci, stage):
            copy.wait_recv()
        if stage >= len(levels):
            return
        size = self.size(levels, stage)
        acc = self.acc.reshape(2 * self.acc.shape[0], LANES)
        res = self.res.reshape(2 * self.res.shape[0], LANES)
        count = self.landing.shape[1] * 2
        landing = self.landing.reshape(self.landing.shape[0] * count, LANES)
        step = 16
        while size % (2 * step) == 0 and step < 128:
            step *= 2
        halves = (0, 1) if stage < levels.index(None) else (s,)
        each = counts[stage] // len(halves)
        for k, half in enumerate(halves):
            slots = [self.slot(ci, stage, k * each + m) for m in range(each)]
            src = (layer * 2 + half) * self.half_rows + base + self.offset(levels, stage)
            out, out_at = acc, src
            if stage == len(levels) - 1:
                out, out_at = res, layer * self.half_rows + base + self.offset(levels, stage)

            @pl.loop(0, size // step)
            def _(i):
                def rows(start):
                    return pl.ds(pl.multiple_of(start + i * step, 16), step)

                total = acc[rows(src), :].astype(f32)
                for slot in slots:
                    total = total + landing[rows(ci * count + slot), :].astype(f32)
                out[rows(out_at), :] = total.astype(bf16)

    def advance(self, chunks):
        for ci in chunks:
            stage = self.state.get(ci, -1)
            if stage >= self.stages:
                continue
            if stage >= 0:
                self.finish(ci, stage)
            stage += 1
            self.state[ci] = stage
            if stage < self.stages:
                self.begin(ci, stage)

    def drain(self):
        for ci, stage in self.begun:
            for copy in self.describe(ci, stage):
                copy.wait_send()


def pad_rows(src, dst):
    rows, pad = src.shape[0], dst.shape[0]
    edge = rows // 16 * 16
    dst[:edge, :] = src[:edge, :]
    dst[edge:, :] = jnp.zeros((pad - edge, dst.shape[1]), dst.dtype)
    dst[edge:rows, :] = src[edge:, :]


def step_kernel(ranks, rows, half_rows, frames, cot_in, weights, enc_out, dx_out, out0, out1, x0, cot,
                wqkv0, wo0, wup0, wdown0, vec0, wqkv1, wo1, wup1, wdown1, vec1,
                q0, kv0, o_t0, lse0, h10, x1, q1, kv1, o_t1, lse1, h11, a2, a_t, da, dh1,
                do, delta, dq, dqkv, dkv_oth, dkv_in, dq_t, values_t, enc_in, main, tail, acc, res, landing,
                load, store, swap_sems, relay_sems, rest_sems, hop_sems, kv_sems, send_sems, recv_sems):
    s, r = lax.axis_index("shard"), lax.axis_index("rep")
    shift = half_rows - N_HALF
    across, core, beside = {"shard": 1 - s}, {"rep": r ^ 1}, {"rep": r ^ 2}
    diagonal = {"shard": 1 - s, "rep": r ^ 1}
    stays = s == r % 2
    filling = pltpu.make_async_copy(weights, acc.at[pl.ds(s * N_HALF, N_HALF)], load.at[0])
    filling.start()
    partners = [{"rep": r ^ (m << level[0])} for level in levels_of(ranks) if level is not None for m in peers_of(level)]
    partners += [diagonal, across]
    greet(partners)
    outs = [wqkv0, wo0, wup0, wdown0, vec0, wqkv1, wo1, wup1, wdown1, vec1]
    flat = acc.reshape(2 * acc.shape[0], LANES)
    pad_rows(frames, a2)
    pad_rows(cot_in, dq)
    filling.wait()

    @pl.when(s == 0)
    def _():
        unpack_weights(flat, outs, main, 0)

    pl.semaphore_wait(pltpu.get_barrier_semaphore(), len(partners))

    def swap(src, dst, k):
        @pl.when(stays)
        def _():
            pltpu.make_async_copy(src, dst, load.at[1 + k]).start()

        @pl.when(jnp.logical_not(stays))
        def _():
            to(src, dst, swap_sems.at[0, k], swap_sems.at[1, k], diagonal).start()

    def swapped(src, dst, k):
        @pl.when(stays)
        def _():
            pltpu.make_async_copy(src, dst, load.at[1 + k]).wait()

        @pl.when(jnp.logical_not(stays))
        def _():
            to(src, dst, swap_sems.at[0, k], swap_sems.at[1, k], diagonal).wait()

    q = r % 4
    second = (N_HALF - N_QKV - N_SMALL) // 4
    last = N_QKV + 4 * second
    part = D // 4

    def flow(kind, c, which):
        return (hop_sems.at[kind, 0, c], hop_sems.at[kind, 1, c], (across, beside, core, core)[kind])

    def wide(c, which):
        w, start, size = ((wqkv0, 0, part // 2), (wqkv0, part // 2, part // 2), (wqkv1, 0, part))[c]
        return w.at[pl.ds(pl.multiple_of(which * part + start, 16), size), :]

    def units(c, which, half):
        at, quarter, start, size = (
            (N_QKV, second, 0, second // 2),
            (N_QKV, second, second // 2, second - second // 2),
            (0, N_QKV // 4, 0, N_QKV // 8),
            (0, N_QKV // 4, N_QKV // 8, N_QKV // 8),
        )[c - 3]
        return acc.at[pl.ds(half * N_HALF + at + which * quarter + start, size)]

    def hop(kind, c):
        which = q ^ 2 if kind == 3 else q
        half = s if kind == 0 else 1 - s
        ref = wide(c, which) if c < 3 else units(c, which, half)
        return to(ref, ref, *flow(kind, c, which))

    def only(c, sender):
        if c in (3, 4):
            return lambda do_it: do_it()
        return pl.when(s == ((0 if sender else 1) if c < 3 else (1 if sender else 0)))

    def launch(c):
        @only(c, True)
        def _():
            hop(0, c).start()

    def spread(c):
        @only(c, False)
        def _():
            hop(0, c).wait_recv()
            hop(1, c).start()
            hop(2, c).start()

    def pass_on(c):
        @only(c, False)
        def _():
            hop(1, c).wait_recv()
            hop(3, c).start()

    def arrived(c):
        @only(c, False)
        def _():
            hop(2, c).wait_recv()
            hop(3, c).wait_recv()

    def sent(c):
        @only(c, True)
        def _():
            hop(0, c).wait_send()

        @only(c, False)
        def _():
            for kind in (1, 2, 3):
                hop(kind, c).wait_send()

    rest = acc.at[pl.ds(s * N_HALF + last, N_HALF - last)]
    rests = to(rest, rest, rest_sems.at[0], rest_sems.at[1], across)
    launch(0)
    launch(1)
    rests.start()
    top, low = pl.ds(0, x0.shape[0] // 2), pl.ds(x0.shape[0] // 2, x0.shape[0] // 2)
    direct = to(a2.at[top], x0.at[top], swap_sems.at[0, 0], swap_sems.at[1, 0], diagonal)
    aside = to(a2.at[low], do.at[low], relay_sems.at[0, 0], relay_sems.at[0, 1], core)
    onward = to(do.at[low], x0.at[low], relay_sems.at[1, 0], relay_sems.at[1, 1], across)
    local = pltpu.make_async_copy(a2, x0, load.at[1])

    @pl.when(jnp.logical_not(stays))
    def _():
        aside.start()
        direct.start()

    @pl.when(stays)
    def _():
        local.start()
        aside.wait_recv()
        onward.start()

    for c in (2, 3, 4, 5, 6):
        launch(c)
    spread(0)
    spread(1)
    rests.wait_recv()
    unpack_small(flat, outs, main)
    pass_on(0)
    pass_on(1)
    arrived(0)
    arrived(1)

    exchanges = []

    def exchange(src, dst):
        k = len(exchanges)
        copy = to(src, dst, kv_sems.at[0, k], kv_sems.at[1, k], core)
        copy.start()
        exchanges.append(copy)
        return copy


    @pl.when(jnp.logical_not(stays))
    def _():
        aside.wait_send()
        direct.wait()
        onward.wait_recv()

    @pl.when(stays)
    def _():
        local.wait()

    qkv_forward(x0, wqkv0, vec0, q0, kv0.at[0])
    first_kv = exchange(kv0.at[0], kv0.at[1])
    spread(2)
    spread(3)
    pass_on(2)
    first_kv.wait_recv()

    def relay(k):
        spread(4 + k)
        if k == 0:
            swap(dq, cot, 1)
        if k == 2:
            pass_on(3)
            pass_on(4)

    attend(q0, kv0, o_t0, lse0, values_t, rows, relay)
    pass_on(5)
    pass_on(6)
    for c in (2, 3, 4, 5, 6):
        arrived(c)
    for c in range(7):
        sent(c)
    rests.wait_send()

    @pl.when(stays)
    def _():
        onward.wait_send()

    for which in (1, 2, 3):
        unpack_weights(flat, outs, main, which)
    out_forward(x0, o_t0, wo0, vec0, h10)
    second_norm(h10, vec0, a2)
    mlp_forward(h10, a2, wup0, wdown0, vec0, x1)
    qkv_forward(x1, wqkv1, vec1, q1, kv1.at[0])
    exchange(kv1.at[0], kv1.at[1]).wait_recv()
    attend(q1, kv1, o_t1, lse1, values_t, rows)
    out_forward(x1, o_t1, wo1, vec1, h11)
    second_norm(h11, vec1, a2)

    enc = wdown1.at[pl.ds(0, x0.shape[0])]
    reducer = Reducer(ranks, half_rows, acc, res, landing, send_sems, recv_sems)
    early = [[layer * CHUNKS + c for c in range(CHUNKS // 2, CHUNKS)] for layer in range(LAYERS)]
    late = [[layer * CHUNKS + c for c in range(CHUNKS // 2)] for layer in range(LAYERS)]
    moved = (N_MAIN + shift) // 16 * 16

    def main_start():
        edge = N_HALF - N_QKV
        main[edge : edge + shift, :] = jnp.zeros((shift, LANES), f32)
        last = N_MAIN + shift
        main[last:, :] = jnp.zeros((main.shape[0] - last, LANES), f32)

    def main_end(layer):
        base = layer * 2 * half_rows
        to_low(main, 0, flat, base + N_QKV, N_MAIN)
        to_low(main, N_MAIN, flat, base + N_QKV + N_MAIN, main.shape[0] - N_MAIN)
        to_low(main, half_rows - N_QKV, flat, base + N_QKV + moved, 32, 32)
        tail[...] = main[moved : moved + 32, :]

    def late_start(layer):
        to_low(main, 0, flat, layer * 2 * half_rows, N_QKV)
        reducer.advance(late[layer][1:])

    def late_end(layer):
        to_low(tail, 0, flat, layer * 2 * half_rows + half_rows, 32, 32)
        reducer.advance(late[layer][:1])

    tail_shift = N_MAIN + shift - moved
    main_start()
    swapped(dq, cot, 1)
    mlp_backward(shift, cot, h11, a2, a_t, wup1, wdown1, vec1, main, da, dh1, enc)
    swap(enc, enc_in, 2)
    out_backward(shift, dh1, o_t1, wo1, main, do, delta)
    main_end(1)
    reducer.advance(early[1])
    attend_backward(q1, kv1, lse1, do, delta, dqkv, dkv_oth, dq_t, rows,
                    lambda hp: reducer.advance(early[1]))
    exchange(dkv_oth, dkv_in).wait_recv()
    qkv_backward(tail_shift, x1, dqkv, dkv_in, dh1, wqkv1, vec1, main, tail, a2, a_t, da, h11,
                 lambda: late_start(1))
    late_end(1)
    reducer.advance(early[1])
    main_start()
    second_norm(h10, vec0, a2)
    reducer.advance(late[1])
    exchanges[-1].wait_send()
    mlp_backward(shift, h11, h10, a2, a_t, wup0, wdown0, vec0, main, da, dh1, None)
    reducer.advance(early[1])
    out_backward(shift, dh1, o_t0, wo0, main, do, delta)
    main_end(0)
    reducer.advance(late[1])
    reducer.advance(early[0])
    attend_backward(q0, kv0, lse0, do, delta, dqkv, dkv_oth, dq_t, rows,
                    lambda hp: reducer.advance(early[1] + late[1] + early[0]))
    exchange(dkv_oth, kv1.at[1]).wait_recv()
    qkv_backward(tail_shift, x0, dqkv, kv1.at[1], dh1, wqkv0, vec0, main, tail, a2, a_t, da, do,
                 lambda: late_start(0))
    swap(do, cot, 3)
    late_end(0)
    others = early[0] + late[1] + early[1]
    for tick in range(reducer.stages):
        reducer.advance(late[0][::-1])
        reducer.advance(others)
    reducer.drain()
    for k, copy in enumerate(exchanges):
        if k != 2:
            copy.wait_send()

    @pl.when(s == 1)
    def _():
        out = res.reshape(2 * res.shape[0], LANES)
        for layer in range(LAYERS):
            one = pl.ds(layer * half_rows, 32)
            two = pl.ds(layer * half_rows + N_QKV + moved - half_rows, 32)
            keep = out[one, :]
            out[one, :] = out[two, :]
            out[two, :] = keep

    outs = [
        pltpu.make_async_copy(res.at[pl.ds(k * half_rows // 2, half_rows // 2)], out, store.at[k])
        for k, out in enumerate((out0, out1))
    ]
    for copy in outs:
        copy.start()
    swapped(enc, enc_in, 2)
    enc_out[...] = enc_in[:rows, :]
    swapped(do, cot, 3)
    dx_out[...] = cot[:rows, :]
    for copy in outs:
        copy.wait()


def adam_kernel(g0_ref, g1_ref, w_ref, one_ref, two_ref, g_out, p_out, one_out, two_out):
    block = 2 * g0_ref.shape[0]
    flat = lambda ref: ref.reshape(LAYERS * block, LANES)
    low = lambda ref: ref.reshape(block, LANES)
    for layer, g_ref in enumerate((g0_ref, g1_ref)):
        flat(g_out)[pl.ds(layer, block, stride=LAYERS), :] = low(g_ref)[...].astype(f32)

    @pl.loop(0, LAYERS * block // 128)
    def _(i):
        rows = pl.ds(pl.multiple_of(i * 128, 128), 128)
        grad = flat(g_out)[rows, :]
        weight = flat(w_ref)[rows, :].astype(f32)
        one = beta_one * flat(one_ref)[rows, :] + (1.0 - beta_one) * grad
        two = beta_two * flat(two_ref)[rows, :] + (1.0 - beta_two) * grad * grad
        square = two * (1.0 / fix_two)
        root = square * lax.rsqrt(square)
        step = one * lax.rsqrt(square + adam_eps * (2.0 * root + adam_eps))
        flat(p_out)[rows, :] = weight * (1.0 - rate * decay) - (rate / fix_one) * step
        flat(one_out)[rows, :] = one
        flat(two_out)[rows, :] = two


def to_rows(array):
    view = array.reshape(LAYERS, -1, LANES)
    return with_layout_constraint(view, Layout(major_to_minor=(1, 0, 2))).transpose(1, 0, 2)


def from_rows(array):
    view = with_layout_constraint(array.transpose(1, 0, 2), Layout(major_to_minor=(1, 0, 2)))
    return view.reshape(LAYERS, -1)


def body(ranks, frames_in, params, moment_one, moment_two, cotangent):
    rows = frames_in.shape[1]
    pad = -(-rows // RC) * RC

    def vm(shape, dtype):
        return pltpu.VMEM(shape, dtype)

    def sd(shape, dtype):
        return jax.ShapeDtypeStruct(shape, dtype)

    unit = 16 * ranks * CHUNKS
    half_rows = -(-N_HALF // unit) * unit
    tail_rows = -(-(half_rows - N_HALF + N_SMALL + 32) // 64) * 64
    w_rows = to_rows(params)
    row_b = vm((pad, D), bf16)
    kv_b = vm((2, pad, D), bf16)
    kv_both = vm((2, 2, pad, D), bf16)
    row_f = vm((pad, D), f32)
    lse_f = vm((8, pad), f32)
    o_t_b = vm((D, pad), bf16)
    layer_w = [vm((D, 3 * D), bf16), vm((D, D), bf16), vm((D, FF), bf16), vm((FF, D), bf16), vm((VECS, D), f32)]
    down, up = copies_of(levels_of(ranks, True))
    total = LAYERS * CHUNKS
    chunk_sems = pltpu.SemaphoreType.DMA((total, sum(down) + sum(up)))
    anywhere = pl.BlockSpec(memory_space=pl.ANY)
    inside = pl.BlockSpec(memory_space=pltpu.VMEM)
    enc, dx, g0, g1 = pl.pallas_call(
        partial(step_kernel, ranks, rows, half_rows),
        out_shape=[sd((rows, D), bf16)] * 2 + [sd((half_rows // 2, 2, LANES), bf16)] * 2,
        in_specs=[inside, inside, anywhere],
        out_specs=[inside] * 2 + [anywhere] * 2,
        scratch_shapes=[row_b, row_b] + layer_w * 2
        + [row_b, kv_both, o_t_b, lse_f, row_f, row_f, row_b, kv_both, o_t_b, lse_f, row_f, row_b, o_t_b]
        + [row_f, row_f, row_b, lse_f, row_b, vm((3, pad, D), bf16), kv_b, kv_b]
        + [vm((LANES, pad), f32), vm((LANES + 16, 2 * pad), bf16), row_b]
        + [vm((N_MAIN + tail_rows, LANES), f32), vm((32, LANES), f32), vm((2 * half_rows, 2, LANES), bf16)]
        + [vm((half_rows, 2, LANES), bf16), vm((total, half_rows // CHUNKS, 2, LANES), bf16)]
        + [pltpu.SemaphoreType.DMA((5,)), pltpu.SemaphoreType.DMA((2,)), pltpu.SemaphoreType.DMA((2, 4))]
        + [pltpu.SemaphoreType.DMA((2, 2)), pltpu.SemaphoreType.DMA((2,)), pltpu.SemaphoreType.DMA((4, 2, 7)), pltpu.SemaphoreType.DMA((2, 4))]
        + [chunk_sems, chunk_sems],
        compiler_params=pltpu.CompilerParams(vmem_limit_bytes=67043328, collective_id=0, has_side_effects=True),
        name="step",
    )(frames_in[0], cotangent[0], w_rows)
    encoded, frames_grad = enc[None], dx[None]
    block = 1280
    low = pl.BlockSpec((block // 2, 2, LANES), lambda i: (i, 0, 0))
    spec = pl.BlockSpec((block, 2, LANES), lambda i: (i, 0, 0))
    row_shape = sd((N_HALF, 2, LANES), f32)
    grad, new_params, new_one, new_two = pl.pallas_call(
        adam_kernel, grid=(pl.cdiv(N_HALF, block),), in_specs=[low, low, spec, spec, spec], out_specs=[spec] * 4,
        out_shape=[row_shape] * 4,
        compiler_params=pltpu.CompilerParams(vmem_limit_bytes=62 << 20), name="adam",
    )(g0, g1, w_rows, to_rows(moment_one), to_rows(moment_two))
    return (encoded, frames_grad, from_rows(grad), from_rows(new_params), from_rows(new_one), from_rows(new_two))


def solution(mesh):
    in_specs = (
        P("rep", "shard", None),
        P(None, "shard"),
        P(None, "shard"),
        P(None, "shard"),
        P("rep", "shard", None),
    )
    out_specs = (
        P("rep", "shard", None),
        P("rep", "shard", None),
        P(None, "shard"),
        P(None, "shard"),
        P(None, "shard"),
        P(None, "shard"),
    )
    return jax.shard_map(
        partial(body, mesh.shape["rep"]), mesh=mesh, in_specs=in_specs, out_specs=out_specs, check_vma=False
    )
```
